32 devices in a mesh: fsdp: 2 (over x), ctx: 4 (over y, core), tp: 4 (over z).
Axes of the slice: x: 2, y: 2, z: 4, core: 2. Of those that a mesh axis runs over, the one named last changes fastest.
Arguments:
- tokens: bfloat16 [2, 3072, 2304], P('fsdp', 'ctx'), may hold values from -6 to 6
- cotangent: bfloat16 [2, 3072, 2304], P('fsdp', 'ctx'), may hold values from -6 to 6
- prefix_length: int32 [2], P('fsdp'), may hold values from 307 to 1536
- sequence_adapter_index: int32 [2], P('fsdp'), may hold values from 0 to 7
- gains: float32 [4, 2304], replicated, may hold values from 0.5 to 1.5
- query_weight: bfloat16 [2304, 2048], P(('fsdp', 'ctx'), 'tp'), may hold values from -0.1875 to 0.1875
- key_weight: bfloat16 [2304, 1024], P(('fsdp', 'ctx'), 'tp'), may hold values from -0.1875 to 0.1875
- value_weight: bfloat16 [2304, 1024], P(('fsdp', 'ctx'), 'tp'), may hold values from -0.125 to 0.125
- output_weight: bfloat16 [2048, 2304], P('tp', ('fsdp', 'ctx')), may hold values from -0.125 to 0.125
- gate_weight: bfloat16 [2304, 9216], P(('fsdp', 'ctx'), 'tp'), may hold values from -0.125 to 0.125
- up_weight: bfloat16 [2304, 9216], P(('fsdp', 'ctx'), 'tp'), may hold values from -0.125 to 0.125
- down_weight: bfloat16 [9216, 2304], P('tp', ('fsdp', 'ctx')), may hold values from -0.0625 to 0.0625
- adapter_first_input: bfloat16 [5, 8, 2304, 16], replicated, may hold values from -0.125 to 0.125
- adapter_second_query: bfloat16 [8, 16, 2048], P(None, None, 'tp'), may hold values from -1.5 to 1.5
- adapter_second_keyvalue: bfloat16 [2, 8, 16, 1024], P(None, None, None, 'tp'), may hold values from -1.5 to 1.5
- adapter_second_gate: bfloat16 [2, 8, 16, 9216], P(None, None, None, 'tp'), may hold values from -1.5 to 1.5
- adapter_first_output: bfloat16 [8, 2048, 16], P(None, 'tp'), may hold values from -0.125 to 0.125
- adapter_first_down: bfloat16 [8, 9216, 16], P(None, 'tp'), may hold values from -0.0625 to 0.0625
- adapter_second_output: bfloat16 [2, 8, 16, 2304], replicated, may hold values from -1.5 to 1.5
Outputs:
- activations: bfloat16 [2, 3072, 2304], P('fsdp', 'ctx')
- input_grad: float32 [2, 3072, 2304], P('fsdp', 'ctx')
- grad_a_in: float32 [5, 8, 2304, 16], P(None, None, ('fsdp', 'ctx'))
- grad_b_query: float32 [8, 16, 2048], P(None, None, 'tp')
- grad_b_kv: float32 [2, 8, 16, 1024], P(None, None, None, 'tp')
- grad_b_gate_up: float32 [2, 8, 16, 9216], P(None, None, None, 'tp')
- grad_a_out: float32 [8, 2048, 16], P(None, 'tp')
- grad_a_down: float32 [8, 9216, 16], P(None, 'tp')
- grad_b_out: float32 [2, 8, 16, 2304], P(None, None, None, ('fsdp', 'ctx'))
The draws below stay inside these ranges and needn't reach their ends.
All inputs are finite; a program needn't handle non-finite values.
Results may differ from the reference program's by a relative error of at most 0.03.
Values may be sent and summed in bfloat16 or wider, within the bound.
A program may use at most 256 MiB of HBM per device.

```python
import math
import jax
import jax.numpy as jnp
from jax import lax

MODEL_WIDTH = 2304
QUERY_HEADS = 8
KEY_HEADS = 4
HEAD_SIZE = 256
HIDDEN_UNITS = 9216
ADAPTER_RANK = 16
ADAPTER_COUNT = 8
LEN = 3072
SEQS = 2


def steps_of(key, dims, shards, least, high):
    def one(position, parts):
        heights = jax.random.uniform(jax.random.fold_in(jax.random.fold_in(key, 6), position), (parts,), jnp.float32, least / len(shards), high / len(shards))
        return jnp.repeat(jnp.exp(heights), dims[position] // parts).reshape((-1,) + (1,) * (len(dims) - position - 1))

    level = one(*shards[0])
    for cut in shards[1:]:
        level = level * one(*cut)
    return level


def scatter_about(key, dims, scale, reach, shards=(), kind=jnp.bfloat16):
    array = scale * jax.random.normal(key, dims, jnp.float32)
    if shards:
        array = array * steps_of(key, dims, shards, -0.22, 0.18)
    return jnp.clip(array, -reach, reach).astype(kind)


def setup_inputs(seed: int = 0) -> dict:
    key_of = jax.random.split(jax.random.key(seed), 20)
    return {
        "tokens": scatter_about(key_of[0], (SEQS, LEN, MODEL_WIDTH), 1.0, 6.0, ((0, 2), (1, 4))),
        "cotangent": scatter_about(key_of[1], (SEQS, LEN, MODEL_WIDTH), 1.0, 6.0, ((0, 2), (1, 4))),
        "prefix_length": jax.random.randint(key_of[2], (SEQS,), LEN // 10, LEN // 2 + 1).astype(jnp.int32),
        "sequence_adapter_index": jax.random.randint(key_of[3], (SEQS,), 0, ADAPTER_COUNT).astype(jnp.int32),
        "gains": jnp.clip(1.0 + 0.1 * jax.random.normal(key_of[4], (4, MODEL_WIDTH), jnp.float32), 0.5, 1.5),
        "query_weight": scatter_about(key_of[5], (MODEL_WIDTH, QUERY_HEADS * HEAD_SIZE), (MODEL_WIDTH // 2) ** -0.5, 0.1875, ((0, 8), (1, 4))),
        "key_weight": scatter_about(key_of[6], (MODEL_WIDTH, KEY_HEADS * HEAD_SIZE), (MODEL_WIDTH // 2) ** -0.5, 0.1875, ((0, 8), (1, 4))),
        "value_weight": scatter_about(key_of[7], (MODEL_WIDTH, KEY_HEADS * HEAD_SIZE), MODEL_WIDTH ** -0.5, 0.125, ((0, 8), (1, 4))),
        "output_weight": scatter_about(key_of[8], (QUERY_HEADS * HEAD_SIZE, MODEL_WIDTH), (QUERY_HEADS * HEAD_SIZE) ** -0.5, 0.125, ((0, 4), (1, 8))),
        "gate_weight": scatter_about(key_of[9], (MODEL_WIDTH, HIDDEN_UNITS), MODEL_WIDTH ** -0.5, 0.125, ((0, 8), (1, 4))),
        "up_weight": scatter_about(key_of[10], (MODEL_WIDTH, HIDDEN_UNITS), MODEL_WIDTH ** -0.5, 0.125, ((0, 8), (1, 4))),
        "down_weight": scatter_about(key_of[11], (HIDDEN_UNITS, MODEL_WIDTH), HIDDEN_UNITS ** -0.5, 0.0625, ((0, 4), (1, 8))),
        "adapter_first_input": scatter_about(key_of[12], (5, ADAPTER_COUNT, MODEL_WIDTH, ADAPTER_RANK), MODEL_WIDTH ** -0.5, 0.125),
        "adapter_second_query": scatter_about(key_of[13], (ADAPTER_COUNT, ADAPTER_RANK, QUERY_HEADS * HEAD_SIZE), ADAPTER_RANK ** -0.5, 1.5, ((2, 4),)),
        "adapter_second_keyvalue": scatter_about(key_of[14], (2, ADAPTER_COUNT, ADAPTER_RANK, KEY_HEADS * HEAD_SIZE), ADAPTER_RANK ** -0.5, 1.5, ((3, 4),)),
        "adapter_second_gate": scatter_about(key_of[15], (2, ADAPTER_COUNT, ADAPTER_RANK, HIDDEN_UNITS), ADAPTER_RANK ** -0.5, 1.5, ((3, 4),)),
        "adapter_first_output": scatter_about(key_of[16], (ADAPTER_COUNT, QUERY_HEADS * HEAD_SIZE, ADAPTER_RANK), (QUERY_HEADS * HEAD_SIZE) ** -0.5, 0.125, ((1, 4),)),
        "adapter_first_down": scatter_about(key_of[17], (ADAPTER_COUNT, HIDDEN_UNITS, ADAPTER_RANK), HIDDEN_UNITS ** -0.5, 0.0625, ((1, 4),)),
        "adapter_second_output": scatter_about(key_of[18], (2, ADAPTER_COUNT, ADAPTER_RANK, MODEL_WIDTH), ADAPTER_RANK ** -0.5, 1.5),
    }


@jax.custom_vjp
def low(v):
    return lax.optimization_barrier(v.astype(jnp.bfloat16)).astype(jnp.float32)

@jax.custom_vjp
def low_back(v):
    return v

def low_keep(v):
    return (low(v), None)

def low_pass(kept, grad):
    return (grad,)

def back_keep(v):
    return (v, None)

def back_low(kept, grad):
    return (low(grad),)
low.defvjp(low_keep, low_pass)
low_back.defvjp(back_keep, back_low)
epsilon = 1e-06
soft_cap = 50.0
masked_low = -1e+30
highest = lax.Precision.HIGHEST

def matmul(left, right):
    return jnp.dot(left, right, precision=highest, preferred_element_type=jnp.float32)

def rms_norm(values, gain):
    return values * lax.rsqrt(lax.optimization_barrier(jnp.mean(values * values, axis=-1, keepdims=True)) + epsilon) * gain

def rotate(values, positions, sign):
    half = values.shape[-1] // 2
    freqs = jnp.exp(jnp.arange(half, dtype=jnp.float32) * (-2.0 * math.log(10000.0) / values.shape[-1]))
    angle = positions[:, None] * freqs[None, :]
    cosine = jnp.cos(angle)[:, None, :]
    sine = sign * jnp.sin(angle)[:, None, :]
    first = values[..., :half]
    second = values[..., half:]
    return jnp.concatenate([first * cosine - second * sine, second * cosine + first * sine], axis=-1)

def adapt(values, down_product, upward):
    inner_product = low_back(low(matmul(values, down_product)))
    return matmul(inner_product, upward)

def reference(tokens, cotangent, prefix_length, sequence_adapter_index, gains, query_weight, key_weight, value_weight, output_weight, gate_weight, up_weight, down_weight, adapter_first_input, adapter_second_query, adapter_second_keyvalue, adapter_second_gate, adapter_first_output, adapter_first_down, adapter_second_output):
    widened_rows = lambda source_array: source_array.astype(jnp.float32)
    wq, wk, wv, wo, wg, wu, wd = [widened_rows(w) for w in (query_weight, key_weight, value_weight, output_weight, gate_weight, up_weight, down_weight)]
    groups = QUERY_HEADS // KEY_HEADS
    scale = HEAD_SIZE ** (-0.5)
    positions = jnp.arange(LEN).astype(jnp.float32)
    key_pos = jnp.arange(LEN, dtype=jnp.int32)

    def forward_layer(layer_inputs, adapter_update):
        first_input_factor, second_query_factor, second_keyvalue_factor, second_gate_factor, first_output_factor, first_down_factor, second_output_factor = adapter_update

        def sequence(item):
            xs, plen, aid = item
            picked = first_input_factor[:, aid]
            xn1 = low(rms_norm(xs, gains[0]))
            q_lin = low_back(matmul(xn1, wq) + adapt(xn1, picked[0], second_query_factor[aid]))
            k_lin = low_back(matmul(xn1, wk) + adapt(xn1, picked[1], second_keyvalue_factor[0, aid]))
            v_lin = low_back(matmul(xn1, wv) + adapt(xn1, picked[2], second_keyvalue_factor[1, aid]))
            q_att = low(rotate(q_lin.reshape(LEN, QUERY_HEADS, HEAD_SIZE), positions, 1.0) * scale)
            k_att = low(rotate(k_lin.reshape(LEN, KEY_HEADS, HEAD_SIZE), positions, 1.0))
            v_att = low(v_lin).reshape(LEN, KEY_HEADS, HEAD_SIZE)
            visible = (key_pos[None, :] <= key_pos[:, None]) | (key_pos[None, :] < plen)
            q_heads = q_att.reshape(LEN, KEY_HEADS, groups, HEAD_SIZE).transpose(1, 2, 0, 3)
            k_heads = k_att.transpose(1, 0, 2)
            v_heads = v_att.transpose(1, 0, 2)

            def attend(group):
                q_one, k_one, v_one = group
                raw = low_back(jnp.einsum('gqd,kd->gqk', q_one, k_one, precision=highest))
                capped = jnp.where(visible[None], soft_cap * jnp.tanh(raw / soft_cap), masked_low)
                probs = jax.nn.softmax(capped, axis=-1)
                return jnp.einsum('gqk,kd->gqd', low(probs), v_one, precision=highest)
            mixed = lax.map(jax.checkpoint(attend), (q_heads, k_heads, v_heads))
            o_b = low_back(low(mixed.transpose(2, 0, 1, 3).reshape(LEN, QUERY_HEADS * HEAD_SIZE)))
            y_att = low_back(matmul(o_b, wo) + adapt(o_b, first_output_factor[aid], second_output_factor[0, aid]))
            h_one = xs + rms_norm(y_att, gains[1])
            xn2 = low(rms_norm(h_one, gains[2]))
            gate = low_back(matmul(xn2, wg) + adapt(xn2, picked[3], second_gate_factor[0, aid]))
            upper = low_back(matmul(xn2, wu) + adapt(xn2, picked[4], second_gate_factor[1, aid]))
            act = low(jax.nn.gelu(gate, approximate=True) * upper)
            y_ffn = low_back(matmul(act, wd) + adapt(act, first_down_factor[aid], second_output_factor[1, aid]))
            return h_one + rms_norm(y_ffn, gains[3])
        return lax.map(jax.checkpoint(sequence), (layer_inputs, prefix_length, sequence_adapter_index))
    adapter_update = tuple((widened_rows(source_array) for source_array in (adapter_first_input, adapter_second_query, adapter_second_keyvalue, adapter_second_gate, adapter_first_output, adapter_first_down, adapter_second_output)))
    layer_result, gather_rows = jax.vjp(forward_layer, widened_rows(tokens), adapter_update)
    input_grad, grads = gather_rows(widened_rows(cotangent))
    return (layer_result.astype(jnp.bfloat16), input_grad, grads[0], grads[1], grads[2], grads[3], grads[4], grads[5], grads[6])
```

```python
import functools
import math

import jax
import jax.numpy as jnp
from jax import lax
from jax.experimental import pallas as pl
from jax.experimental.pallas import tpu as pltpu
from jax.sharding import PartitionSpec as P

QUERY_HEADS = 8
KEY_HEADS = 4
HEAD_SIZE = 256

epsilon = 1e-06
soft_cap = 50.0
masked_low = -1e30
MESH = pl.DeviceIdType.MESH
f32 = jnp.float32
bf16 = jnp.bfloat16


def rms_norm(values, gain):
    return values * lax.rsqrt(jnp.mean(values * values, axis=-1, keepdims=True) + epsilon) * gain


def norm_back(values, gain, incoming):
    scale = lax.rsqrt(jnp.mean(values * values, axis=-1, keepdims=True) + epsilon)
    unit = values * scale
    weighted = incoming * gain
    return scale * (weighted - unit * jnp.mean(weighted * unit, axis=-1, keepdims=True))


def rotate(values, cosine, sine):
    half = values.shape[-1] // 2
    first = values[..., :half]
    second = values[..., half:]
    return jnp.concatenate(
        [first * cosine - second * sine, second * cosine + first * sine], axis=-1
    )


def dot_nn(left, right):
    return lax.dot_general(left, right, (((1,), (0,)), ((), ())), preferred_element_type=f32)


def dot_nt(left, right):
    return lax.dot_general(left, right, (((1,), (1,)), ((), ())), preferred_element_type=f32)


def dot_tn(left, right):
    return lax.dot_general(left, right, (((0,), (0,)), ((), ())), preferred_element_type=f32)


def sum_kernel(count, width, chunks, slots, *refs):
    lefts = refs[:count]
    rights = refs[count : 2 * count]
    refs = refs[2 * count :]
    terms = None
    if slots:
        terms, out, every = refs[:3]
        refs = refs[3:]
    else:
        out = refs[0]
        refs = refs[1:]
    part, mine, got_a, got_b, a_send, a_recv, b_send, b_recv, c_send, c_recv = refs[:10]
    z = lax.axis_index("tp")
    inner = (z == 1) | (z == 2)
    outer = (z == 0) | (z == 3)
    pair = z + 1 - 2 * lax.rem(z, 2)
    across = 3 - z
    barrier = pltpu.get_barrier_semaphore()

    def greet(axis, peer):
        pl.semaphore_signal(barrier, inc=1, device_id={axis: peer}, device_id_type=MESH)

    others = 0
    if slots:
        at = lax.axis_index("ctx")
        core = lax.rem(at, 2)
        row = lax.div(at, 2)
        core_peer = at + 1 - 2 * core
        row_peer = at + 2 - 4 * row
        seq = lax.axis_index("fsdp")
        others = 2 + slots - 1
        greet("ctx", core_peer)
        greet("ctx", row_peer)
        for d in range(1, slots):
            greet("fsdp", lax.rem(seq + d, slots))
    greet("tp", pair)

    @pl.when(inner)
    def _():
        greet("tp", across)
        pl.semaphore_wait(barrier, others + 2)

    @pl.when(outer)
    def _():
        pl.semaphore_wait(barrier, others + 1)

    def cols(c):
        return pl.ds(pl.multiple_of(c * width, width), width)

    def remote(source, target, send, recv, axis, peer):
        return pltpu.make_async_remote_copy(
            source, target, send, recv, device_id={axis: peer}, device_id_type=MESH
        )

    def copy_a(c):
        return remote(mine.at[c], got_a.at[c], a_send.at[c], a_recv.at[c], "tp", pair)

    def copy_b(c):
        return remote(mine.at[c], got_b.at[c], b_send.at[c], b_recv.at[c], "tp", across)

    def copy_c(c):
        place = out.at[:, cols(c)]
        return remote(place, place, c_send.at[c], c_recv.at[c], "tp", pair)

    def finish(c):
        copy_b(c).wait_recv()
        out[:, cols(c)] = (mine[c].astype(f32) + got_b[c].astype(f32)).astype(bf16)
        copy_c(c).start()

    if slots:
        from_core, with_core, from_row, held, held_a, held_b, full, g_send, g_recv = refs[10:]
        summed = held_a.shape[0]
        rest = pl.ds(summed, full.shape[0] - summed)

        def core_copy(j):
            source = terms.at[2 * j + 1 - core]
            return remote(source, from_core.at[j], g_send.at[j], g_recv.at[j], "ctx", core_peer)

        def row_copy():
            source = with_core.at[1 - row]
            return remote(source, from_row, g_send.at[2], g_recv.at[2], "ctx", row_peer)

        def line_a():
            source = held.at[pl.ds(0, summed)]
            return remote(source, held_a, g_send.at[3], g_recv.at[3], "tp", pair)

        def line_b():
            source = held.at[pl.ds(0, summed)]
            return remote(source, held_b, g_send.at[4], g_recv.at[4], "tp", across)

        def line_c():
            place = full.at[pl.ds(0, summed)]
            return remote(place, place, g_send.at[5], g_recv.at[5], "tp", pair)

        def seq_copy(d):
            peer = lax.rem(seq + d, slots)
            return remote(
                full, every.at[seq, at], g_send.at[8 + d], g_recv.at[8 + d], "fsdp", peer
            )

        def row_back():
            place = every.at[:, at]
            return remote(place, place, g_send.at[6], g_recv.at[6], "ctx", row_peer)

        def core_back(j):
            place = every.at[:, 2 * j + core]
            return remote(place, place, g_send.at[7 + j], g_recv.at[7 + j], "ctx", core_peer)

        core_copy(0).start()
        core_copy(1).start()

        def reduce_terms(c):
            @pl.when(c == 1)
            def _():
                for j in range(2):
                    core_copy(j).wait_recv()
                    total = terms[2 * j + core].astype(f32) + from_core[j].astype(f32)
                    with_core[j] = total.astype(bf16)
                row_copy().start()

            @pl.when(c == 3)
            def _():
                row_copy().wait_recv()
                held[...] = (with_core[row].astype(f32) + from_row[...].astype(f32)).astype(bf16)
                full[rest, :] = held[rest, :]

            @pl.when((c == 3) & outer)
            def _():
                line_a().start()

            @pl.when((c == 6) & inner)
            def _():
                line_a().wait_recv()
                total = held[:summed].astype(f32) + held_a[...].astype(f32)
                held[:summed] = total.astype(bf16)
                line_b().start()

            @pl.when((c == 8) & inner)
            def _():
                line_b().wait_recv()
                total = held[:summed].astype(f32) + held_b[...].astype(f32)
                full[:summed] = total.astype(bf16)
                line_c().start()

            @pl.when((c == 11) & outer)
            def _():
                line_c().wait_recv()

            @pl.when(c == 11)
            def _():
                every[seq, at] = full[...]
                for d in range(1, slots):
                    seq_copy(d).start()

            @pl.when(c == 13)
            def _():
                for d in range(1, slots):
                    seq_copy(d).wait_recv()
                row_back().start()

            @pl.when(c == 15)
            def _():
                row_back().wait_recv()
                core_back(0).start()
                core_back(1).start()

    def body(c, carry):
        for i, (left, right) in enumerate(zip(lefts, rights)):
            for m in range(0, left.shape[0], 256):
                term = dot_nt(left[m : m + 256, :], right[cols(c), :])
                part[m : m + 256, :] = term if i == 0 else part[m : m + 256, :] + term

        @pl.when(outer)
        def _():
            mine[c] = part[...].astype(bf16)
            copy_a(c).start()

        @pl.when(inner)
        def _():
            copy_a(c).wait_recv()
            mine[c] = (part[...] + got_a[c].astype(f32)).astype(bf16)
            copy_b(c).start()

        @pl.when(inner & (c >= 1))
        def _():
            finish(c - 1)

        if slots:
            reduce_terms(c)
        return carry

    lax.fori_loop(0, chunks, body, 0)

    @pl.when(inner)
    def _():
        finish(chunks - 1)

        def drain(c, carry):
            copy_b(c).wait_send()
            copy_c(c).wait_send()
            return carry

        lax.fori_loop(0, chunks, drain, 0)

    @pl.when(outer)
    def _():
        def drain(c, carry):
            copy_a(c).wait_send()
            copy_c(c).wait_recv()
            return carry

        lax.fori_loop(0, chunks, drain, 0)

    if slots:
        for j in range(2):
            core_copy(j).wait_send()
            core_back(j).wait()
        row_copy().wait_send()
        row_back().wait_send()
        for d in range(1, slots):
            seq_copy(d).wait_send()

        @pl.when(outer)
        def _():
            line_a().wait_send()

        @pl.when(inner)
        def _():
            line_b().wait_send()
            line_c().wait_send()


def matmul_sum(lefts, rights, collective_id, width=128, terms=None, slots=0, summed=0):
    rows = lefts[0].shape[0]
    total = rights[0].shape[0]
    chunks = total // width
    flops = sum(2 * rows * total * left.shape[1] for left in lefts)
    moved = sum(left.size + right.size for left, right in zip(lefts, rights)) + rows * total
    scratch = (
        [pltpu.VMEM((rows, width), f32)]
        + [pltpu.VMEM((chunks, rows, width), bf16)] * 3
        + [pltpu.SemaphoreType.DMA((chunks,))] * 6
    )
    shapes = [jax.ShapeDtypeStruct((rows, total), bf16)]
    operands = [*lefts, *rights]
    if slots:
        assert chunks >= 17
        block = terms.shape[1:]
        lead = (summed, block[1])
        operands.append(terms)
        shapes.append(jax.ShapeDtypeStruct((slots, *terms.shape), bf16))
        scratch += [
            pltpu.VMEM((2, *block), bf16),
            pltpu.VMEM((2, *block), bf16),
            pltpu.VMEM(block, bf16),
            pltpu.VMEM(block, bf16),
            pltpu.VMEM(lead, bf16),
            pltpu.VMEM(lead, bf16),
            pltpu.VMEM(block, bf16),
            pltpu.SemaphoreType.DMA((9 + slots,)),
            pltpu.SemaphoreType.DMA((9 + slots,)),
        ]
    vmem = pl.BlockSpec(memory_space=pltpu.VMEM)
    result = pl.pallas_call(
        functools.partial(sum_kernel, len(lefts), width, chunks, slots),
        out_shape=shapes,
        in_specs=[vmem] * len(operands),
        out_specs=[vmem] * len(shapes),
        scratch_shapes=scratch,
        compiler_params=pltpu.CompilerParams(
            collective_id=collective_id, has_side_effects=True, vmem_limit_bytes=60 * 1024 * 1024
        ),
        cost_estimate=pl.CostEstimate(flops=flops, bytes_accessed=2 * moved, transcendentals=0),
        name=f"matmul_sum_{collective_id}",
    )(*operands)
    return result if slots else result[0]


def swap(values, step):
    return lax.ppermute(values, "ctx", [(i, i ^ step) for i in range(lax.axis_size("ctx"))])


def per_device(
    tokens,
    cotangent,
    prefix_length,
    sequence_adapter_index,
    gains,
    query_weight,
    key_weight,
    value_weight,
    output_weight,
    gate_weight,
    up_weight,
    down_weight,
    adapter_first_input,
    adapter_second_query,
    adapter_second_keyvalue,
    adapter_second_gate,
    adapter_first_output,
    adapter_first_down,
    adapter_second_output,
):
    seqs, rows, width = tokens.shape
    assert seqs == 1 and lax.axis_size("ctx") == 4 and lax.axis_size("tp") == 4
    groups = QUERY_HEADS // KEY_HEADS
    scale = HEAD_SIZE ** (-0.5)
    q_cols = query_weight.shape[1]
    k_cols = key_weight.shape[1]
    adapter_count, rank = adapter_second_query.shape[:2]
    both = ("fsdp", "ctx")
    adapter = sequence_adapter_index[0]

    def chosen(table, dim):
        return lax.dynamic_index_in_dim(table, adapter, dim, keepdims=False)

    attn_local = jnp.concatenate(
        [query_weight, key_weight, value_weight, output_weight.T], axis=1
    )
    attn_full = lax.all_gather(attn_local, both, axis=0, tiled=True)
    gate_full = lax.all_gather(gate_weight, both, axis=0, tiled=True)
    up_full = lax.all_gather(up_weight, both, axis=0, tiled=True)
    down_full = lax.all_gather(down_weight.T, both, axis=0, tiled=True)
    qkv_cols = q_cols + 2 * k_cols
    qkv_full = attn_full[:, :qkv_cols]
    out_full = attn_full[:, qkv_cols:]

    a_in = chosen(adapter_first_input, 1)
    b_query = chosen(adapter_second_query, 0)
    b_kv = chosen(adapter_second_keyvalue, 1)
    b_gate = chosen(adapter_second_gate, 1)
    a_out = chosen(adapter_first_output, 0)
    a_down = chosen(adapter_first_down, 0)
    b_out = chosen(adapter_second_output, 1)
    a_qkv = jnp.concatenate([a_in[0], a_in[1], a_in[2]], axis=1)
    a_gu = jnp.concatenate([a_in[3], a_in[4]], axis=1)

    ctx = lax.axis_index("ctx")
    query_pos = ctx * rows + jnp.arange(rows, dtype=jnp.int32)
    half = HEAD_SIZE // 2
    freqs = jnp.exp(jnp.arange(half, dtype=f32) * (-2.0 * math.log(10000.0) / HEAD_SIZE))
    angle = query_pos.astype(f32)[:, None] * freqs[None, :]
    cosine = jnp.cos(angle)[:, None, :]
    sine = jnp.sin(angle)[:, None, :]

    residual = tokens[0].astype(f32)
    d_final = cotangent[0].astype(f32)
    n1 = rms_norm(residual, gains[0]).astype(bf16)
    u_qkv = dot_nn(n1, a_qkv).astype(bf16)
    lin = dot_nn(n1, qkv_full)
    query = lin[:, :q_cols] + dot_nn(u_qkv[:, :rank], b_query)
    key = lin[:, q_cols : q_cols + k_cols] + dot_nn(u_qkv[:, rank : 2 * rank], b_kv[0])
    value = lin[:, q_cols + k_cols :] + dot_nn(u_qkv[:, 2 * rank :], b_kv[1])
    qa = (rotate(query.reshape(rows, -1, HEAD_SIZE), cosine, sine) * scale).astype(bf16)
    ka = rotate(key.reshape(rows, -1, HEAD_SIZE), cosine, sine).reshape(rows, -1).astype(bf16)
    va = value.astype(bf16)

    own = jnp.stack([ka, va])
    from_row = swap(own, 2)
    near = jnp.stack([own, from_row])
    far = swap(near, 1)
    blocks = jnp.concatenate([near, far])
    keys = blocks[:, 0].reshape(-1, HEAD_SIZE)
    values = blocks[:, 1].reshape(-1, HEAD_SIZE)
    block_of = jnp.stack([ctx, ctx ^ 2, ctx ^ 1, ctx ^ 3])
    key_pos = (block_of[:, None] * rows + jnp.arange(rows, dtype=jnp.int32)[None, :]).reshape(-1)
    visible = (key_pos[None, :] <= query_pos[:, None]) | (key_pos[None, :] < prefix_length[0])

    q_heads = qa.transpose(1, 0, 2)
    raw = jnp.einsum("gqd,kd->gqk", q_heads, keys, preferred_element_type=f32)
    capped = jnp.where(visible[None], soft_cap * jnp.tanh(raw / soft_cap), masked_low)
    top = jnp.max(capped, axis=-1, keepdims=True)
    expo = jnp.exp(capped - top)
    total = jnp.sum(expo, axis=-1, keepdims=True)
    probs = (expo / total).astype(bf16)
    mixed = jnp.einsum("gqk,kd->gqd", probs, values, preferred_element_type=f32)
    lse = top + jnp.log(total)
    ob = mixed.astype(bf16).transpose(1, 0, 2).reshape(rows, -1)

    u_out = dot_nn(ob, a_out).astype(bf16)
    y_att = matmul_sum([ob, u_out], [out_full, b_out[0].T], 1).astype(f32)
    h1 = residual + rms_norm(y_att, gains[1])
    n2 = rms_norm(h1, gains[2]).astype(bf16)
    u_gu = dot_nn(n2, a_gu).astype(bf16)
    gate = dot_nn(n2, gate_full) + dot_nn(u_gu[:, :rank], b_gate[0])
    upper = dot_nn(n2, up_full) + dot_nn(u_gu[:, rank:], b_gate[1])
    act = (jax.nn.gelu(gate, approximate=True) * upper).astype(bf16)
    u_down = dot_nn(act, a_down).astype(bf16)
    y_ffn = matmul_sum([act, u_down], [down_full, b_out[1].T], 2).astype(f32)
    final = (h1 + rms_norm(y_ffn, gains[3])).astype(bf16)

    e_ffn = norm_back(y_ffn, gains[3], d_final).astype(bf16)
    du_down = dot_nt(e_ffn, b_out[1]).astype(bf16)
    d_act = dot_nn(e_ffn, down_full) + dot_nt(du_down, a_down)
    _, gelu_pull = jax.vjp(lambda gin, uin: jax.nn.gelu(gin, approximate=True) * uin, gate, upper)
    d_gate, d_up = gelu_pull(d_act)
    d_gate = d_gate.astype(bf16)
    d_up = d_up.astype(bf16)
    du_gate = dot_nt(d_gate, b_gate[0]).astype(bf16)
    du_up = dot_nt(d_up, b_gate[1]).astype(bf16)
    du_gu = jnp.concatenate([du_gate, du_up], axis=1)
    dn2 = matmul_sum([d_gate, d_up, du_gu], [gate_full, up_full, a_gu], 3).astype(f32)
    dh1 = d_final + norm_back(h1, gains[2], dn2)
    e_att = norm_back(y_att, gains[1], dh1).astype(bf16)
    du_out = dot_nt(e_att, b_out[0]).astype(bf16)
    d_ob = (dot_nn(e_att, out_full) + dot_nt(du_out, a_out)).astype(bf16)
    d_mixed = d_ob.reshape(rows, -1, HEAD_SIZE).transpose(1, 0, 2)

    p_back = jnp.exp(capped - lse)
    d_probs = jnp.einsum("gqd,kd->gqk", d_mixed, values, preferred_element_type=f32)
    delta = jnp.sum(p_back * d_probs, axis=-1, keepdims=True)
    slope = 1.0 - jnp.square(jnp.tanh(raw / soft_cap))
    d_raw = (p_back * (d_probs - delta) * slope).astype(bf16)
    dqa = jnp.einsum("gqk,kd->gqd", d_raw, keys, preferred_element_type=f32)
    dka = jnp.einsum("gqk,gqd->kd", d_raw, q_heads, preferred_element_type=f32)
    dva = jnp.einsum(
        "gqk,gqd->kd", p_back.astype(bf16), d_mixed, preferred_element_type=f32
    )
    d_blocks = jnp.stack([dka, dva]).reshape(2, 4, rows, -1)
    got_far = swap(d_blocks[:, 2:].astype(bf16), 1)
    d_near = d_blocks[:, :2] + got_far.astype(f32)
    got_row = swap(d_near[:, 1].astype(bf16), 2)
    d_own = d_near[:, 0] + got_row.astype(f32)

    d_query = (rotate(dqa.transpose(1, 0, 2), cosine, -sine) * scale).reshape(rows, -1)
    d_key = rotate(d_own[0].reshape(rows, -1, HEAD_SIZE), cosine, -sine).reshape(rows, -1)
    d_query = d_query.astype(bf16)
    d_key = d_key.astype(bf16)
    d_value = d_own[1].astype(bf16)
    d_qkv = jnp.concatenate([d_query, d_key, d_value], axis=1)
    du_query = dot_nt(d_query, b_query).astype(bf16)
    du_key = dot_nt(d_key, b_kv[0]).astype(bf16)
    du_value = dot_nt(d_value, b_kv[1]).astype(bf16)
    du_qkv = jnp.concatenate([du_query, du_key, du_value], axis=1)

    wide = jnp.concatenate(
        [
            dot_tn(du_qkv, n1),
            dot_tn(du_gu, n2),
            dot_tn(u_out, e_att),
            dot_tn(u_down, e_ffn),
        ]
    )
    hidden = d_gate.shape[1]
    g_b_gate = dot_tn(u_gu[:, :rank], d_gate)
    g_b_up = dot_tn(u_gu[:, rank:], d_up)
    g_a_down = dot_tn(du_down, act)
    g_b_query = dot_tn(u_qkv[:, :rank], d_query)
    g_b_key = dot_tn(u_qkv[:, rank : 2 * rank], d_key)
    g_b_value = dot_tn(u_qkv[:, 2 * rank :], d_value)
    g_a_out = dot_tn(du_out, ob)
    small = jnp.concatenate([g_b_query, g_b_key, g_b_value, g_a_out], axis=1)
    small = jnp.pad(small, ((0, 0), (0, hidden - small.shape[1])))
    split = jnp.concatenate([g_b_gate, g_b_up, g_a_down, small])

    slots = lax.axis_size("fsdp")
    first = ((ctx == 0) & (lax.axis_index("tp") == 0)).astype(f32)
    note = jnp.full((1, width), adapter.astype(f32) * first)
    wide = jnp.pad(jnp.concatenate([wide, note]), ((0, 8 * rank - wide.shape[0] - 1), (0, 0)))
    terms = jnp.concatenate(
        [wide.reshape(4, 2 * rank, width), split.reshape(4, rank, width)], axis=1
    ).astype(bf16)
    dn1, every = matmul_sum(
        [d_qkv, du_qkv], [qkv_full, a_qkv], 4, terms=terms, slots=slots, summed=2 * rank
    )
    dn1 = dn1.astype(f32)
    input_grad = dh1 + norm_back(residual, gains[0], dn1)

    wide_all = every[:, :, : 2 * rank].astype(f32).reshape(slots, 8 * rank, width)
    split_all = every[:, :, 2 * rank :].astype(f32).reshape(slots, 4 * rank, width)
    used = wide_all[:, 7 * rank, 0].astype(jnp.int32)
    select = (used[:, None] == jnp.arange(adapter_count, dtype=jnp.int32)[None, :]).astype(f32)

    def to_adapters(terms):
        return jnp.sum(select[:, :, None, None] * terms[:, None], axis=0)

    share = width // (slots * lax.axis_size("ctx"))
    start = (lax.axis_index("fsdp") * lax.axis_size("ctx") + ctx) * share
    wide_own = to_adapters(lax.dynamic_slice_in_dim(wide_all, start, share, axis=2))
    wide_own = wide_own[:, : 7 * rank].reshape(adapter_count, 7, rank, share)
    split_own = to_adapters(split_all).reshape(adapter_count, 4, rank, hidden)
    grad_a_in = wide_own[:, :5].transpose(1, 0, 3, 2)
    grad_b_out = wide_own[:, 5:].transpose(1, 0, 2, 3)
    small_own = split_own[:, 3]
    grad_b_query = small_own[:, :, :q_cols]
    grad_b_kv = jnp.stack(
        [small_own[:, :, q_cols : q_cols + k_cols], small_own[:, :, q_cols + k_cols : qkv_cols]]
    )
    grad_a_out = small_own[:, :, qkv_cols : qkv_cols + q_cols].transpose(0, 2, 1)
    grad_b_gate_up = split_own[:, :2].transpose(1, 0, 2, 3)
    grad_a_down = split_own[:, 2].transpose(0, 2, 1)
    return (
        final[None],
        input_grad[None],
        grad_a_in,
        grad_b_query,
        grad_b_kv,
        grad_b_gate_up,
        grad_a_out,
        grad_a_down,
        grad_b_out,
    )


def solution(mesh):
    both = ("fsdp", "ctx")
    in_specs = (
        P("fsdp", "ctx", None),
        P("fsdp", "ctx", None),
        P("fsdp"),
        P("fsdp"),
        P(),
        P(both, "tp"),
        P(both, "tp"),
        P(both, "tp"),
        P("tp", both),
        P(both, "tp"),
        P(both, "tp"),
        P("tp", both),
        P(),
        P(None, None, "tp"),
        P(None, None, None, "tp"),
        P(None, None, None, "tp"),
        P(None, "tp", None),
        P(None, "tp", None),
        P(),
    )
    out_specs = (
        P("fsdp", "ctx", None),
        P("fsdp", "ctx", None),
        P(None, None, both, None),
        P(None, None, "tp"),
        P(None, None, None, "tp"),
        P(None, None, None, "tp"),
        P(None, "tp", None),
        P(None, "tp", None),
        P(None, None, None, both),
    )
    return jax.shard_map(
        per_device, mesh=mesh, in_specs=in_specs, out_specs=out_specs, check_vma=False
    )
```

```python
import functools
import math

import jax
import jax.numpy as jnp
from jax import lax
from jax.experimental import pallas as pl
from jax.experimental.pallas import tpu as pltpu
from jax.sharding import PartitionSpec as P

QUERY_HEADS = 8
KEY_HEADS = 4
HEAD_SIZE = 256

epsilon = 1e-06
soft_cap = 50.0
masked_low = -1e30
MESH = pl.DeviceIdType.MESH
f32 = jnp.float32
bf16 = jnp.bfloat16


def rms_norm(values, gain):
    return values * lax.rsqrt(jnp.mean(values * values, axis=-1, keepdims=True) + epsilon) * gain


def norm_back(values, gain, incoming):
    scale = lax.rsqrt(jnp.mean(values * values, axis=-1, keepdims=True) + epsilon)
    unit = values * scale
    weighted = incoming * gain
    return scale * (weighted - unit * jnp.mean(weighted * unit, axis=-1, keepdims=True))


def rotate(values, cosine, sine):
    half = values.shape[-1] // 2
    first = values[..., :half]
    second = values[..., half:]
    return jnp.concatenate(
        [first * cosine - second * sine, second * cosine + first * sine], axis=-1
    )


def dot_nn(left, right):
    return lax.dot_general(left, right, (((1,), (0,)), ((), ())), preferred_element_type=f32)


def dot_nt(left, right):
    return lax.dot_general(left, right, (((1,), (1,)), ((), ())), preferred_element_type=f32)


def dot_tn(left, right):
    return lax.dot_general(left, right, (((0,), (0,)), ((), ())), preferred_element_type=f32)


def sum_kernel(count, width, chunks, slots, *refs):
    lefts = refs[:count]
    rights = refs[count : 2 * count]
    refs = refs[2 * count :]
    terms = None
    if slots:
        terms, out, every = refs[:3]
        refs = refs[3:]
    else:
        out = refs[0]
        refs = refs[1:]
    part, mine, got_a, got_b, a_send, a_recv, b_send, b_recv, c_send, c_recv = refs[:10]
    z = lax.axis_index("tp")
    inner = (z == 1) | (z == 2)
    outer = (z == 0) | (z == 3)
    pair = z + 1 - 2 * lax.rem(z, 2)
    across = 3 - z
    barrier = pltpu.get_barrier_semaphore()

    def greet(axis, peer):
        pl.semaphore_signal(barrier, inc=1, device_id={axis: peer}, device_id_type=MESH)

    others = 0
    if slots:
        at = lax.axis_index("ctx")
        core = lax.rem(at, 2)
        row = lax.div(at, 2)
        core_peer = at + 1 - 2 * core
        row_peer = at + 2 - 4 * row
        seq = lax.axis_index("fsdp")
        others = 2 + slots - 1
        greet("ctx", core_peer)
        greet("ctx", row_peer)
        for d in range(1, slots):
            greet("fsdp", lax.rem(seq + d, slots))
    greet("tp", pair)

    @pl.when(inner)
    def _():
        greet("tp", across)
        pl.semaphore_wait(barrier, others + 2)

    @pl.when(outer)
    def _():
        pl.semaphore_wait(barrier, others + 1)

    def cols(c):
        return pl.ds(pl.multiple_of(c * width, width), width)

    def remote(source, target, send, recv, axis, peer):
        return pltpu.make_async_remote_copy(
            source, target, send, recv, device_id={axis: peer}, device_id_type=MESH
        )

    def copy_a(c):
        return remote(mine.at[c], got_a.at[c], a_send.at[c], a_recv.at[c], "tp", pair)

    def copy_b(c):
        return remote(mine.at[c], got_b.at[c], b_send.at[c], b_recv.at[c], "tp", across)

    def copy_c(c):
        place = out.at[:, cols(c)]
        return remote(place, place, c_send.at[c], c_recv.at[c], "tp", pair)

    def finish(c):
        copy_b(c).wait_recv()
        out[:, cols(c)] = (mine[c].astype(f32) + got_b[c].astype(f32)).astype(bf16)
        copy_c(c).start()

    if slots:
        from_core, with_core, from_row, held, held_a, held_b, full, g_send, g_recv = refs[10:]
        summed = held_a.shape[0]
        rest = pl.ds(summed, full.shape[0] - summed)

        def core_copy(j):
            source = terms.at[2 * j + 1 - core]
            return remote(source, from_core.at[j], g_send.at[j], g_recv.at[j], "ctx", core_peer)

        def row_copy():
            source = with_core.at[1 - row]
            return remote(source, from_row, g_send.at[2], g_recv.at[2], "ctx", row_peer)

        def line_a():
            source = held.at[pl.ds(0, summed)]
            return remote(source, held_a, g_send.at[3], g_recv.at[3], "tp", pair)

        def line_b():
            source = held.at[pl.ds(0, summed)]
            return remote(source, held_b, g_send.at[4], g_recv.at[4], "tp", across)

        def line_c():
            place = full.at[pl.ds(0, summed)]
            return remote(place, place, g_send.at[5], g_recv.at[5], "tp", pair)

        def seq_copy(d):
            peer = lax.rem(seq + d, slots)
            return remote(
                full, every.at[seq, at], g_send.at[8 + d], g_recv.at[8 + d], "fsdp", peer
            )

        def row_back():
            place = every.at[:, at]
            return remote(place, place, g_send.at[6], g_recv.at[6], "ctx", row_peer)

        def core_back(j):
            place = every.at[:, 2 * j + core]
            return remote(place, place, g_send.at[7 + j], g_recv.at[7 + j], "ctx", core_peer)

        core_copy(0).start()
        core_copy(1).start()

        def reduce_terms(c):
            @pl.when(c == 1)
            def _():
                for j in range(2):
                    core_copy(j).wait_recv()
                    total = terms[2 * j + core].astype(f32) + from_core[j].astype(f32)
                    with_core[j] = total.astype(bf16)
                row_copy().start()

            @pl.when(c == 3)
            def _():
                row_copy().wait_recv()
                held[...] = (with_core[row].astype(f32) + from_row[...].astype(f32)).astype(bf16)
                full[rest, :] = held[rest, :]

            @pl.when((c == 3) & outer)
            def _():
                line_a().start()

            @pl.when((c == 6) & inner)
            def _():
                line_a().wait_recv()
                total = held[:summed].astype(f32) + held_a[...].astype(f32)
                held[:summed] = total.astype(bf16)
                line_b().start()

            @pl.when((c == 8) & inner)
            def _():
                line_b().wait_recv()
                total = held[:summed].astype(f32) + held_b[...].astype(f32)
                full[:summed] = total.astype(bf16)
                line_c().start()

            @pl.when((c == 11) & outer)
            def _():
                line_c().wait_recv()

            @pl.when(c == 11)
            def _():
                every[seq, at] = full[...]
                for d in range(1, slots):
                    seq_copy(d).start()

            @pl.when(c == 13)
            def _():
                for d in range(1, slots):
                    seq_copy(d).wait_recv()
                row_back().start()

            @pl.when(c == 15)
            def _():
                row_back().wait_recv()
                core_back(0).start()
                core_back(1).start()

    def body(c, carry):
        for i, (left, right) in enumerate(zip(lefts, rights)):
            for m in range(0, left.shape[0], 256):
                term = dot_nt(left[m : m + 256, :], right[cols(c), :])
                part[m : m + 256, :] = term if i == 0 else part[m : m + 256, :] + term

        @pl.when(outer)
        def _():
            mine[c] = part[...].astype(bf16)
            copy_a(c).start()

        @pl.when(inner)
        def _():
            copy_a(c).wait_recv()
            mine[c] = (part[...] + got_a[c].astype(f32)).astype(bf16)
            copy_b(c).start()

        @pl.when(inner & (c >= 1))
        def _():
            finish(c - 1)

        if slots:
            reduce_terms(c)
        return carry

    lax.fori_loop(0, chunks, body, 0)

    @pl.when(inner)
    def _():
        finish(chunks - 1)

        def drain(c, carry):
            copy_b(c).wait_send()
            copy_c(c).wait_send()
            return carry

        lax.fori_loop(0, chunks, drain, 0)

    @pl.when(outer)
    def _():
        def drain(c, carry):
            copy_a(c).wait_send()
            copy_c(c).wait_recv()
            return carry

        lax.fori_loop(0, chunks, drain, 0)

    if slots:
        for j in range(2):
            core_copy(j).wait_send()
            core_back(j).wait()
        row_copy().wait_send()
        row_back().wait_send()
        for d in range(1, slots):
            seq_copy(d).wait_send()

        @pl.when(outer)
        def _():
            line_a().wait_send()

        @pl.when(inner)
        def _():
            line_b().wait_send()
            line_c().wait_send()


def matmul_sum(lefts, rights, collective_id, width=128, terms=None, slots=0, summed=0):
    rows = lefts[0].shape[0]
    total = rights[0].shape[0]
    chunks = total // width
    flops = sum(2 * rows * total * left.shape[1] for left in lefts)
    moved = sum(left.size + right.size for left, right in zip(lefts, rights)) + rows * total
    scratch = (
        [pltpu.VMEM((rows, width), f32)]
        + [pltpu.VMEM((chunks, rows, width), bf16)] * 3
        + [pltpu.SemaphoreType.DMA((chunks,))] * 6
    )
    shapes = [jax.ShapeDtypeStruct((rows, total), bf16)]
    operands = [*lefts, *rights]
    if slots:
        assert chunks >= 17
        block = terms.shape[1:]
        lead = (summed, block[1])
        operands.append(terms)
        shapes.append(jax.ShapeDtypeStruct((slots, *terms.shape), bf16))
        scratch += [
            pltpu.VMEM((2, *block), bf16),
            pltpu.VMEM((2, *block), bf16),
            pltpu.VMEM(block, bf16),
            pltpu.VMEM(block, bf16),
            pltpu.VMEM(lead, bf16),
            pltpu.VMEM(lead, bf16),
            pltpu.VMEM(block, bf16),
            pltpu.SemaphoreType.DMA((9 + slots,)),
            pltpu.SemaphoreType.DMA((9 + slots,)),
        ]
    vmem = pl.BlockSpec(memory_space=pltpu.VMEM)
    result = pl.pallas_call(
        functools.partial(sum_kernel, len(lefts), width, chunks, slots),
        out_shape=shapes,
        in_specs=[vmem] * len(operands),
        out_specs=[vmem] * len(shapes),
        scratch_shapes=scratch,
        compiler_params=pltpu.CompilerParams(
            collective_id=collective_id, has_side_effects=True, vmem_limit_bytes=60 * 1024 * 1024
        ),
        cost_estimate=pl.CostEstimate(flops=flops, bytes_accessed=2 * moved, transcendentals=0),
        name=f"matmul_sum_{collective_id}",
    )(*operands)
    return result if slots else result[0]


def ffn_kernel(
    n2_all,
    cot_all,
    u_gu,
    gain,
    b_gate,
    a_down,
    b_down,
    a_gu,
    gate_all,
    up_all,
    down_all,
    y_all,
    dn2_all,
    act_all,
    e_all,
    dg_all,
    du_all,
    w_gate,
    w_up,
    w_down,
    n2_buf,
    cot_buf,
    act_buf,
    e_buf,
    dg_buf,
    du_buf,
    keep_up,
    keep_gate,
    part,
    mine,
    got_a,
    got_b,
    total,
    load_sem,
    in_sem,
    out_sem,
    a_send,
    a_recv,
    b_send,
    b_recv,
    c_send,
    c_recv,
):
    n, rows, width = n2_all.shape
    ring = mine.shape[0]
    rank = b_down.shape[0]
    tile = width // 3
    z = lax.axis_index("tp")
    inner = (z == 1) | (z == 2)
    outer = (z == 0) | (z == 3)
    pair = z + 1 - 2 * lax.rem(z, 2)
    across = 3 - z

    weights = [
        pltpu.make_async_copy(source, target, load_sem.at[i])
        for i, (source, target) in enumerate(
            ((gate_all, w_gate), (up_all, w_up), (down_all, w_down))
        )
    ]

    def n2_copy(c):
        return pltpu.make_async_copy(n2_all.at[c], n2_buf.at[lax.rem(c, 2)], in_sem.at[lax.rem(c, 2)])

    def cot_copy(c):
        slot = lax.rem(c, 2)
        return pltpu.make_async_copy(cot_all.at[c], cot_buf.at[slot], in_sem.at[2 + slot])

    n2_copy(0).start()
    for copy in weights:
        copy.start()
    n2_copy(1).start()
    cot_copy(0).start()
    cot_copy(1).start()

    barrier = pltpu.get_barrier_semaphore()
    pl.semaphore_signal(barrier, inc=1, device_id={"tp": pair}, device_id_type=MESH)

    @pl.when(inner)
    def _():
        pl.semaphore_signal(barrier, inc=1, device_id={"tp": across}, device_id_type=MESH)
        pl.semaphore_wait(barrier, 2)

    @pl.when(outer)
    def _():
        pl.semaphore_wait(barrier, 1)

    def remote(source, target, send, recv, peer):
        return pltpu.make_async_remote_copy(
            source, target, send, recv, device_id={"tp": peer}, device_id_type=MESH
        )

    def copy_a(k):
        slot = lax.rem(k, ring)
        return remote(mine.at[slot], got_a.at[slot], a_send.at[k], a_recv.at[k], pair)

    def copy_b(k):
        slot = lax.rem(k, ring)
        return remote(mine.at[slot], got_b.at[slot], b_send.at[k], b_recv.at[k], across)

    def copy_c(k):
        place = total.at[lax.rem(k, n)]
        return remote(place, place, c_send.at[k], c_recv.at[k], pair)

    def finish(k):
        slot = lax.rem(k, ring)
        copy_b(k).wait_recv()
        total[lax.rem(k, n)] = (mine[slot].astype(f32) + got_b[slot].astype(f32)).astype(bf16)
        copy_c(k).start()

    def exchange(k):
        slot = lax.rem(k, ring)

        @pl.when(outer & (k >= ring))
        def _():
            copy_c(k - ring).wait_recv()
            copy_a(k - ring).wait_send()

        @pl.when(outer)
        def _():
            mine[slot] = part[...].astype(bf16)
            copy_a(k).start()

        @pl.when(inner & (k >= ring))
        def _():
            copy_b(k - ring).wait_send()

        @pl.when(inner)
        def _():
            copy_a(k).wait_recv()
            mine[slot] = (part[...] + got_a[slot].astype(f32)).astype(bf16)
            copy_b(k).start()

        @pl.when(inner & (k >= n + 1))
        def _():
            copy_c(k - 1 - n).wait_send()

        @pl.when(inner & (k >= 1))
        def _():
            finish(k - 1)

    def put(i, buf, target, c):
        return pltpu.make_async_copy(buf, target.at[c], out_sem.at[i])

    def act_out(c):
        return put(0, act_buf, act_all, c)

    def forward(k, carry):
        n2_copy(k).wait()

        @pl.when(k == 0)
        def _():
            weights[0].wait()
            weights[1].wait()

        @pl.when(k >= 1)
        def _():
            act_out(k - 1).wait()

        slot = lax.rem(k, 2)
        u_here = u_gu[k]
        for i in range(3):
            cols = slice(i * tile, (i + 1) * tile)
            gate = dot_nn(n2_buf[slot], w_gate[:, cols]) + dot_nn(u_here[:, :rank], b_gate[0, :, cols])
            upper = dot_nn(n2_buf[slot], w_up[:, cols]) + dot_nn(u_here[:, rank:], b_gate[1, :, cols])
            square = gate * gate
            slant = math.sqrt(2.0 / math.pi)
            bend = jnp.tanh(slant * (gate + 0.044715 * (square * gate)))
            side = 0.5 * (1.0 + bend)
            curve = gate * side
            rise = side + 0.5 * gate * (1.0 - bend * bend) * (
                slant * (1.0 + 3.0 * 0.044715 * square)
            )
            act_buf[:, cols] = (curve * upper).astype(bf16)
            keep_up[k, :, cols] = curve.astype(bf16)
            keep_gate[k, :, cols] = (rise * upper).astype(bf16)

        @pl.when(k + 2 < n)
        def _():
            n2_copy(k + 2).start()

        act_out(k).start()

        @pl.when(k == 0)
        def _():
            weights[2].wait()

        u_down = dot_nt(act_buf[...], a_down[...]).astype(bf16)
        for i in range(3):
            cols = slice(i * tile, (i + 1) * tile)
            part[:, cols] = dot_nt(act_buf[...], w_down[cols, :]) + dot_nn(u_down, b_down[:, cols])
        exchange(k)
        return carry

    def back_out(i, c):
        if i == 0:
            return put(1, e_buf, e_all, c)
        if i == 1:
            return put(2, dg_buf, dg_all, c)
        if i == 2:
            return put(3, du_buf, du_all, c)
        return put(4, total.at[c], y_all, c)

    def backward(c, carry):
        cot_copy(c).wait()
        back_out(3, c).start()

        @pl.when(c >= 1)
        def _():
            for i in range(3):
                back_out(i, c - 1).wait()

        slot = lax.rem(c, 2)

        def norm(i, inside):
            lines = pl.ds(pl.multiple_of(i * 16, 16), 16)
            values = total[c, lines, :].astype(f32)
            scale = lax.rsqrt(jnp.mean(values * values, axis=-1, keepdims=True) + epsilon)
            unit = values * scale
            weighted = cot_buf[slot, lines, :].astype(f32) * gain[...]
            e_buf[lines, :] = (
                scale * (weighted - unit * jnp.mean(weighted * unit, axis=-1, keepdims=True))
            ).astype(bf16)
            return inside

        lax.fori_loop(0, rows // 16, norm, 0)

        @pl.when(c + 2 < n)
        def _():
            cot_copy(c + 2).start()

        back_out(0, c).start()
        du_down = dot_nt(e_buf[...], b_down[...]).astype(bf16)
        for i in range(3):
            cols = slice(i * tile, (i + 1) * tile)
            d_act = dot_nn(e_buf[...], w_down[:, cols]) + dot_nn(du_down, a_down[:, cols])
            dg_buf[:, cols] = (d_act * keep_gate[c, :, cols].astype(f32)).astype(bf16)
            du_buf[:, cols] = (d_act * keep_up[c, :, cols].astype(f32)).astype(bf16)
        back_out(1, c).start()
        back_out(2, c).start()
        du_gate = dot_nt(dg_buf[...], b_gate[0]).astype(bf16)
        du_up = dot_nt(du_buf[...], b_gate[1]).astype(bf16)
        for i in range(3):
            cols = slice(i * tile, (i + 1) * tile)
            part[:, cols] = (
                dot_nt(dg_buf[...], w_gate[cols, :])
                + dot_nt(du_buf[...], w_up[cols, :])
                + dot_nn(du_gate, a_gu[0, :, cols])
                + dot_nn(du_up, a_gu[1, :, cols])
            )
        back_out(3, c).wait()
        exchange(n + c)
        return carry

    def result(c):
        return pltpu.make_async_copy(total.at[c], dn2_all.at[c], out_sem.at[5 + c])

    lax.fori_loop(0, n, forward, 0)
    lax.fori_loop(0, n, backward, 0)
    act_out(n - 1).wait()
    for i in range(3):
        back_out(i, n - 1).wait()

    @pl.when(inner)
    def _():
        copy_c(n - 1).wait_send()
        finish(2 * n - 1)

        def drain(k, carry):
            copy_b(k).wait_send()
            return carry

        lax.fori_loop(2 * n - ring, 2 * n, drain, 0)

        def drain_c(k, carry):
            copy_c(k).wait_send()
            return carry

        lax.fori_loop(n, 2 * n, drain_c, 0)

    @pl.when(outer)
    def _():
        def drain(k, carry):
            copy_c(k).wait_recv()
            copy_a(k).wait_send()
            return carry

        lax.fori_loop(2 * n - ring, 2 * n, drain, 0)

    for c in range(n):
        result(c).start()
    for c in range(n):
        result(c).wait()


def feed_forward(
    n2, cot, u_gu, gain, b_gate, a_down, b_down, a_gu, gate_full, up_full, down_full, collective_id
):
    rows, width = n2.shape
    hidden = gate_full.shape[1]
    assert hidden == width
    step = 128
    n = rows // step
    ring = 4
    full = jax.ShapeDtypeStruct((n, step, width), bf16)
    vmem = pl.BlockSpec(memory_space=pltpu.VMEM)
    anywhere = pl.BlockSpec(memory_space=pl.ANY)
    block = pltpu.VMEM((step, width), bf16)
    results = pl.pallas_call(
        ffn_kernel,
        out_shape=[full] * 6,
        in_specs=[anywhere] * 2 + [vmem] * 6 + [anywhere] * 3,
        out_specs=[anywhere] * 6,
        scratch_shapes=[pltpu.VMEM((width, width), bf16)] * 3
        + [pltpu.VMEM((2, step, width), bf16)] * 2
        + [block] * 4
        + [pltpu.VMEM((n, step, width), bf16)] * 2
        + [pltpu.VMEM((step, width), f32)]
        + [pltpu.VMEM((ring, step, width), bf16)] * 3
        + [pltpu.VMEM((n, step, width), bf16)]
        + [
            pltpu.SemaphoreType.DMA((3,)),
            pltpu.SemaphoreType.DMA((4,)),
            pltpu.SemaphoreType.DMA((5 + n,)),
        ]
        + [pltpu.SemaphoreType.DMA((2 * n,))] * 6,
        compiler_params=pltpu.CompilerParams(
            collective_id=collective_id, has_side_effects=True, vmem_limit_bytes=67043328
        ),
        cost_estimate=pl.CostEstimate(
            flops=12 * rows * width * hidden, bytes_accessed=60 * 2**20, transcendentals=rows * hidden
        ),
        name=f"feed_forward_{collective_id}",
    )(
        n2.reshape(n, step, width),
        cot.reshape(n, step, width),
        u_gu.reshape(n, step, -1),
        gain,
        b_gate,
        a_down,
        b_down,
        a_gu,
        gate_full,
        up_full,
        down_full,
    )
    return [value.reshape(rows, width) for value in results]


def swap(values, step):
    return lax.ppermute(values, "ctx", [(i, i ^ step) for i in range(lax.axis_size("ctx"))])


def per_device(
    tokens,
    cotangent,
    prefix_length,
    sequence_adapter_index,
    gains,
    query_weight,
    key_weight,
    value_weight,
    output_weight,
    gate_weight,
    up_weight,
    down_weight,
    adapter_first_input,
    adapter_second_query,
    adapter_second_keyvalue,
    adapter_second_gate,
    adapter_first_output,
    adapter_first_down,
    adapter_second_output,
):
    seqs, rows, width = tokens.shape
    assert seqs == 1 and lax.axis_size("ctx") == 4 and lax.axis_size("tp") == 4
    groups = QUERY_HEADS // KEY_HEADS
    scale = HEAD_SIZE ** (-0.5)
    q_cols = query_weight.shape[1]
    k_cols = key_weight.shape[1]
    adapter_count, rank = adapter_second_query.shape[:2]
    both = ("fsdp", "ctx")
    adapter = sequence_adapter_index[0]

    def chosen(table, dim):
        return lax.dynamic_index_in_dim(table, adapter, dim, keepdims=False)

    attn_local = jnp.concatenate(
        [query_weight, key_weight, value_weight, output_weight.T], axis=1
    )
    attn_full = lax.all_gather(attn_local, both, axis=0, tiled=True)
    gate_full = lax.all_gather(gate_weight, both, axis=0, tiled=True)
    up_full = lax.all_gather(up_weight, both, axis=0, tiled=True)
    down_full = lax.all_gather(down_weight.T, both, axis=0, tiled=True)
    qkv_cols = q_cols + 2 * k_cols
    qkv_full = attn_full[:, :qkv_cols]
    out_full = attn_full[:, qkv_cols:]

    a_in = chosen(adapter_first_input, 1)
    b_query = chosen(adapter_second_query, 0)
    b_kv = chosen(adapter_second_keyvalue, 1)
    b_gate = chosen(adapter_second_gate, 1)
    a_out = chosen(adapter_first_output, 0)
    a_down = chosen(adapter_first_down, 0)
    b_out = chosen(adapter_second_output, 1)
    a_qkv = jnp.concatenate([a_in[0], a_in[1], a_in[2]], axis=1)
    a_gu = jnp.concatenate([a_in[3], a_in[4]], axis=1)

    ctx = lax.axis_index("ctx")
    query_pos = ctx * rows + jnp.arange(rows, dtype=jnp.int32)
    half = HEAD_SIZE // 2
    freqs = jnp.exp(jnp.arange(half, dtype=f32) * (-2.0 * math.log(10000.0) / HEAD_SIZE))
    angle = query_pos.astype(f32)[:, None] * freqs[None, :]
    cosine = jnp.cos(angle)[:, None, :]
    sine = jnp.sin(angle)[:, None, :]

    residual = tokens[0].astype(f32)
    d_final = cotangent[0].astype(f32)
    n1 = rms_norm(residual, gains[0]).astype(bf16)
    u_qkv = dot_nn(n1, a_qkv).astype(bf16)
    lin = dot_nn(n1, qkv_full)
    query = lin[:, :q_cols] + dot_nn(u_qkv[:, :rank], b_query)
    key = lin[:, q_cols : q_cols + k_cols] + dot_nn(u_qkv[:, rank : 2 * rank], b_kv[0])
    value = lin[:, q_cols + k_cols :] + dot_nn(u_qkv[:, 2 * rank :], b_kv[1])
    qa = (rotate(query.reshape(rows, -1, HEAD_SIZE), cosine, sine) * scale).astype(bf16)
    ka = rotate(key.reshape(rows, -1, HEAD_SIZE), cosine, sine).reshape(rows, -1).astype(bf16)
    va = value.astype(bf16)

    own = jnp.stack([ka, va])
    from_row = swap(own, 2)
    near = jnp.stack([own, from_row])
    far = swap(near, 1)
    blocks = jnp.concatenate([near, far])
    keys = blocks[:, 0].reshape(-1, HEAD_SIZE)
    values = blocks[:, 1].reshape(-1, HEAD_SIZE)
    block_of = jnp.stack([ctx, ctx ^ 2, ctx ^ 1, ctx ^ 3])
    key_pos = (block_of[:, None] * rows + jnp.arange(rows, dtype=jnp.int32)[None, :]).reshape(-1)
    visible = (key_pos[None, :] <= query_pos[:, None]) | (key_pos[None, :] < prefix_length[0])

    q_heads = qa.transpose(1, 0, 2)
    raw = jnp.einsum("gqd,kd->gqk", q_heads, keys, preferred_element_type=f32)
    capped = jnp.where(visible[None], soft_cap * jnp.tanh(raw / soft_cap), masked_low)
    top = jnp.max(capped, axis=-1, keepdims=True)
    expo = jnp.exp(capped - top)
    total = jnp.sum(expo, axis=-1, keepdims=True)
    probs = (expo / total).astype(bf16)
    mixed = jnp.einsum("gqk,kd->gqd", probs, values, preferred_element_type=f32)
    lse = top + jnp.log(total)
    ob = mixed.astype(bf16).transpose(1, 0, 2).reshape(rows, -1)

    u_out = dot_nn(ob, a_out).astype(bf16)
    y_att = matmul_sum([ob, u_out], [out_full, b_out[0].T], 1).astype(f32)
    h1 = residual + rms_norm(y_att, gains[1])
    n2 = rms_norm(h1, gains[2]).astype(bf16)
    u_gu = dot_nn(n2, a_gu).astype(bf16)
    y_ffn, dn2, act, e_ffn, d_gate, d_up = feed_forward(
        n2,
        cotangent[0],
        u_gu,
        gains[3][None],
        b_gate,
        a_down.T,
        b_out[1],
        jnp.stack([a_in[3].T, a_in[4].T]),
        gate_full,
        up_full,
        down_full,
        2,
    )
    y_ffn = y_ffn.astype(f32)
    dn2 = dn2.astype(f32)
    final = (h1 + rms_norm(y_ffn, gains[3])).astype(bf16)
    u_down = dot_nn(act, a_down).astype(bf16)
    du_down = dot_nt(e_ffn, b_out[1]).astype(bf16)
    du_gate = dot_nt(d_gate, b_gate[0]).astype(bf16)
    du_up = dot_nt(d_up, b_gate[1]).astype(bf16)
    du_gu = jnp.concatenate([du_gate, du_up], axis=1)
    dh1 = d_final + norm_back(h1, gains[2], dn2)
    e_att = norm_back(y_att, gains[1], dh1).astype(bf16)
    du_out = dot_nt(e_att, b_out[0]).astype(bf16)
    d_ob = (dot_nn(e_att, out_full) + dot_nt(du_out, a_out)).astype(bf16)
    d_mixed = d_ob.reshape(rows, -1, HEAD_SIZE).transpose(1, 0, 2)

    p_back = jnp.exp(capped - lse)
    d_probs = jnp.einsum("gqd,kd->gqk", d_mixed, values, preferred_element_type=f32)
    delta = jnp.sum(p_back * d_probs, axis=-1, keepdims=True)
    slope = 1.0 - jnp.square(jnp.tanh(raw / soft_cap))
    d_raw = (p_back * (d_probs - delta) * slope).astype(bf16)
    dqa = jnp.einsum("gqk,kd->gqd", d_raw, keys, preferred_element_type=f32)
    dka = jnp.einsum("gqk,gqd->kd", d_raw, q_heads, preferred_element_type=f32)
    dva = jnp.einsum(
        "gqk,gqd->kd", p_back.astype(bf16), d_mixed, preferred_element_type=f32
    )
    d_blocks = jnp.stack([dka, dva]).reshape(2, 4, rows, -1)
    got_far = swap(d_blocks[:, 2:].astype(bf16), 1)
    d_near = d_blocks[:, :2] + got_far.astype(f32)
    got_row = swap(d_near[:, 1].astype(bf16), 2)
    d_own = d_near[:, 0] + got_row.astype(f32)

    d_query = (rotate(dqa.transpose(1, 0, 2), cosine, -sine) * scale).reshape(rows, -1)
    d_key = rotate(d_own[0].reshape(rows, -1, HEAD_SIZE), cosine, -sine).reshape(rows, -1)
    d_query = d_query.astype(bf16)
    d_key = d_key.astype(bf16)
    d_value = d_own[1].astype(bf16)
    d_qkv = jnp.concatenate([d_query, d_key, d_value], axis=1)
    du_query = dot_nt(d_query, b_query).astype(bf16)
    du_key = dot_nt(d_key, b_kv[0]).astype(bf16)
    du_value = dot_nt(d_value, b_kv[1]).astype(bf16)
    du_qkv = jnp.concatenate([du_query, du_key, du_value], axis=1)

    wide = jnp.concatenate(
        [
            dot_tn(du_qkv, n1),
            dot_tn(du_gu, n2),
            dot_tn(u_out, e_att),
            dot_tn(u_down, e_ffn),
        ]
    )
    hidden = d_gate.shape[1]
    g_b_gate = dot_tn(u_gu[:, :rank], d_gate)
    g_b_up = dot_tn(u_gu[:, rank:], d_up)
    g_a_down = dot_tn(du_down, act)
    g_b_query = dot_tn(u_qkv[:, :rank], d_query)
    g_b_key = dot_tn(u_qkv[:, rank : 2 * rank], d_key)
    g_b_value = dot_tn(u_qkv[:, 2 * rank :], d_value)
    g_a_out = dot_tn(du_out, ob)
    small = jnp.concatenate([g_b_query, g_b_key, g_b_value, g_a_out], axis=1)
    small = jnp.pad(small, ((0, 0), (0, hidden - small.shape[1])))
    split = jnp.concatenate([g_b_gate, g_b_up, g_a_down, small])

    slots = lax.axis_size("fsdp")
    first = ((ctx == 0) & (lax.axis_index("tp") == 0)).astype(f32)
    note = jnp.full((1, width), adapter.astype(f32) * first)
    wide = jnp.pad(jnp.concatenate([wide, note]), ((0, 8 * rank - wide.shape[0] - 1), (0, 0)))
    terms = jnp.concatenate(
        [wide.reshape(4, 2 * rank, width), split.reshape(4, rank, width)], axis=1
    ).astype(bf16)
    dn1, every = matmul_sum(
        [d_qkv, du_qkv], [qkv_full, a_qkv], 4, terms=terms, slots=slots, summed=2 * rank
    )
    dn1 = dn1.astype(f32)
    input_grad = dh1 + norm_back(residual, gains[0], dn1)

    wide_all = every[:, :, : 2 * rank].astype(f32).reshape(slots, 8 * rank, width)
    split_all = every[:, :, 2 * rank :].astype(f32).reshape(slots, 4 * rank, width)
    used = wide_all[:, 7 * rank, 0].astype(jnp.int32)
    select = (used[:, None] == jnp.arange(adapter_count, dtype=jnp.int32)[None, :]).astype(f32)

    def to_adapters(terms):
        return jnp.sum(select[:, :, None, None] * terms[:, None], axis=0)

    share = width // (slots * lax.axis_size("ctx"))
    start = (lax.axis_index("fsdp") * lax.axis_size("ctx") + ctx) * share
    wide_own = to_adapters(lax.dynamic_slice_in_dim(wide_all, start, share, axis=2))
    wide_own = wide_own[:, : 7 * rank].reshape(adapter_count, 7, rank, share)
    split_own = to_adapters(split_all).reshape(adapter_count, 4, rank, hidden)
    grad_a_in = wide_own[:, :5].transpose(1, 0, 3, 2)
    grad_b_out = wide_own[:, 5:].transpose(1, 0, 2, 3)
    small_own = split_own[:, 3]
    grad_b_query = small_own[:, :, :q_cols]
    grad_b_kv = jnp.stack(
        [small_own[:, :, q_cols : q_cols + k_cols], small_own[:, :, q_cols + k_cols : qkv_cols]]
    )
    grad_a_out = small_own[:, :, qkv_cols : qkv_cols + q_cols].transpose(0, 2, 1)
    grad_b_gate_up = split_own[:, :2].transpose(1, 0, 2, 3)
    grad_a_down = split_own[:, 2].transpose(0, 2, 1)
    return (
        final[None],
        input_grad[None],
        grad_a_in,
        grad_b_query,
        grad_b_kv,
        grad_b_gate_up,
        grad_a_out,
        grad_a_down,
        grad_b_out,
    )


def solution(mesh):
    both = ("fsdp", "ctx")
    in_specs = (
        P("fsdp", "ctx", None),
        P("fsdp", "ctx", None),
        P("fsdp"),
        P("fsdp"),
        P(),
        P(both, "tp"),
        P(both, "tp"),
        P(both, "tp"),
        P("tp", both),
        P(both, "tp"),
        P(both, "tp"),
        P("tp", both),
        P(),
        P(None, None, "tp"),
        P(None, None, None, "tp"),
        P(None, None, None, "tp"),
        P(None, "tp", None),
        P(None, "tp", None),
        P(),
    )
    out_specs = (
        P("fsdp", "ctx", None),
        P("fsdp", "ctx", None),
        P(None, None, both, None),
        P(None, None, "tp"),
        P(None, None, None, "tp"),
        P(None, None, None, "tp"),
        P(None, "tp", None),
        P(None, "tp", None),
        P(None, None, None, both),
    )
    return jax.shard_map(
        per_device, mesh=mesh, in_specs=in_specs, out_specs=out_specs, check_vma=False
    )
```

```python
import functools
import math

import jax
import jax.numpy as jnp
from jax import lax
from jax.experimental import pallas as pl
from jax.experimental.pallas import tpu as pltpu
from jax.sharding import PartitionSpec as P

QUERY_HEADS = 8
KEY_HEADS = 4
HEAD_SIZE = 256

epsilon = 1e-06
soft_cap = 50.0
MESH = pl.DeviceIdType.MESH
f32 = jnp.float32
bf16 = jnp.bfloat16


def rms_norm(values, gain):
    return values * lax.rsqrt(jnp.mean(values * values, axis=-1, keepdims=True) + epsilon) * gain


def norm_back(values, gain, incoming):
    scale = lax.rsqrt(jnp.mean(values * values, axis=-1, keepdims=True) + epsilon)
    unit = values * scale
    weighted = incoming * gain
    return scale * (weighted - unit * jnp.mean(weighted * unit, axis=-1, keepdims=True))


def rotate(values, cosine, sine):
    half = HEAD_SIZE // 2
    parts = []
    for at in range(0, values.shape[1], HEAD_SIZE):
        first = values[:, at : at + half]
        second = values[:, at + half : at + HEAD_SIZE]
        parts += [first * cosine - second * sine, second * cosine + first * sine]
    return jnp.concatenate(parts, axis=1)


def dot_nn(left, right):
    return lax.dot_general(left, right, (((1,), (0,)), ((), ())), preferred_element_type=f32)


def dot_nt(left, right):
    return lax.dot_general(left, right, (((1,), (1,)), ((), ())), preferred_element_type=f32)


def dot_tn(left, right):
    return lax.dot_general(left, right, (((0,), (0,)), ((), ())), preferred_element_type=f32)


def sum_kernel(count, width, chunks, slots, *refs):
    lefts = refs[:count]
    rights = refs[count : 2 * count]
    refs = refs[2 * count :]
    terms = None
    if slots:
        terms, out, every = refs[:3]
        refs = refs[3:]
    else:
        out = refs[0]
        refs = refs[1:]
    part, mine, got_a, got_b, a_send, a_recv, b_send, b_recv, c_send, c_recv = refs[:10]
    z = lax.axis_index("tp")
    inner = (z == 1) | (z == 2)
    outer = (z == 0) | (z == 3)
    pair = z + 1 - 2 * lax.rem(z, 2)
    across = 3 - z
    barrier = pltpu.get_barrier_semaphore()

    def greet(axis, peer):
        pl.semaphore_signal(barrier, inc=1, device_id={axis: peer}, device_id_type=MESH)

    others = 0
    if slots:
        at = lax.axis_index("ctx")
        core = lax.rem(at, 2)
        row = lax.div(at, 2)
        core_peer = at + 1 - 2 * core
        row_peer = at + 2 - 4 * row
        seq = lax.axis_index("fsdp")
        others = 2 + slots - 1
        greet("ctx", core_peer)
        greet("ctx", row_peer)
        for d in range(1, slots):
            greet("fsdp", lax.rem(seq + d, slots))
    greet("tp", pair)

    @pl.when(inner)
    def _():
        greet("tp", across)
        pl.semaphore_wait(barrier, others + 2)

    @pl.when(outer)
    def _():
        pl.semaphore_wait(barrier, others + 1)

    def cols(c):
        return pl.ds(pl.multiple_of(c * width, width), width)

    def remote(source, target, send, recv, axis, peer):
        return pltpu.make_async_remote_copy(
            source, target, send, recv, device_id={axis: peer}, device_id_type=MESH
        )

    def copy_a(c):
        return remote(mine.at[c], got_a.at[c], a_send.at[c], a_recv.at[c], "tp", pair)

    def copy_b(c):
        return remote(mine.at[c], got_b.at[c], b_send.at[c], b_recv.at[c], "tp", across)

    def copy_c(c):
        place = out.at[:, cols(c)]
        return remote(place, place, c_send.at[c], c_recv.at[c], "tp", pair)

    def finish(c):
        copy_b(c).wait_recv()
        out[:, cols(c)] = (mine[c].astype(f32) + got_b[c].astype(f32)).astype(bf16)
        copy_c(c).start()

    if slots:
        from_core, with_core, from_row, held, held_a, held_b, full, g_send, g_recv = refs[10:]
        summed = held_a.shape[0]
        rest = pl.ds(summed, full.shape[0] - summed)

        def core_copy(j):
            source = terms.at[2 * j + 1 - core]
            return remote(source, from_core.at[j], g_send.at[j], g_recv.at[j], "ctx", core_peer)

        def row_copy():
            source = with_core.at[1 - row]
            return remote(source, from_row, g_send.at[2], g_recv.at[2], "ctx", row_peer)

        def line_a():
            source = held.at[pl.ds(0, summed)]
            return remote(source, held_a, g_send.at[3], g_recv.at[3], "tp", pair)

        def line_b():
            source = held.at[pl.ds(0, summed)]
            return remote(source, held_b, g_send.at[4], g_recv.at[4], "tp", across)

        def line_c():
            place = full.at[pl.ds(0, summed)]
            return remote(place, place, g_send.at[5], g_recv.at[5], "tp", pair)

        def seq_copy(d):
            peer = lax.rem(seq + d, slots)
            return remote(
                full, every.at[seq, at], g_send.at[8 + d], g_recv.at[8 + d], "fsdp", peer
            )

        def row_back():
            place = every.at[:, at]
            return remote(place, place, g_send.at[6], g_recv.at[6], "ctx", row_peer)

        def core_back(j):
            place = every.at[:, 2 * j + core]
            return remote(place, place, g_send.at[7 + j], g_recv.at[7 + j], "ctx", core_peer)

        core_copy(0).start()
        core_copy(1).start()

        def reduce_terms(c):
            @pl.when(c == 1)
            def _():
                for j in range(2):
                    core_copy(j).wait_recv()
                    total = terms[2 * j + core].astype(f32) + from_core[j].astype(f32)
                    with_core[j] = total.astype(bf16)
                row_copy().start()

            @pl.when(c == 3)
            def _():
                row_copy().wait_recv()
                held[...] = (with_core[row].astype(f32) + from_row[...].astype(f32)).astype(bf16)
                full[rest, :] = held[rest, :]

            @pl.when((c == 3) & outer)
            def _():
                line_a().start()

            @pl.when((c == 6) & inner)
            def _():
                line_a().wait_recv()
                total = held[:summed].astype(f32) + held_a[...].astype(f32)
                held[:summed] = total.astype(bf16)
                line_b().start()

            @pl.when((c == 8) & inner)
            def _():
                line_b().wait_recv()
                total = held[:summed].astype(f32) + held_b[...].astype(f32)
                full[:summed] = total.astype(bf16)
                line_c().start()

            @pl.when((c == 11) & outer)
            def _():
                line_c().wait_recv()

            @pl.when(c == 11)
            def _():
                every[seq, at] = full[...]
                for d in range(1, slots):
                    seq_copy(d).start()

            @pl.when(c == 13)
            def _():
                for d in range(1, slots):
                    seq_copy(d).wait_recv()
                row_back().start()

            @pl.when(c == 15)
            def _():
                row_back().wait_recv()
                core_back(0).start()
                core_back(1).start()

    def body(c, carry):
        for i, (left, right) in enumerate(zip(lefts, rights)):
            for m in range(0, left.shape[0], 256):
                term = dot_nt(left[m : m + 256, :], right[cols(c), :])
                part[m : m + 256, :] = term if i == 0 else part[m : m + 256, :] + term

        @pl.when(outer)
        def _():
            mine[c] = part[...].astype(bf16)
            copy_a(c).start()

        @pl.when(inner)
        def _():
            copy_a(c).wait_recv()
            mine[c] = (part[...] + got_a[c].astype(f32)).astype(bf16)
            copy_b(c).start()

        @pl.when(inner & (c >= 1))
        def _():
            finish(c - 1)

        if slots:
            reduce_terms(c)
        return carry

    lax.fori_loop(0, chunks, body, 0)

    @pl.when(inner)
    def _():
        finish(chunks - 1)

        def drain(c, carry):
            copy_b(c).wait_send()
            copy_c(c).wait_send()
            return carry

        lax.fori_loop(0, chunks, drain, 0)

    @pl.when(outer)
    def _():
        def drain(c, carry):
            copy_a(c).wait_send()
            copy_c(c).wait_recv()
            return carry

        lax.fori_loop(0, chunks, drain, 0)

    if slots:
        for j in range(2):
            core_copy(j).wait_send()
            core_back(j).wait()
        row_copy().wait_send()
        row_back().wait_send()
        for d in range(1, slots):
            seq_copy(d).wait_send()

        @pl.when(outer)
        def _():
            line_a().wait_send()

        @pl.when(inner)
        def _():
            line_b().wait_send()
            line_c().wait_send()


def matmul_sum(lefts, rights, collective_id, width=128, terms=None, slots=0, summed=0):
    rows = lefts[0].shape[0]
    total = rights[0].shape[0]
    chunks = total // width
    flops = sum(2 * rows * total * left.shape[1] for left in lefts)
    moved = sum(left.size + right.size for left, right in zip(lefts, rights)) + rows * total
    scratch = (
        [pltpu.VMEM((rows, width), f32)]
        + [pltpu.VMEM((chunks, rows, width), bf16)] * 3
        + [pltpu.SemaphoreType.DMA((chunks,))] * 6
    )
    shapes = [jax.ShapeDtypeStruct((rows, total), bf16)]
    operands = [*lefts, *rights]
    if slots:
        assert chunks >= 17
        block = terms.shape[1:]
        lead = (summed, block[1])
        operands.append(terms)
        shapes.append(jax.ShapeDtypeStruct((slots, *terms.shape), bf16))
        scratch += [
            pltpu.VMEM((2, *block), bf16),
            pltpu.VMEM((2, *block), bf16),
            pltpu.VMEM(block, bf16),
            pltpu.VMEM(block, bf16),
            pltpu.VMEM(lead, bf16),
            pltpu.VMEM(lead, bf16),
            pltpu.VMEM(block, bf16),
            pltpu.SemaphoreType.DMA((9 + slots,)),
            pltpu.SemaphoreType.DMA((9 + slots,)),
        ]
    vmem = pl.BlockSpec(memory_space=pltpu.VMEM)
    result = pl.pallas_call(
        functools.partial(sum_kernel, len(lefts), width, chunks, slots),
        out_shape=shapes,
        in_specs=[vmem] * len(operands),
        out_specs=[vmem] * len(shapes),
        scratch_shapes=scratch,
        compiler_params=pltpu.CompilerParams(
            collective_id=collective_id, has_side_effects=True, vmem_limit_bytes=60 * 1024 * 1024
        ),
        cost_estimate=pl.CostEstimate(flops=flops, bytes_accessed=2 * moved, transcendentals=0),
        name=f"matmul_sum_{collective_id}",
    )(*operands)
    return result if slots else result[0]


def ffn_kernel(
    n2_all,
    cot_all,
    u_gu,
    gain,
    b_gate,
    a_down,
    b_down,
    a_gu,
    ffn_all,
    y_all,
    dn2_all,
    act_all,
    e_all,
    dg_all,
    du_all,
    w_gate,
    w_up,
    w_down,
    n2_buf,
    cot_buf,
    act_buf,
    e_buf,
    dg_buf,
    du_buf,
    keep_up,
    keep_gate,
    part,
    mine,
    got_a,
    got_b,
    total,
    load_sem,
    in_sem,
    out_sem,
    a_send,
    a_recv,
    b_send,
    b_recv,
    c_send,
    c_recv,
):
    n, rows, width = n2_all.shape
    ring = mine.shape[0]
    rank = b_down.shape[0]
    tile = width // 3
    z = lax.axis_index("tp")
    inner = (z == 1) | (z == 2)
    outer = (z == 0) | (z == 3)
    pair = z + 1 - 2 * lax.rem(z, 2)
    across = 3 - z

    weights = [
        pltpu.make_async_copy(
            ffn_all.at[:, pl.ds(i * width, width)], target, load_sem.at[i]
        )
        for i, target in enumerate((w_gate, w_up, w_down))
    ]

    def n2_copy(c):
        return pltpu.make_async_copy(n2_all.at[c], n2_buf.at[lax.rem(c, 2)], in_sem.at[lax.rem(c, 2)])

    def cot_copy(c):
        slot = lax.rem(c, 2)
        return pltpu.make_async_copy(cot_all.at[c], cot_buf.at[slot], in_sem.at[2 + slot])

    n2_copy(0).start()
    for copy in weights:
        copy.start()
    n2_copy(1).start()
    cot_copy(0).start()
    cot_copy(1).start()

    barrier = pltpu.get_barrier_semaphore()
    pl.semaphore_signal(barrier, inc=1, device_id={"tp": pair}, device_id_type=MESH)

    @pl.when(inner)
    def _():
        pl.semaphore_signal(barrier, inc=1, device_id={"tp": across}, device_id_type=MESH)
        pl.semaphore_wait(barrier, 2)

    @pl.when(outer)
    def _():
        pl.semaphore_wait(barrier, 1)

    def remote(source, target, send, recv, peer):
        return pltpu.make_async_remote_copy(
            source, target, send, recv, device_id={"tp": peer}, device_id_type=MESH
        )

    def copy_a(k):
        slot = lax.rem(k, ring)
        return remote(mine.at[slot], got_a.at[slot], a_send.at[k], a_recv.at[k], pair)

    def copy_b(k):
        slot = lax.rem(k, ring)
        return remote(mine.at[slot], got_b.at[slot], b_send.at[k], b_recv.at[k], across)

    def copy_c(k):
        place = total.at[lax.rem(k, n)]
        return remote(place, place, c_send.at[k], c_recv.at[k], pair)

    def finish(k):
        slot = lax.rem(k, ring)
        copy_b(k).wait_recv()
        total[lax.rem(k, n)] = (mine[slot].astype(f32) + got_b[slot].astype(f32)).astype(bf16)
        copy_c(k).start()

    def exchange(k):
        slot = lax.rem(k, ring)

        @pl.when(outer & (k >= ring))
        def _():
            copy_c(k - ring).wait_recv()
            copy_a(k - ring).wait_send()

        @pl.when(outer)
        def _():
            mine[slot] = part[...].astype(bf16)
            copy_a(k).start()

        @pl.when(inner & (k >= ring))
        def _():
            copy_b(k - ring).wait_send()

        @pl.when(inner)
        def _():
            copy_a(k).wait_recv()
            mine[slot] = (part[...] + got_a[slot].astype(f32)).astype(bf16)
            copy_b(k).start()

        @pl.when(inner & (k >= n + 1))
        def _():
            copy_c(k - 1 - n).wait_send()

        @pl.when(inner & (k >= 1))
        def _():
            finish(k - 1)

    def put(i, buf, target, c):
        return pltpu.make_async_copy(buf, target.at[c], out_sem.at[i])

    def act_out(c):
        return put(0, act_buf, act_all, c)

    def forward(k, carry):
        n2_copy(k).wait()

        @pl.when(k == 0)
        def _():
            weights[0].wait()
            weights[1].wait()

        @pl.when(k >= 1)
        def _():
            act_out(k - 1).wait()

        slot = lax.rem(k, 2)
        u_here = u_gu[k]
        for i in range(3):
            cols = slice(i * tile, (i + 1) * tile)
            gate = dot_nn(n2_buf[slot], w_gate[:, cols]) + dot_nn(u_here[:, :rank], b_gate[0, :, cols])
            upper = dot_nn(n2_buf[slot], w_up[:, cols]) + dot_nn(u_here[:, rank:], b_gate[1, :, cols])
            square = gate * gate
            slant = math.sqrt(2.0 / math.pi)
            bend = jnp.tanh(slant * (gate + 0.044715 * (square * gate)))
            side = 0.5 * (1.0 + bend)
            curve = gate * side
            rise = side + 0.5 * gate * (1.0 - bend * bend) * (
                slant * (1.0 + 3.0 * 0.044715 * square)
            )
            act_buf[:, cols] = (curve * upper).astype(bf16)
            keep_up[k, :, cols] = curve.astype(bf16)
            keep_gate[k, :, cols] = (rise * upper).astype(bf16)

        @pl.when(k + 2 < n)
        def _():
            n2_copy(k + 2).start()

        act_out(k).start()

        @pl.when(k == 0)
        def _():
            weights[2].wait()

        u_down = dot_nt(act_buf[...], a_down[...]).astype(bf16)
        for i in range(3):
            cols = slice(i * tile, (i + 1) * tile)
            part[:, cols] = dot_nt(act_buf[...], w_down[cols, :]) + dot_nn(u_down, b_down[:, cols])
        exchange(k)
        return carry

    def back_out(i, c):
        if i == 0:
            return put(1, e_buf, e_all, c)
        if i == 1:
            return put(2, dg_buf, dg_all, c)
        if i == 2:
            return put(3, du_buf, du_all, c)
        return put(4, total.at[c], y_all, c)

    def backward(c, carry):
        cot_copy(c).wait()
        back_out(3, c).start()

        @pl.when(c >= 1)
        def _():
            for i in range(3):
                back_out(i, c - 1).wait()

        slot = lax.rem(c, 2)

        def norm(i, inside):
            lines = pl.ds(pl.multiple_of(i * 16, 16), 16)
            values = total[c, lines, :].astype(f32)
            scale = lax.rsqrt(jnp.mean(values * values, axis=-1, keepdims=True) + epsilon)
            unit = values * scale
            weighted = cot_buf[slot, lines, :].astype(f32) * gain[...]
            e_buf[lines, :] = (
                scale * (weighted - unit * jnp.mean(weighted * unit, axis=-1, keepdims=True))
            ).astype(bf16)
            return inside

        lax.fori_loop(0, rows // 16, norm, 0)

        @pl.when(c + 2 < n)
        def _():
            cot_copy(c + 2).start()

        back_out(0, c).start()
        du_down = dot_nt(e_buf[...], b_down[...]).astype(bf16)
        for i in range(3):
            cols = slice(i * tile, (i + 1) * tile)
            d_act = dot_nn(e_buf[...], w_down[:, cols]) + dot_nn(du_down, a_down[:, cols])
            dg_buf[:, cols] = (d_act * keep_gate[c, :, cols].astype(f32)).astype(bf16)
            du_buf[:, cols] = (d_act * keep_up[c, :, cols].astype(f32)).astype(bf16)
        back_out(1, c).start()
        back_out(2, c).start()
        du_gate = dot_nt(dg_buf[...], b_gate[0]).astype(bf16)
        du_up = dot_nt(du_buf[...], b_gate[1]).astype(bf16)
        for i in range(3):
            cols = slice(i * tile, (i + 1) * tile)
            part[:, cols] = (
                dot_nt(dg_buf[...], w_gate[cols, :])
                + dot_nt(du_buf[...], w_up[cols, :])
                + dot_nn(du_gate, a_gu[0, :, cols])
                + dot_nn(du_up, a_gu[1, :, cols])
            )
        back_out(3, c).wait()
        exchange(n + c)
        return carry

    def result(c):
        return pltpu.make_async_copy(total.at[c], dn2_all.at[c], out_sem.at[5 + c])

    lax.fori_loop(0, n, forward, 0)
    lax.fori_loop(0, n, backward, 0)
    act_out(n - 1).wait()
    for i in range(3):
        back_out(i, n - 1).wait()

    @pl.when(inner)
    def _():
        copy_c(n - 1).wait_send()
        finish(2 * n - 1)

        def drain(k, carry):
            copy_b(k).wait_send()
            return carry

        lax.fori_loop(2 * n - ring, 2 * n, drain, 0)

        def drain_c(k, carry):
            copy_c(k).wait_send()
            return carry

        lax.fori_loop(n, 2 * n, drain_c, 0)

    @pl.when(outer)
    def _():
        def drain(k, carry):
            copy_c(k).wait_recv()
            copy_a(k).wait_send()
            return carry

        lax.fori_loop(2 * n - ring, 2 * n, drain, 0)

    for c in range(n):
        result(c).start()
    for c in range(n):
        result(c).wait()


def feed_forward(
    n2, cot, u_gu, gain, b_gate, a_down, b_down, a_gu, ffn_full, collective_id
):
    rows, width = n2.shape
    hidden = ffn_full.shape[1] // 3
    assert hidden == width
    step = 128
    n = rows // step
    ring = 4
    full = jax.ShapeDtypeStruct((n, step, width), bf16)
    vmem = pl.BlockSpec(memory_space=pltpu.VMEM)
    anywhere = pl.BlockSpec(memory_space=pl.ANY)
    block = pltpu.VMEM((step, width), bf16)
    results = pl.pallas_call(
        ffn_kernel,
        out_shape=[full] * 6,
        in_specs=[anywhere] * 2 + [vmem] * 6 + [anywhere],
        out_specs=[anywhere] * 6,
        scratch_shapes=[pltpu.VMEM((width, width), bf16)] * 3
        + [pltpu.VMEM((2, step, width), bf16)] * 2
        + [block] * 4
        + [pltpu.VMEM((n, step, width), bf16)] * 2
        + [pltpu.VMEM((step, width), f32)]
        + [pltpu.VMEM((ring, step, width), bf16)] * 3
        + [pltpu.VMEM((n, step, width), bf16)]
        + [
            pltpu.SemaphoreType.DMA((3,)),
            pltpu.SemaphoreType.DMA((4,)),
            pltpu.SemaphoreType.DMA((5 + n,)),
        ]
        + [pltpu.SemaphoreType.DMA((2 * n,))] * 6,
        compiler_params=pltpu.CompilerParams(
            collective_id=collective_id, has_side_effects=True, vmem_limit_bytes=67043328
        ),
        cost_estimate=pl.CostEstimate(
            flops=12 * rows * width * hidden, bytes_accessed=60 * 2**20, transcendentals=rows * hidden
        ),
        name=f"feed_forward_{collective_id}",
    )(
        n2.reshape(n, step, width),
        cot.reshape(n, step, width),
        u_gu.reshape(n, step, -1),
        gain,
        b_gate,
        a_down,
        b_down,
        a_gu,
        ffn_full,
    )
    return [value.reshape(rows, width) for value in results]


def attend_kernel(tile, bases, q, limit, keys, values, out, sums):
    rows = q.shape[0]
    block = keys.shape[0] // bases.shape[0]
    last = limit[...]
    acc = jnp.zeros((rows, HEAD_SIZE), f32)
    norm = jnp.zeros((rows, 1), f32)
    for i in range(keys.shape[0] // tile):
        span = slice(i * tile, (i + 1) * tile)
        base = bases[i * tile // block] + (i * tile) % block
        raw = dot_nt(q[...], keys[span, :])
        weight = jnp.exp(soft_cap * jnp.tanh(raw * (1.0 / soft_cap)))
        place = lax.broadcasted_iota(jnp.int32, (rows, tile), 1) + base
        weight = jnp.where(place <= last, weight, 0.0)
        norm = norm + jnp.sum(weight, axis=-1, keepdims=True)
        acc = acc + dot_nn(weight.astype(bf16), values[span, :])
    out[...] = (acc / norm).astype(bf16)
    sums[...] = norm


def attend(q, limit, keys, values, bases):
    rows, cols = q.shape
    step = 256
    return pl.pallas_call(
        functools.partial(attend_kernel, 768),
        out_shape=[
            jax.ShapeDtypeStruct((rows, cols), bf16),
            jax.ShapeDtypeStruct((cols // HEAD_SIZE, rows, 1), f32),
        ],
        grid=(rows // step, cols // HEAD_SIZE),
        in_specs=[
            pl.BlockSpec(memory_space=pltpu.SMEM),
            pl.BlockSpec((step, HEAD_SIZE), lambda i, g: (i, g)),
            pl.BlockSpec((step, 1), lambda i, g: (i, 0)),
            pl.BlockSpec(keys.shape, lambda i, g: (0, 0)),
            pl.BlockSpec(keys.shape, lambda i, g: (0, 0)),
        ],
        out_specs=[
            pl.BlockSpec((step, HEAD_SIZE), lambda i, g: (i, g)),
            pl.BlockSpec((None, step, 1), lambda i, g: (g, i, 0)),
        ],
        compiler_params=pltpu.CompilerParams(vmem_limit_bytes=50 * 2**20),
        cost_estimate=pl.CostEstimate(
            flops=4 * rows * cols * keys.shape[0],
            bytes_accessed=8 * 2**20,
            transcendentals=2 * rows * cols * keys.shape[0] // HEAD_SIZE,
        ),
        name="attend",
    )(bases, q, limit, keys, values)


def attend_back_kernel(
    tile, bases, q, d_out, limit, inverse, delta, keys, values, dq, near, far, dk_sum, dv_sum
):
    rows = q.shape[0]
    total = keys.shape[0]
    block = total // bases.shape[0]
    here = pl.program_id(0) * pl.num_programs(1) + pl.program_id(1)
    steps = pl.num_programs(0) * pl.num_programs(1)

    @pl.when(here == 0)
    def _():
        dk_sum[...] = jnp.zeros_like(dk_sum)
        dv_sum[...] = jnp.zeros_like(dv_sum)

    last = limit[...]
    scale = inverse[...]
    shift = delta[...]
    dq_sum = jnp.zeros((rows, HEAD_SIZE), f32)
    for i in range(total // tile):
        span = slice(i * tile, (i + 1) * tile)
        base = bases[i * tile // block] + (i * tile) % block
        raw = dot_nt(keys[span, :], q[...])
        bend = jnp.tanh(raw * (1.0 / soft_cap))
        place = lax.broadcasted_iota(jnp.int32, (tile, rows), 0) + base
        weight = jnp.where(place <= last, jnp.exp(soft_cap * bend) * scale, 0.0)
        d_weight = dot_nt(values[span, :], d_out[...])
        d_raw = (weight * (d_weight - shift) * (1.0 - bend * bend)).astype(bf16)
        dv_sum[span, :] += dot_nn(weight.astype(bf16), d_out[...])
        dk_sum[span, :] += dot_nn(d_raw, q[...])
        dq_sum = dq_sum + dot_tn(d_raw, keys[span, :])
    dq[...] = dq_sum

    @pl.when(here == steps - 1)
    def _():
        half = total // 2
        near[0] = dk_sum[:half]
        near[1] = dv_sum[:half]
        far[0] = dk_sum[half:].astype(bf16)
        far[1] = dv_sum[half:].astype(bf16)


def attend_back(q, d_out, limit, inverse, delta, keys, values, bases):
    rows, cols = q.shape
    step = 256
    total = keys.shape[0]
    mat = pl.BlockSpec((step, HEAD_SIZE), lambda i, g: (i, g))
    line = pl.BlockSpec((None, 1, step), lambda i, g: (g, 0, i))
    whole = pl.BlockSpec(keys.shape, lambda i, g: (0, 0))
    half = (2, total // 2, HEAD_SIZE)
    return pl.pallas_call(
        functools.partial(attend_back_kernel, 768),
        out_shape=[
            jax.ShapeDtypeStruct((rows, cols), f32),
            jax.ShapeDtypeStruct(half, f32),
            jax.ShapeDtypeStruct(half, bf16),
        ],
        grid=(rows // step, cols // HEAD_SIZE),
        in_specs=[
            pl.BlockSpec(memory_space=pltpu.SMEM),
            mat,
            mat,
            pl.BlockSpec((1, step), lambda i, g: (0, i)),
            line,
            line,
            whole,
            whole,
        ],
        out_specs=[
            mat,
            pl.BlockSpec(half, lambda i, g: (0, 0, 0)),
            pl.BlockSpec(half, lambda i, g: (0, 0, 0)),
        ],
        scratch_shapes=[pltpu.VMEM((total, HEAD_SIZE), f32)] * 2,
        compiler_params=pltpu.CompilerParams(vmem_limit_bytes=60 * 2**20),
        cost_estimate=pl.CostEstimate(
            flops=10 * rows * cols * total,
            bytes_accessed=16 * 2**20,
            transcendentals=2 * rows * cols * total // HEAD_SIZE,
        ),
        name="attend_back",
    )(bases, q, d_out, limit, inverse, delta, keys, values)


def q_pairs(q_cols, k_cols):
    return k_cols == HEAD_SIZE and q_cols == QUERY_HEADS // KEY_HEADS * HEAD_SIZE


def swap(values, step):
    return lax.ppermute(values, "ctx", [(i, i ^ step) for i in range(lax.axis_size("ctx"))])


def per_device(
    tokens,
    cotangent,
    prefix_length,
    sequence_adapter_index,
    gains,
    query_weight,
    key_weight,
    value_weight,
    output_weight,
    gate_weight,
    up_weight,
    down_weight,
    adapter_first_input,
    adapter_second_query,
    adapter_second_keyvalue,
    adapter_second_gate,
    adapter_first_output,
    adapter_first_down,
    adapter_second_output,
):
    seqs, rows, width = tokens.shape
    assert seqs == 1 and lax.axis_size("ctx") == 4 and lax.axis_size("tp") == 4
    assert q_pairs(query_weight.shape[1], key_weight.shape[1])
    scale = HEAD_SIZE ** (-0.5)
    q_cols = query_weight.shape[1]
    k_cols = key_weight.shape[1]
    adapter_count, rank = adapter_second_query.shape[:2]
    both = ("fsdp", "ctx")
    adapter = sequence_adapter_index[0]

    def chosen(table, dim):
        return lax.dynamic_index_in_dim(table, adapter, dim, keepdims=False)

    def gathered(*parts):
        return lax.all_gather(jnp.concatenate(parts, axis=1), both, axis=0, tiled=True)

    kv_full = gathered(key_weight, value_weight)
    query_full = gathered(query_weight, output_weight.T)
    ffn_full = gathered(gate_weight, up_weight, down_weight.T)
    qkv_cols = q_cols + 2 * k_cols
    out_full = query_full[:, q_cols:]
    query_full = query_full[:, :q_cols]

    a_in = chosen(adapter_first_input, 1)
    b_query = chosen(adapter_second_query, 0)
    b_kv = chosen(adapter_second_keyvalue, 1)
    b_gate = chosen(adapter_second_gate, 1)
    a_out = chosen(adapter_first_output, 0)
    a_down = chosen(adapter_first_down, 0)
    b_out = chosen(adapter_second_output, 1)
    a_qkv = jnp.concatenate([a_in[0], a_in[1], a_in[2]], axis=1)
    a_gu = jnp.concatenate([a_in[3], a_in[4]], axis=1)

    ctx = lax.axis_index("ctx")
    query_pos = ctx * rows + jnp.arange(rows, dtype=jnp.int32)
    half = HEAD_SIZE // 2
    freqs = jnp.exp(jnp.arange(half, dtype=f32) * (-2.0 * math.log(10000.0) / HEAD_SIZE))
    angle = query_pos.astype(f32)[:, None] * freqs[None, :]
    cosine = jnp.cos(angle)
    sine = jnp.sin(angle)

    residual = tokens[0].astype(f32)
    d_final = cotangent[0].astype(f32)
    n1 = rms_norm(residual, gains[0]).astype(bf16)
    u_qkv = dot_nn(n1, a_qkv).astype(bf16)
    lin_kv = dot_nn(n1, kv_full)
    query = dot_nn(n1, query_full) + dot_nn(u_qkv[:, :rank], b_query)
    key = lin_kv[:, :k_cols] + dot_nn(u_qkv[:, rank : 2 * rank], b_kv[0])
    value = lin_kv[:, k_cols:] + dot_nn(u_qkv[:, 2 * rank :], b_kv[1])
    qa = (rotate(query, cosine, sine) * scale).astype(bf16)
    ka = rotate(key, cosine, sine).astype(bf16)
    va = value.astype(bf16)

    own = jnp.stack([ka, va])
    from_row = swap(own, 2)
    near = jnp.concatenate([own, from_row], axis=1)
    far = swap(near, 1)
    keys, values = jnp.concatenate([near, far], axis=1)
    bases = jnp.stack([ctx, ctx ^ 2, ctx ^ 1, ctx ^ 3]) * rows
    limit = jnp.maximum(query_pos, prefix_length[0] - 1)
    ob, sums = attend(qa, limit[:, None], keys, values, bases)

    u_out = dot_nn(ob, a_out).astype(bf16)
    y_att = matmul_sum([ob, u_out], [out_full, b_out[0].T], 1).astype(f32)
    h1 = residual + rms_norm(y_att, gains[1])
    n2 = rms_norm(h1, gains[2]).astype(bf16)
    u_gu = dot_nn(n2, a_gu).astype(bf16)
    y_ffn, dn2, act, e_ffn, d_gate, d_up = feed_forward(
        n2,
        cotangent[0],
        u_gu,
        gains[3][None],
        b_gate,
        a_down.T,
        b_out[1],
        jnp.stack([a_in[3].T, a_in[4].T]),
        ffn_full,
        2,
    )
    dn2 = dn2.astype(f32)
    dh1 = d_final + norm_back(h1, gains[2], dn2)
    e_att = norm_back(y_att, gains[1], dh1).astype(bf16)
    du_out = dot_nt(e_att, b_out[0]).astype(bf16)
    d_ob = (dot_nn(e_att, out_full) + dot_nt(du_out, a_out)).astype(bf16)
    overlap = d_ob.astype(f32) * ob.astype(f32)
    delta = jnp.stack(
        [
            jnp.sum(overlap[:, at : at + HEAD_SIZE], axis=-1)[None]
            for at in range(0, q_cols, HEAD_SIZE)
        ]
    )
    dqa, d_near, d_far = attend_back(
        qa,
        d_ob,
        limit[None],
        (1.0 / sums)[..., 0][:, None],
        delta,
        keys,
        values,
        bases,
    )
    d_query = (rotate(dqa, cosine, -sine) * scale).astype(bf16)
    d_near = d_near + swap(d_far, 1).astype(f32)
    d_row = d_near[:, rows:].astype(bf16)
    d_row, y_ffn, act, e_ffn, d_gate, d_up, e_att, du_out, d_query = lax.optimization_barrier(
        (d_row, y_ffn, act, e_ffn, d_gate, d_up, e_att, du_out, d_query)
    )
    d_own = d_near[:, :rows] + swap(d_row, 2).astype(f32)
    final = (h1 + rms_norm(y_ffn.astype(f32), gains[3])).astype(bf16)
    u_down = dot_nn(act, a_down).astype(bf16)
    du_down = dot_nt(e_ffn, b_out[1]).astype(bf16)
    du_gate = dot_nt(d_gate, b_gate[0]).astype(bf16)
    du_up = dot_nt(d_up, b_gate[1]).astype(bf16)
    du_gu = jnp.concatenate([du_gate, du_up], axis=1)

    d_key = rotate(d_own[0], cosine, -sine).astype(bf16)
    d_value = d_own[1].astype(bf16)
    d_kv = jnp.concatenate([d_key, d_value], axis=1)
    du_query = dot_nt(d_query, b_query).astype(bf16)
    du_key = dot_nt(d_key, b_kv[0]).astype(bf16)
    du_value = dot_nt(d_value, b_kv[1]).astype(bf16)
    du_qkv = jnp.concatenate([du_query, du_key, du_value], axis=1)

    wide = jnp.concatenate(
        [
            dot_tn(du_qkv, n1),
            dot_tn(du_gu, n2),
            dot_tn(u_out, e_att),
            dot_tn(u_down, e_ffn),
        ]
    )
    hidden = d_gate.shape[1]
    g_b_gate = dot_tn(u_gu[:, :rank], d_gate)
    g_b_up = dot_tn(u_gu[:, rank:], d_up)
    g_a_down = dot_tn(du_down, act)
    g_b_query = dot_tn(u_qkv[:, :rank], d_query)
    g_b_key = dot_tn(u_qkv[:, rank : 2 * rank], d_key)
    g_b_value = dot_tn(u_qkv[:, 2 * rank :], d_value)
    g_a_out = dot_tn(du_out, ob)
    small = jnp.concatenate([g_b_query, g_b_key, g_b_value, g_a_out], axis=1)
    small = jnp.pad(small, ((0, 0), (0, hidden - small.shape[1])))
    split = jnp.concatenate([g_b_gate, g_b_up, g_a_down, small])

    slots = lax.axis_size("fsdp")
    first = ((ctx == 0) & (lax.axis_index("tp") == 0)).astype(f32)
    note = jnp.full((1, width), adapter.astype(f32) * first)
    wide = jnp.pad(jnp.concatenate([wide, note]), ((0, 8 * rank - wide.shape[0] - 1), (0, 0)))
    terms = jnp.concatenate(
        [wide.reshape(4, 2 * rank, width), split.reshape(4, rank, width)], axis=1
    ).astype(bf16)
    dn1, every = matmul_sum(
        [d_query, d_kv, du_qkv], [query_full, kv_full, a_qkv], 4, terms=terms, slots=slots, summed=2 * rank
    )
    dn1 = dn1.astype(f32)
    input_grad = dh1 + norm_back(residual, gains[0], dn1)

    wide_all = every[:, :, : 2 * rank].astype(f32).reshape(slots, 8 * rank, width)
    split_all = every[:, :, 2 * rank :].astype(f32).reshape(slots, 4 * rank, width)
    used = wide_all[:, 7 * rank, 0].astype(jnp.int32)
    select = (used[:, None] == jnp.arange(adapter_count, dtype=jnp.int32)[None, :]).astype(f32)

    def to_adapters(terms):
        return jnp.sum(select[:, :, None, None] * terms[:, None], axis=0)

    share = width // (slots * lax.axis_size("ctx"))
    start = (lax.axis_index("fsdp") * lax.axis_size("ctx") + ctx) * share
    wide_own = to_adapters(lax.dynamic_slice_in_dim(wide_all, start, share, axis=2))
    wide_own = wide_own[:, : 7 * rank].reshape(adapter_count, 7, rank, share)
    split_own = to_adapters(split_all).reshape(adapter_count, 4, rank, hidden)
    grad_a_in = wide_own[:, :5].transpose(1, 0, 3, 2)
    grad_b_out = wide_own[:, 5:].transpose(1, 0, 2, 3)
    small_own = split_own[:, 3]
    grad_b_query = small_own[:, :, :q_cols]
    grad_b_kv = jnp.stack(
        [small_own[:, :, q_cols : q_cols + k_cols], small_own[:, :, q_cols + k_cols : qkv_cols]]
    )
    grad_a_out = small_own[:, :, qkv_cols : qkv_cols + q_cols].transpose(0, 2, 1)
    grad_b_gate_up = split_own[:, :2].transpose(1, 0, 2, 3)
    grad_a_down = split_own[:, 2].transpose(0, 2, 1)
    return (
        final[None],
        input_grad[None],
        grad_a_in,
        grad_b_query,
        grad_b_kv,
        grad_b_gate_up,
        grad_a_out,
        grad_a_down,
        grad_b_out,
    )


def solution(mesh):
    both = ("fsdp", "ctx")
    in_specs = (
        P("fsdp", "ctx", None),
        P("fsdp", "ctx", None),
        P("fsdp"),
        P("fsdp"),
        P(),
        P(both, "tp"),
        P(both, "tp"),
        P(both, "tp"),
        P("tp", both),
        P(both, "tp"),
        P(both, "tp"),
        P("tp", both),
        P(),
        P(None, None, "tp"),
        P(None, None, None, "tp"),
        P(None, None, None, "tp"),
        P(None, "tp", None),
        P(None, "tp", None),
        P(),
    )
    out_specs = (
        P("fsdp", "ctx", None),
        P("fsdp", "ctx", None),
        P(None, None, both, None),
        P(None, None, "tp"),
        P(None, None, None, "tp"),
        P(None, None, None, "tp"),
        P(None, "tp", None),
        P(None, "tp", None),
        P(None, None, None, both),
    )
    return jax.shard_map(
        per_device, mesh=mesh, in_specs=in_specs, out_specs=out_specs, check_vma=False
    )
```

```python
import functools
import math

import jax
import jax.numpy as jnp
from jax import lax
from jax.experimental import pallas as pl
from jax.experimental.pallas import tpu as pltpu
from jax.sharding import PartitionSpec as P

QUERY_HEADS = 8
KEY_HEADS = 4
HEAD_SIZE = 256

epsilon = 1e-06
soft_cap = 50.0
MESH = pl.DeviceIdType.MESH
f32 = jnp.float32
bf16 = jnp.bfloat16


def rms_norm(values, gain):
    return values * lax.rsqrt(jnp.mean(values * values, axis=-1, keepdims=True) + epsilon) * gain


def norm_back(values, gain, incoming):
    scale = lax.rsqrt(jnp.mean(values * values, axis=-1, keepdims=True) + epsilon)
    unit = values * scale
    weighted = incoming * gain
    return scale * (weighted - unit * jnp.mean(weighted * unit, axis=-1, keepdims=True))


def rotate(values, cosine, sine):
    half = HEAD_SIZE // 2
    parts = []
    for at in range(0, values.shape[1], HEAD_SIZE):
        first = values[:, at : at + half]
        second = values[:, at + half : at + HEAD_SIZE]
        parts += [first * cosine - second * sine, second * cosine + first * sine]
    return jnp.concatenate(parts, axis=1)


def dot_nn(left, right):
    return lax.dot_general(left, right, (((1,), (0,)), ((), ())), preferred_element_type=f32)


def dot_nt(left, right):
    return lax.dot_general(left, right, (((1,), (1,)), ((), ())), preferred_element_type=f32)


def dot_tn(left, right):
    return lax.dot_general(left, right, (((0,), (0,)), ((), ())), preferred_element_type=f32)


def sum_kernel(count, width, chunks, slots, *refs):
    lefts = refs[:count]
    rights = refs[count : 2 * count]
    refs = refs[2 * count :]
    terms = None
    if slots:
        terms, out, every = refs[:3]
        refs = refs[3:]
    else:
        out = refs[0]
        refs = refs[1:]
    part, mine, got_a, got_b, a_send, a_recv, b_send, b_recv, c_send, c_recv = refs[:10]
    z = lax.axis_index("tp")
    inner = (z == 1) | (z == 2)
    outer = (z == 0) | (z == 3)
    pair = z + 1 - 2 * lax.rem(z, 2)
    across = 3 - z
    barrier = pltpu.get_barrier_semaphore()

    def greet(axis, peer):
        pl.semaphore_signal(barrier, inc=1, device_id={axis: peer}, device_id_type=MESH)

    others = 0
    if slots:
        at = lax.axis_index("ctx")
        core = lax.rem(at, 2)
        row = lax.div(at, 2)
        core_peer = at + 1 - 2 * core
        row_peer = at + 2 - 4 * row
        seq = lax.axis_index("fsdp")
        others = 2 + slots - 1
        greet("ctx", core_peer)
        greet("ctx", row_peer)
        for d in range(1, slots):
            greet("fsdp", lax.rem(seq + d, slots))
    greet("tp", pair)

    @pl.when(inner)
    def _():
        greet("tp", across)
        pl.semaphore_wait(barrier, others + 2)

    @pl.when(outer)
    def _():
        pl.semaphore_wait(barrier, others + 1)

    def cols(c):
        return pl.ds(pl.multiple_of(c * width, width), width)

    def remote(source, target, send, recv, axis, peer):
        return pltpu.make_async_remote_copy(
            source, target, send, recv, device_id={axis: peer}, device_id_type=MESH
        )

    def copy_a(c):
        return remote(mine.at[c], got_a.at[c], a_send.at[c], a_recv.at[c], "tp", pair)

    def copy_b(c):
        return remote(mine.at[c], got_b.at[c], b_send.at[c], b_recv.at[c], "tp", across)

    def copy_c(c):
        place = out.at[:, cols(c)]
        return remote(place, place, c_send.at[c], c_recv.at[c], "tp", pair)

    def finish(c):
        copy_b(c).wait_recv()
        out[:, cols(c)] = (mine[c].astype(f32) + got_b[c].astype(f32)).astype(bf16)
        copy_c(c).start()

    if slots:
        from_core, with_core, from_row, held, held_a, held_b, full, g_send, g_recv = refs[10:]
        summed = held_a.shape[0]
        rest = pl.ds(summed, full.shape[0] - summed)

        def core_copy(j):
            source = terms.at[2 * j + 1 - core]
            return remote(source, from_core.at[j], g_send.at[j], g_recv.at[j], "ctx", core_peer)

        def row_copy():
            source = with_core.at[1 - row]
            return remote(source, from_row, g_send.at[2], g_recv.at[2], "ctx", row_peer)

        def line_a():
            source = held.at[pl.ds(0, summed)]
            return remote(source, held_a, g_send.at[3], g_recv.at[3], "tp", pair)

        def line_b():
            source = held.at[pl.ds(0, summed)]
            return remote(source, held_b, g_send.at[4], g_recv.at[4], "tp", across)

        def line_c():
            place = full.at[pl.ds(0, summed)]
            return remote(place, place, g_send.at[5], g_recv.at[5], "tp", pair)

        def seq_copy(d):
            peer = lax.rem(seq + d, slots)
            return remote(
                full, every.at[seq, at], g_send.at[8 + d], g_recv.at[8 + d], "fsdp", peer
            )

        def row_back():
            place = every.at[:, at]
            return remote(place, place, g_send.at[6], g_recv.at[6], "ctx", row_peer)

        def core_back(j):
            place = every.at[:, 2 * j + core]
            return remote(place, place, g_send.at[7 + j], g_recv.at[7 + j], "ctx", core_peer)

        core_copy(0).start()
        core_copy(1).start()

        def reduce_terms(c):
            @pl.when(c == 1)
            def _():
                for j in range(2):
                    core_copy(j).wait_recv()
                    total = terms[2 * j + core].astype(f32) + from_core[j].astype(f32)
                    with_core[j] = total.astype(bf16)
                row_copy().start()

            @pl.when(c == 3)
            def _():
                row_copy().wait_recv()
                held[...] = (with_core[row].astype(f32) + from_row[...].astype(f32)).astype(bf16)
                full[rest, :] = held[rest, :]

            @pl.when((c == 3) & outer)
            def _():
                line_a().start()

            @pl.when((c == 6) & inner)
            def _():
                line_a().wait_recv()
                total = held[:summed].astype(f32) + held_a[...].astype(f32)
                held[:summed] = total.astype(bf16)
                line_b().start()

            @pl.when((c == 8) & inner)
            def _():
                line_b().wait_recv()
                total = held[:summed].astype(f32) + held_b[...].astype(f32)
                full[:summed] = total.astype(bf16)
                line_c().start()

            @pl.when((c == 11) & outer)
            def _():
                line_c().wait_recv()

            @pl.when(c == 11)
            def _():
                every[seq, at] = full[...]
                for d in range(1, slots):
                    seq_copy(d).start()

            @pl.when(c == 13)
            def _():
                for d in range(1, slots):
                    seq_copy(d).wait_recv()
                row_back().start()

            @pl.when(c == 15)
            def _():
                row_back().wait_recv()
                core_back(0).start()
                core_back(1).start()

    def body(c, carry):
        for i, (left, right) in enumerate(zip(lefts, rights)):
            for m in range(0, left.shape[0], 256):
                term = dot_nt(left[m : m + 256, :], right[cols(c), :])
                part[m : m + 256, :] = term if i == 0 else part[m : m + 256, :] + term

        @pl.when(outer)
        def _():
            mine[c] = part[...].astype(bf16)
            copy_a(c).start()

        @pl.when(inner)
        def _():
            copy_a(c).wait_recv()
            mine[c] = (part[...] + got_a[c].astype(f32)).astype(bf16)
            copy_b(c).start()

        @pl.when(inner & (c >= 1))
        def _():
            finish(c - 1)

        if slots:
            reduce_terms(c)
        return carry

    lax.fori_loop(0, chunks, body, 0)

    @pl.when(inner)
    def _():
        finish(chunks - 1)

        def drain(c, carry):
            copy_b(c).wait_send()
            copy_c(c).wait_send()
            return carry

        lax.fori_loop(0, chunks, drain, 0)

    @pl.when(outer)
    def _():
        def drain(c, carry):
            copy_a(c).wait_send()
            copy_c(c).wait_recv()
            return carry

        lax.fori_loop(0, chunks, drain, 0)

    if slots:
        for j in range(2):
            core_copy(j).wait_send()
            core_back(j).wait()
        row_copy().wait_send()
        row_back().wait_send()
        for d in range(1, slots):
            seq_copy(d).wait_send()

        @pl.when(outer)
        def _():
            line_a().wait_send()

        @pl.when(inner)
        def _():
            line_b().wait_send()
            line_c().wait_send()


def matmul_sum(lefts, rights, collective_id, width=128, terms=None, slots=0, summed=0):
    rows = lefts[0].shape[0]
    total = rights[0].shape[0]
    chunks = total // width
    flops = sum(2 * rows * total * left.shape[1] for left in lefts)
    moved = sum(left.size + right.size for left, right in zip(lefts, rights)) + rows * total
    scratch = (
        [pltpu.VMEM((rows, width), f32)]
        + [pltpu.VMEM((chunks, rows, width), bf16)] * 3
        + [pltpu.SemaphoreType.DMA((chunks,))] * 6
    )
    shapes = [jax.ShapeDtypeStruct((rows, total), bf16)]
    operands = [*lefts, *rights]
    if slots:
        assert chunks >= 17
        block = terms.shape[1:]
        lead = (summed, block[1])
        operands.append(terms)
        shapes.append(jax.ShapeDtypeStruct((slots, *terms.shape), bf16))
        scratch += [
            pltpu.VMEM((2, *block), bf16),
            pltpu.VMEM((2, *block), bf16),
            pltpu.VMEM(block, bf16),
            pltpu.VMEM(block, bf16),
            pltpu.VMEM(lead, bf16),
            pltpu.VMEM(lead, bf16),
            pltpu.VMEM(block, bf16),
            pltpu.SemaphoreType.DMA((9 + slots,)),
            pltpu.SemaphoreType.DMA((9 + slots,)),
        ]
    vmem = pl.BlockSpec(memory_space=pltpu.VMEM)
    result = pl.pallas_call(
        functools.partial(sum_kernel, len(lefts), width, chunks, slots),
        out_shape=shapes,
        in_specs=[vmem] * len(operands),
        out_specs=[vmem] * len(shapes),
        scratch_shapes=scratch,
        compiler_params=pltpu.CompilerParams(
            collective_id=collective_id, has_side_effects=True, vmem_limit_bytes=60 * 1024 * 1024
        ),
        cost_estimate=pl.CostEstimate(flops=flops, bytes_accessed=2 * moved, transcendentals=0),
        name=f"matmul_sum_{collective_id}",
    )(*operands)
    return result if slots else result[0]


def ffn_kernel(
    n2_all,
    cot_all,
    u_gu,
    gain,
    b_gate,
    a_down,
    b_down,
    a_gu,
    ffn_all,
    h1_all,
    att_all,
    w_out,
    b_out,
    a_out,
    y_all,
    act_all,
    e_all,
    dg_all,
    du_all,
    dh_all,
    e_att_all,
    d_ob_all,
    w_gate,
    w_up,
    w_down,
    n2_buf,
    cot_buf,
    act_buf,
    e_buf,
    dg_buf,
    du_buf,
    keep_up,
    keep_gate,
    h1_buf,
    att_buf,
    cot_back,
    dh_buf,
    e_att_buf,
    d_ob_buf,
    part,
    mine,
    got_a,
    got_b,
    total,
    load_sem,
    in_sem,
    back_sem,
    out_sem,
    a_send,
    a_recv,
    b_send,
    b_recv,
    c_send,
    c_recv,
):
    n, rows, width = n2_all.shape
    ring = mine.shape[0]
    rank = b_down.shape[0]
    tile = width // 3
    z = lax.axis_index("tp")
    inner = (z == 1) | (z == 2)
    outer = (z == 0) | (z == 3)
    pair = z + 1 - 2 * lax.rem(z, 2)
    across = 3 - z

    weights = [
        pltpu.make_async_copy(
            ffn_all.at[:, pl.ds(i * width, width)], target, load_sem.at[i]
        )
        for i, target in enumerate((w_gate, w_up, w_down))
    ]

    def n2_copy(c):
        return pltpu.make_async_copy(n2_all.at[c], n2_buf.at[lax.rem(c, 2)], in_sem.at[lax.rem(c, 2)])

    def cot_copy(c):
        slot = lax.rem(c, 2)
        return pltpu.make_async_copy(cot_all.at[c], cot_buf.at[slot], in_sem.at[2 + slot])

    def last_in(i, c):
        source, target = ((h1_all, h1_buf), (att_all, att_buf), (cot_all, cot_back))[i]
        return pltpu.make_async_copy(source.at[c], target, back_sem.at[i])

    for i in range(3):
        last_in(i, 0).start()
    n2_copy(0).start()
    for copy in weights:
        copy.start()
    n2_copy(1).start()
    cot_copy(0).start()
    cot_copy(1).start()

    barrier = pltpu.get_barrier_semaphore()
    pl.semaphore_signal(barrier, inc=1, device_id={"tp": pair}, device_id_type=MESH)

    @pl.when(inner)
    def _():
        pl.semaphore_signal(barrier, inc=1, device_id={"tp": across}, device_id_type=MESH)
        pl.semaphore_wait(barrier, 2)

    @pl.when(outer)
    def _():
        pl.semaphore_wait(barrier, 1)

    def remote(source, target, send, recv, peer):
        return pltpu.make_async_remote_copy(
            source, target, send, recv, device_id={"tp": peer}, device_id_type=MESH
        )

    def copy_a(k):
        slot = lax.rem(k, ring)
        return remote(mine.at[slot], got_a.at[slot], a_send.at[k], a_recv.at[k], pair)

    def copy_b(k):
        slot = lax.rem(k, ring)
        return remote(mine.at[slot], got_b.at[slot], b_send.at[k], b_recv.at[k], across)

    def copy_c(k):
        place = total.at[lax.rem(k, n)]
        return remote(place, place, c_send.at[k], c_recv.at[k], pair)

    def finish(k):
        slot = lax.rem(k, ring)
        copy_b(k).wait_recv()
        total[lax.rem(k, n)] = (mine[slot].astype(f32) + got_b[slot].astype(f32)).astype(bf16)
        copy_c(k).start()

    def exchange(k):
        slot = lax.rem(k, ring)

        @pl.when(outer & (k >= ring))
        def _():
            copy_c(k - ring).wait_recv()
            copy_a(k - ring).wait_send()

        @pl.when(outer)
        def _():
            mine[slot] = part[...].astype(bf16)
            copy_a(k).start()

        @pl.when(inner & (k >= ring))
        def _():
            copy_b(k - ring).wait_send()

        @pl.when(inner)
        def _():
            copy_a(k).wait_recv()
            mine[slot] = (part[...] + got_a[slot].astype(f32)).astype(bf16)
            copy_b(k).start()

        @pl.when(inner & (k >= n + 1))
        def _():
            copy_c(k - 1 - n).wait_send()

        @pl.when(inner & (k >= 1))
        def _():
            finish(k - 1)

    def put(i, buf, target, c):
        return pltpu.make_async_copy(buf, target.at[c], out_sem.at[i])

    def act_out(c):
        return put(0, act_buf, act_all, c)

    def forward(k, carry):
        n2_copy(k).wait()

        @pl.when(k == 0)
        def _():
            weights[0].wait()
            weights[1].wait()

        @pl.when(k >= 1)
        def _():
            act_out(k - 1).wait()

        slot = lax.rem(k, 2)
        u_here = u_gu[k]
        for i in range(3):
            cols = slice(i * tile, (i + 1) * tile)
            gate = dot_nn(n2_buf[slot], w_gate[:, cols]) + dot_nn(u_here[:, :rank], b_gate[0, :, cols])
            upper = dot_nn(n2_buf[slot], w_up[:, cols]) + dot_nn(u_here[:, rank:], b_gate[1, :, cols])
            square = gate * gate
            slant = math.sqrt(2.0 / math.pi)
            bend = jnp.tanh(slant * (gate + 0.044715 * (square * gate)))
            side = 0.5 * (1.0 + bend)
            curve = gate * side
            rise = side + 0.5 * gate * (1.0 - bend * bend) * (
                slant * (1.0 + 3.0 * 0.044715 * square)
            )
            act_buf[:, cols] = (curve * upper).astype(bf16)
            keep_up[k, :, cols] = curve.astype(bf16)
            keep_gate[k, :, cols] = (rise * upper).astype(bf16)

        @pl.when(k + 2 < n)
        def _():
            n2_copy(k + 2).start()

        act_out(k).start()

        @pl.when(k == 0)
        def _():
            weights[2].wait()

        u_down = dot_nt(act_buf[...], a_down[...]).astype(bf16)
        for i in range(3):
            cols = slice(i * tile, (i + 1) * tile)
            part[:, cols] = dot_nt(act_buf[...], w_down[cols, :]) + dot_nn(u_down, b_down[:, cols])
        exchange(k)
        return carry

    def back_out(i, c):
        if i == 0:
            return put(1, e_buf, e_all, c)
        if i == 1:
            return put(2, dg_buf, dg_all, c)
        if i == 2:
            return put(3, du_buf, du_all, c)
        return put(4, total.at[c], y_all, c)

    def backward(c, carry):
        cot_copy(c).wait()
        back_out(3, c).start()

        @pl.when(c >= 1)
        def _():
            for i in range(3):
                back_out(i, c - 1).wait()

        slot = lax.rem(c, 2)

        def norm(i, inside):
            lines = pl.ds(pl.multiple_of(i * 16, 16), 16)
            values = total[c, lines, :].astype(f32)
            scale = lax.rsqrt(jnp.mean(values * values, axis=-1, keepdims=True) + epsilon)
            unit = values * scale
            weighted = cot_buf[slot, lines, :].astype(f32) * gain[2:3]
            e_buf[lines, :] = (
                scale * (weighted - unit * jnp.mean(weighted * unit, axis=-1, keepdims=True))
            ).astype(bf16)
            return inside

        lax.fori_loop(0, rows // 16, norm, 0)

        @pl.when(c + 2 < n)
        def _():
            cot_copy(c + 2).start()

        back_out(0, c).start()
        du_down = dot_nt(e_buf[...], b_down[...]).astype(bf16)
        for i in range(3):
            cols = slice(i * tile, (i + 1) * tile)
            d_act = dot_nn(e_buf[...], w_down[:, cols]) + dot_nn(du_down, a_down[:, cols])
            dg_buf[:, cols] = (d_act * keep_gate[c, :, cols].astype(f32)).astype(bf16)
            du_buf[:, cols] = (d_act * keep_up[c, :, cols].astype(f32)).astype(bf16)
        back_out(1, c).start()
        back_out(2, c).start()
        du_gate = dot_nt(dg_buf[...], b_gate[0]).astype(bf16)
        du_up = dot_nt(du_buf[...], b_gate[1]).astype(bf16)
        for i in range(3):
            cols = slice(i * tile, (i + 1) * tile)
            part[:, cols] = (
                dot_nt(dg_buf[...], w_gate[cols, :])
                + dot_nt(du_buf[...], w_up[cols, :])
                + dot_nn(du_gate, a_gu[0, :, cols])
                + dot_nn(du_up, a_gu[1, :, cols])
            )
        back_out(3, c).wait()
        exchange(n + c)
        return carry

    def last_out(i, c):
        source, target = (
            (dh_buf, dh_all),
            (e_att_buf, e_att_all),
            (d_ob_buf, d_ob_all),
        )[i]
        return put(5 + i, source, target, c)

    def last(c):
        for i in range(3):
            last_in(i, c).wait()

        @pl.when(c >= 1)
        def _():
            for i in range(3):
                last_out(i, c - 1).wait()

        def lines_of(i, inside):
            lines = pl.ds(pl.multiple_of(i * 16, 16), 16)
            values = h1_buf[lines, :]
            scale = lax.rsqrt(jnp.mean(values * values, axis=-1, keepdims=True) + epsilon)
            unit = values * scale
            weighted = total[c, lines, :].astype(f32) * gain[1:2]
            d_h1 = cot_back[lines, :].astype(f32) + scale * (
                weighted - unit * jnp.mean(weighted * unit, axis=-1, keepdims=True)
            )
            dh_buf[lines, :] = d_h1
            values = att_buf[lines, :].astype(f32)
            scale = lax.rsqrt(jnp.mean(values * values, axis=-1, keepdims=True) + epsilon)
            unit = values * scale
            weighted = d_h1 * gain[0:1]
            e_att_buf[lines, :] = (
                scale * (weighted - unit * jnp.mean(weighted * unit, axis=-1, keepdims=True))
            ).astype(bf16)
            return inside

        lax.fori_loop(0, rows // 16, lines_of, 0)

        @pl.when(c + 1 < n)
        def _():
            for i in range(3):
                last_in(i, c + 1).start()

        du_out = dot_nt(e_att_buf[...], b_out[...]).astype(bf16)
        d_ob_buf[...] = (dot_nn(e_att_buf[...], w_out[...]) + dot_nn(du_out, a_out[...])).astype(
            bf16
        )
        for i in range(3):
            last_out(i, c).start()

    def backward_and_last(c, carry):
        backward(c, carry)

        @pl.when(c >= ring)
        def _():
            last(c - ring)

        return carry

    lax.fori_loop(0, n, forward, 0)
    lax.fori_loop(0, n, backward_and_last, 0)
    act_out(n - 1).wait()
    for i in range(3):
        back_out(i, n - 1).wait()

    def end(c, carry):
        @pl.when(outer)
        def _():
            copy_c(n + c).wait_recv()
            copy_a(n + c).wait_send()

        @pl.when(inner & (c == n - 2))
        def _():
            copy_c(n - 1).wait_send()
            finish(2 * n - 1)

        last(c)
        return carry

    lax.fori_loop(n - ring, n, end, 0)
    for i in range(3):
        last_out(i, n - 1).wait()

    @pl.when(inner)
    def _():
        def drain(k, carry):
            copy_b(k).wait_send()
            return carry

        lax.fori_loop(2 * n - ring, 2 * n, drain, 0)

        def drain_c(k, carry):
            copy_c(k).wait_send()
            return carry

        lax.fori_loop(n, 2 * n, drain_c, 0)


def feed_forward(
    n2,
    cot,
    u_gu,
    gain,
    b_gate,
    a_down,
    b_down,
    a_gu,
    ffn_full,
    h1,
    y_att,
    w_out,
    b_out,
    a_out,
    collective_id,
):
    rows, width = n2.shape
    hidden = ffn_full.shape[1] // 3
    assert hidden == width
    step = 128
    n = rows // step
    ring = 4
    full = jax.ShapeDtypeStruct((n, step, width), bf16)
    shapes = [full] * 5 + [
        jax.ShapeDtypeStruct((n, step, width), f32),
        full,
        jax.ShapeDtypeStruct((n, step, w_out.shape[1]), bf16),
    ]
    vmem = pl.BlockSpec(memory_space=pltpu.VMEM)
    anywhere = pl.BlockSpec(memory_space=pl.ANY)
    block = pltpu.VMEM((step, width), bf16)
    results = pl.pallas_call(
        ffn_kernel,
        out_shape=shapes,
        in_specs=[anywhere] * 2 + [vmem] * 6 + [anywhere] * 3 + [vmem] * 3,
        out_specs=[anywhere] * len(shapes),
        scratch_shapes=[pltpu.VMEM((width, width), bf16)] * 3
        + [pltpu.VMEM((2, step, width), bf16)] * 2
        + [block] * 4
        + [pltpu.VMEM((n, step, width), bf16)] * 2
        + [pltpu.VMEM((step, width), f32), block, block]
        + [pltpu.VMEM((step, width), f32), block, pltpu.VMEM((step, w_out.shape[1]), bf16)]
        + [pltpu.VMEM((step, width), f32)]
        + [pltpu.VMEM((ring, step, width), bf16)] * 3
        + [pltpu.VMEM((n, step, width), bf16)]
        + [
            pltpu.SemaphoreType.DMA((3,)),
            pltpu.SemaphoreType.DMA((4,)),
            pltpu.SemaphoreType.DMA((3,)),
            pltpu.SemaphoreType.DMA((8,)),
        ]
        + [pltpu.SemaphoreType.DMA((2 * n,))] * 6,
        compiler_params=pltpu.CompilerParams(
            collective_id=collective_id, has_side_effects=True, vmem_limit_bytes=67043328
        ),
        cost_estimate=pl.CostEstimate(
            flops=12 * rows * width * hidden, bytes_accessed=60 * 2**20, transcendentals=rows * hidden
        ),
        name=f"feed_forward_{collective_id}",
    )(
        n2.reshape(n, step, width),
        cot.reshape(n, step, width),
        u_gu.reshape(n, step, -1),
        gain,
        b_gate,
        a_down,
        b_down,
        a_gu,
        ffn_full,
        h1.reshape(n, step, width),
        y_att.reshape(n, step, width),
        w_out,
        b_out,
        a_out,
    )
    return [value.reshape(rows, -1) for value in results]


def attend_kernel(tile, bases, q, limit, keys, values, out, sums):
    rows = q.shape[0]
    block = keys.shape[0] // bases.shape[0]
    last = limit[...]
    acc = jnp.zeros((rows, HEAD_SIZE), f32)
    norm = jnp.zeros((rows, 1), f32)
    for i in range(keys.shape[0] // tile):
        span = slice(i * tile, (i + 1) * tile)
        base = bases[i * tile // block] + (i * tile) % block
        raw = dot_nt(q[...], keys[span, :])
        weight = jnp.exp(soft_cap * jnp.tanh(raw * (1.0 / soft_cap)))
        place = lax.broadcasted_iota(jnp.int32, (rows, tile), 1) + base
        weight = jnp.where(place <= last, weight, 0.0)
        norm = norm + jnp.sum(weight, axis=-1, keepdims=True)
        acc = acc + dot_nn(weight.astype(bf16), values[span, :])
    out[...] = (acc / norm).astype(bf16)
    sums[...] = norm


def attend(q, limit, keys, values, bases):
    rows, cols = q.shape
    step = 256
    return pl.pallas_call(
        functools.partial(attend_kernel, 768),
        out_shape=[
            jax.ShapeDtypeStruct((rows, cols), bf16),
            jax.ShapeDtypeStruct((cols // HEAD_SIZE, rows, 1), f32),
        ],
        grid=(rows // step, cols // HEAD_SIZE),
        in_specs=[
            pl.BlockSpec(memory_space=pltpu.SMEM),
            pl.BlockSpec((step, HEAD_SIZE), lambda i, g: (i, g)),
            pl.BlockSpec((step, 1), lambda i, g: (i, 0)),
            pl.BlockSpec(keys.shape, lambda i, g: (0, 0)),
            pl.BlockSpec(keys.shape, lambda i, g: (0, 0)),
        ],
        out_specs=[
            pl.BlockSpec((step, HEAD_SIZE), lambda i, g: (i, g)),
            pl.BlockSpec((None, step, 1), lambda i, g: (g, i, 0)),
        ],
        compiler_params=pltpu.CompilerParams(vmem_limit_bytes=50 * 2**20),
        cost_estimate=pl.CostEstimate(
            flops=4 * rows * cols * keys.shape[0],
            bytes_accessed=8 * 2**20,
            transcendentals=2 * rows * cols * keys.shape[0] // HEAD_SIZE,
        ),
        name="attend",
    )(bases, q, limit, keys, values)


def attend_back_kernel(
    tile, bases, q, d_out, limit, inverse, delta, keys, values, dq, near, far, dk_sum, dv_sum
):
    rows = q.shape[0]
    total = keys.shape[0]
    block = total // bases.shape[0]
    here = pl.program_id(0) * pl.num_programs(1) + pl.program_id(1)
    steps = pl.num_programs(0) * pl.num_programs(1)

    @pl.when(here == 0)
    def _():
        dk_sum[...] = jnp.zeros_like(dk_sum)
        dv_sum[...] = jnp.zeros_like(dv_sum)

    last = limit[...]
    scale = inverse[...]
    shift = delta[...]
    dq_sum = jnp.zeros((rows, HEAD_SIZE), f32)
    for i in range(total // tile):
        span = slice(i * tile, (i + 1) * tile)
        base = bases[i * tile // block] + (i * tile) % block
        raw = dot_nt(keys[span, :], q[...])
        bend = jnp.tanh(raw * (1.0 / soft_cap))
        place = lax.broadcasted_iota(jnp.int32, (tile, rows), 0) + base
        weight = jnp.where(place <= last, jnp.exp(soft_cap * bend) * scale, 0.0)
        d_weight = dot_nt(values[span, :], d_out[...])
        d_raw = (weight * (d_weight - shift) * (1.0 - bend * bend)).astype(bf16)
        dv_sum[span, :] += dot_nn(weight.astype(bf16), d_out[...])
        dk_sum[span, :] += dot_nn(d_raw, q[...])
        dq_sum = dq_sum + dot_tn(d_raw, keys[span, :])
    dq[...] = dq_sum

    @pl.when(here == steps - 1)
    def _():
        half = total // 2
        near[0] = dk_sum[:half]
        near[1] = dv_sum[:half]
        far[0] = dk_sum[half:].astype(bf16)
        far[1] = dv_sum[half:].astype(bf16)


def attend_back(q, d_out, limit, inverse, delta, keys, values, bases):
    rows, cols = q.shape
    step = 256
    total = keys.shape[0]
    mat = pl.BlockSpec((step, HEAD_SIZE), lambda i, g: (i, g))
    line = pl.BlockSpec((None, 1, step), lambda i, g: (g, 0, i))
    whole = pl.BlockSpec(keys.shape, lambda i, g: (0, 0))
    half = (2, total // 2, HEAD_SIZE)
    return pl.pallas_call(
        functools.partial(attend_back_kernel, 768),
        out_shape=[
            jax.ShapeDtypeStruct((rows, cols), f32),
            jax.ShapeDtypeStruct(half, f32),
            jax.ShapeDtypeStruct(half, bf16),
        ],
        grid=(rows // step, cols // HEAD_SIZE),
        in_specs=[
            pl.BlockSpec(memory_space=pltpu.SMEM),
            mat,
            mat,
            pl.BlockSpec((1, step), lambda i, g: (0, i)),
            line,
            line,
            whole,
            whole,
        ],
        out_specs=[
            mat,
            pl.BlockSpec(half, lambda i, g: (0, 0, 0)),
            pl.BlockSpec(half, lambda i, g: (0, 0, 0)),
        ],
        scratch_shapes=[pltpu.VMEM((total, HEAD_SIZE), f32)] * 2,
        compiler_params=pltpu.CompilerParams(vmem_limit_bytes=60 * 2**20),
        cost_estimate=pl.CostEstimate(
            flops=10 * rows * cols * total,
            bytes_accessed=16 * 2**20,
            transcendentals=2 * rows * cols * total // HEAD_SIZE,
        ),
        name="attend_back",
    )(bases, q, d_out, limit, inverse, delta, keys, values)


def q_pairs(q_cols, k_cols):
    return k_cols == HEAD_SIZE and q_cols == QUERY_HEADS // KEY_HEADS * HEAD_SIZE


def swap(values, step):
    return lax.ppermute(values, "ctx", [(i, i ^ step) for i in range(lax.axis_size("ctx"))])


def per_device(
    tokens,
    cotangent,
    prefix_length,
    sequence_adapter_index,
    gains,
    query_weight,
    key_weight,
    value_weight,
    output_weight,
    gate_weight,
    up_weight,
    down_weight,
    adapter_first_input,
    adapter_second_query,
    adapter_second_keyvalue,
    adapter_second_gate,
    adapter_first_output,
    adapter_first_down,
    adapter_second_output,
):
    seqs, rows, width = tokens.shape
    assert seqs == 1 and lax.axis_size("ctx") == 4 and lax.axis_size("tp") == 4
    assert q_pairs(query_weight.shape[1], key_weight.shape[1])
    scale = HEAD_SIZE ** (-0.5)
    q_cols = query_weight.shape[1]
    k_cols = key_weight.shape[1]
    adapter_count, rank = adapter_second_query.shape[:2]
    both = ("fsdp", "ctx")
    adapter = sequence_adapter_index[0]

    def chosen(table, dim):
        return lax.dynamic_index_in_dim(table, adapter, dim, keepdims=False)

    def gathered(*parts):
        return lax.all_gather(jnp.concatenate(parts, axis=1), both, axis=0, tiled=True)

    kv_full = gathered(key_weight, value_weight)
    query_full = gathered(query_weight, output_weight.T)
    ffn_full = gathered(gate_weight, up_weight, down_weight.T)
    qkv_cols = q_cols + 2 * k_cols
    out_full = query_full[:, q_cols:]
    query_full = query_full[:, :q_cols]

    a_in = chosen(adapter_first_input, 1)
    b_query = chosen(adapter_second_query, 0)
    b_kv = chosen(adapter_second_keyvalue, 1)
    b_gate = chosen(adapter_second_gate, 1)
    a_out = chosen(adapter_first_output, 0)
    a_down = chosen(adapter_first_down, 0)
    b_out = chosen(adapter_second_output, 1)
    a_qkv = jnp.concatenate([a_in[0], a_in[1], a_in[2]], axis=1)
    a_gu = jnp.concatenate([a_in[3], a_in[4]], axis=1)

    ctx = lax.axis_index("ctx")
    query_pos = ctx * rows + jnp.arange(rows, dtype=jnp.int32)
    half = HEAD_SIZE // 2
    freqs = jnp.exp(jnp.arange(half, dtype=f32) * (-2.0 * math.log(10000.0) / HEAD_SIZE))
    angle = query_pos.astype(f32)[:, None] * freqs[None, :]
    cosine = jnp.cos(angle)
    sine = jnp.sin(angle)

    residual = tokens[0].astype(f32)
    d_final = cotangent[0].astype(f32)
    n1 = rms_norm(residual, gains[0]).astype(bf16)
    u_qkv = dot_nn(n1, a_qkv).astype(bf16)
    lin_kv = dot_nn(n1, kv_full)
    query = dot_nn(n1, query_full) + dot_nn(u_qkv[:, :rank], b_query)
    key = lin_kv[:, :k_cols] + dot_nn(u_qkv[:, rank : 2 * rank], b_kv[0])
    value = lin_kv[:, k_cols:] + dot_nn(u_qkv[:, 2 * rank :], b_kv[1])
    qa = (rotate(query, cosine, sine) * scale).astype(bf16)
    ka = rotate(key, cosine, sine).astype(bf16)
    va = value.astype(bf16)

    own = jnp.stack([ka, va])
    from_row = swap(own, 2)
    near = jnp.concatenate([own, from_row], axis=1)
    far = swap(near, 1)
    keys, values = jnp.concatenate([near, far], axis=1)
    bases = jnp.stack([ctx, ctx ^ 2, ctx ^ 1, ctx ^ 3]) * rows
    limit = jnp.maximum(query_pos, prefix_length[0] - 1)
    ob, sums = attend(qa, limit[:, None], keys, values, bases)

    u_out = dot_nn(ob, a_out).astype(bf16)
    y_att = matmul_sum([ob, u_out], [out_full, b_out[0].T], 1)
    h1 = residual + rms_norm(y_att.astype(f32), gains[1])
    n2 = rms_norm(h1, gains[2]).astype(bf16)
    u_gu = dot_nn(n2, a_gu).astype(bf16)
    y_ffn, act, e_ffn, d_gate, d_up, dh1, e_att, d_ob = feed_forward(
        n2,
        cotangent[0],
        u_gu,
        gains[1:],
        b_gate,
        a_down.T,
        b_out[1],
        jnp.stack([a_in[3].T, a_in[4].T]),
        ffn_full,
        h1,
        y_att,
        out_full,
        b_out[0],
        a_out.T,
        2,
    )
    overlap = d_ob.astype(f32) * ob.astype(f32)
    delta = jnp.stack(
        [
            jnp.sum(overlap[:, at : at + HEAD_SIZE], axis=-1)[None]
            for at in range(0, q_cols, HEAD_SIZE)
        ]
    )
    dqa, d_near, d_far = attend_back(
        qa,
        d_ob,
        limit[None],
        (1.0 / sums)[..., 0][:, None],
        delta,
        keys,
        values,
        bases,
    )
    d_query = (rotate(dqa, cosine, -sine) * scale).astype(bf16)
    d_near = d_near + swap(d_far, 1).astype(f32)
    d_row = d_near[:, rows:].astype(bf16)
    d_row, y_ffn, act, e_ffn, d_gate, d_up, e_att, d_query = lax.optimization_barrier(
        (d_row, y_ffn, act, e_ffn, d_gate, d_up, e_att, d_query)
    )
    d_own = d_near[:, :rows] + swap(d_row, 2).astype(f32)
    final = (h1 + rms_norm(y_ffn.astype(f32), gains[3])).astype(bf16)
    u_down = dot_nn(act, a_down).astype(bf16)
    du_down = dot_nt(e_ffn, b_out[1]).astype(bf16)
    du_out = dot_nt(e_att, b_out[0]).astype(bf16)
    du_gate = dot_nt(d_gate, b_gate[0]).astype(bf16)
    du_up = dot_nt(d_up, b_gate[1]).astype(bf16)
    du_gu = jnp.concatenate([du_gate, du_up], axis=1)

    d_key = rotate(d_own[0], cosine, -sine).astype(bf16)
    d_value = d_own[1].astype(bf16)
    d_kv = jnp.concatenate([d_key, d_value], axis=1)
    du_query = dot_nt(d_query, b_query).astype(bf16)
    du_key = dot_nt(d_key, b_kv[0]).astype(bf16)
    du_value = dot_nt(d_value, b_kv[1]).astype(bf16)
    du_qkv = jnp.concatenate([du_query, du_key, du_value], axis=1)

    wide = jnp.concatenate(
        [
            dot_tn(du_qkv, n1),
            dot_tn(du_gu, n2),
            dot_tn(u_out, e_att),
            dot_tn(u_down, e_ffn),
        ]
    )
    hidden = d_gate.shape[1]
    g_b_gate = dot_tn(u_gu[:, :rank], d_gate)
    g_b_up = dot_tn(u_gu[:, rank:], d_up)
    g_a_down = dot_tn(du_down, act)
    g_b_query = dot_tn(u_qkv[:, :rank], d_query)
    g_b_key = dot_tn(u_qkv[:, rank : 2 * rank], d_key)
    g_b_value = dot_tn(u_qkv[:, 2 * rank :], d_value)
    g_a_out = dot_tn(du_out, ob)
    small = jnp.concatenate([g_b_query, g_b_key, g_b_value, g_a_out], axis=1)
    small = jnp.pad(small, ((0, 0), (0, hidden - small.shape[1])))
    split = jnp.concatenate([g_b_gate, g_b_up, g_a_down, small])

    slots = lax.axis_size("fsdp")
    first = ((ctx == 0) & (lax.axis_index("tp") == 0)).astype(f32)
    note = jnp.full((1, width), adapter.astype(f32) * first)
    wide = jnp.pad(jnp.concatenate([wide, note]), ((0, 8 * rank - wide.shape[0] - 1), (0, 0)))
    terms = jnp.concatenate(
        [wide.reshape(4, 2 * rank, width), split.reshape(4, rank, width)], axis=1
    ).astype(bf16)
    dn1, every = matmul_sum(
        [d_query, d_kv, du_qkv], [query_full, kv_full, a_qkv], 4, terms=terms, slots=slots, summed=2 * rank
    )
    dn1 = dn1.astype(f32)
    input_grad = dh1 + norm_back(residual, gains[0], dn1)

    wide_all = every[:, :, : 2 * rank].astype(f32).reshape(slots, 8 * rank, width)
    split_all = every[:, :, 2 * rank :].astype(f32).reshape(slots, 4 * rank, width)
    used = wide_all[:, 7 * rank, 0].astype(jnp.int32)
    select = (used[:, None] == jnp.arange(adapter_count, dtype=jnp.int32)[None, :]).astype(f32)

    def to_adapters(terms):
        return jnp.sum(select[:, :, None, None] * terms[:, None], axis=0)

    share = width // (slots * lax.axis_size("ctx"))
    start = (lax.axis_index("fsdp") * lax.axis_size("ctx") + ctx) * share
    wide_own = to_adapters(lax.dynamic_slice_in_dim(wide_all, start, share, axis=2))
    wide_own = wide_own[:, : 7 * rank].reshape(adapter_count, 7, rank, share)
    split_own = to_adapters(split_all).reshape(adapter_count, 4, rank, hidden)
    grad_a_in = wide_own[:, :5].transpose(1, 0, 3, 2)
    grad_b_out = wide_own[:, 5:].transpose(1, 0, 2, 3)
    small_own = split_own[:, 3]
    grad_b_query = small_own[:, :, :q_cols]
    grad_b_kv = jnp.stack(
        [small_own[:, :, q_cols : q_cols + k_cols], small_own[:, :, q_cols + k_cols : qkv_cols]]
    )
    grad_a_out = small_own[:, :, qkv_cols : qkv_cols + q_cols].transpose(0, 2, 1)
    grad_b_gate_up = split_own[:, :2].transpose(1, 0, 2, 3)
    grad_a_down = split_own[:, 2].transpose(0, 2, 1)
    return (
        final[None],
        input_grad[None],
        grad_a_in,
        grad_b_query,
        grad_b_kv,
        grad_b_gate_up,
        grad_a_out,
        grad_a_down,
        grad_b_out,
    )


def solution(mesh):
    both = ("fsdp", "ctx")
    in_specs = (
        P("fsdp", "ctx", None),
        P("fsdp", "ctx", None),
        P("fsdp"),
        P("fsdp"),
        P(),
        P(both, "tp"),
        P(both, "tp"),
        P(both, "tp"),
        P("tp", both),
        P(both, "tp"),
        P(both, "tp"),
        P("tp", both),
        P(),
        P(None, None, "tp"),
        P(None, None, None, "tp"),
        P(None, None, None, "tp"),
        P(None, "tp", None),
        P(None, "tp", None),
        P(),
    )
    out_specs = (
        P("fsdp", "ctx", None),
        P("fsdp", "ctx", None),
        P(None, None, both, None),
        P(None, None, "tp"),
        P(None, None, None, "tp"),
        P(None, None, None, "tp"),
        P(None, "tp", None),
        P(None, "tp", None),
        P(None, None, None, both),
    )
    return jax.shard_map(
        per_device, mesh=mesh, in_specs=in_specs, out_specs=out_specs, check_vma=False
    )
```

```python
import functools
import math

import jax
import jax.numpy as jnp
from jax import lax
from jax.experimental import pallas as pl
from jax.experimental.pallas import tpu as pltpu
from jax.sharding import PartitionSpec as P

QUERY_HEADS = 8
KEY_HEADS = 4
HEAD_SIZE = 256

epsilon = 1e-06
soft_cap = 50.0
MESH = pl.DeviceIdType.MESH
f32 = jnp.float32
bf16 = jnp.bfloat16


def rms_norm(values, gain):
    return values * lax.rsqrt(jnp.mean(values * values, axis=-1, keepdims=True) + epsilon) * gain


def norm_back(values, gain, incoming):
    scale = lax.rsqrt(jnp.mean(values * values, axis=-1, keepdims=True) + epsilon)
    unit = values * scale
    weighted = incoming * gain
    return scale * (weighted - unit * jnp.mean(weighted * unit, axis=-1, keepdims=True))


def rotate(values, cosine, sine):
    half = HEAD_SIZE // 2
    parts = []
    for at in range(0, values.shape[1], HEAD_SIZE):
        first = values[:, at : at + half]
        second = values[:, at + half : at + HEAD_SIZE]
        parts += [first * cosine - second * sine, second * cosine + first * sine]
    return jnp.concatenate(parts, axis=1)


def dot_nn(left, right):
    return lax.dot_general(left, right, (((1,), (0,)), ((), ())), preferred_element_type=f32)


def dot_nt(left, right):
    return lax.dot_general(left, right, (((1,), (1,)), ((), ())), preferred_element_type=f32)


def dot_tn(left, right):
    return lax.dot_general(left, right, (((0,), (0,)), ((), ())), preferred_element_type=f32)


def gather_kernel(seqs, shard, out, w_send, w_recv, own_sem):
    at = lax.axis_index("ctx")
    core = lax.rem(at, 2)
    row = lax.div(at, 2)
    core_peer = at + 1 - 2 * core
    row_peer = at + 2 - 4 * row
    seq = lax.axis_index("fsdp")
    half = shard.shape[1] // 2
    left = pl.ds(0, half)
    right = pl.ds(half, half)
    own = pltpu.make_async_copy(shard, out.at[seq, row, core], own_sem)
    own.start()

    barrier = pltpu.get_barrier_semaphore()

    def greet(axis, peer):
        pl.semaphore_signal(barrier, inc=1, device_id={axis: peer}, device_id_type=MESH)

    greet("ctx", core_peer)
    greet("ctx", row_peer)
    for d in range(1, seqs):
        greet("fsdp", lax.rem(seq + d, seqs))
    pl.semaphore_wait(barrier, seqs + 1)

    def remote(i, source, target, axis, peer):
        return pltpu.make_async_remote_copy(
            source,
            target,
            w_send.at[i],
            w_recv.at[i],
            device_id={axis: peer},
            device_id_type=MESH,
        )

    row_first = remote(
        0, shard.at[:, right], out.at[seq, row, core, :, right], "ctx", row_peer
    )
    row_first.start()
    seq_first = []
    for d in range(1, seqs):
        peer = lax.rem(seq + d, seqs)
        copy = remote(d, shard.at[:, left], out.at[seq, row, core, :, left], "fsdp", peer)
        copy.start()
        seq_first.append(copy)
    own.wait()
    for copy in seq_first:
        copy.wait()
    place = out.at[:, row, core, :, left]
    row_second = remote(seqs, place, place, "ctx", row_peer)
    row_second.start()
    row_first.wait()
    place = out.at[seq, :, core, :, right]
    seq_second = []
    for d in range(1, seqs):
        copy = remote(seqs + d, place, place, "fsdp", lax.rem(seq + d, seqs))
        copy.start()
        seq_second.append(copy)
    row_second.wait()
    for copy in seq_second:
        copy.wait()
    place = out.at[:, :, core]
    core_last = remote(2 * seqs, place, place, "ctx", core_peer)
    core_last.start()
    core_last.wait()


def gather_shards(shard, seqs, collective_id):
    rows, cols = shard.shape
    full = pl.pallas_call(
        functools.partial(gather_kernel, seqs),
        out_shape=jax.ShapeDtypeStruct((seqs, 2, 2, rows, cols), bf16),
        in_specs=[pl.BlockSpec(memory_space=pltpu.VMEM)],
        out_specs=pl.BlockSpec(memory_space=pl.ANY),
        scratch_shapes=[
            pltpu.SemaphoreType.DMA((2 * seqs + 1,)),
            pltpu.SemaphoreType.DMA((2 * seqs + 1,)),
            pltpu.SemaphoreType.DMA,
        ],
        compiler_params=pltpu.CompilerParams(
            collective_id=collective_id, has_side_effects=True, vmem_limit_bytes=16 * 2**20
        ),
        cost_estimate=pl.CostEstimate(
            flops=0, bytes_accessed=8 * seqs * rows * cols, transcendentals=0
        ),
        name=f"gather_{collective_id}",
    )(shard)
    return full.reshape(-1, cols)


def sum_kernel(count, width, chunks, slots, *refs):
    lefts = refs[:count]
    rights = refs[count : 2 * count]
    refs = refs[2 * count :]
    terms = None
    if slots:
        terms, out, every = refs[:3]
        refs = refs[3:]
    else:
        out = refs[0]
        refs = refs[1:]
    part, mine, got_a, got_b, a_send, a_recv, b_send, b_recv, c_send, c_recv = refs[:10]
    z = lax.axis_index("tp")
    inner = (z == 1) | (z == 2)
    outer = (z == 0) | (z == 3)
    pair = z + 1 - 2 * lax.rem(z, 2)
    across = 3 - z
    barrier = pltpu.get_barrier_semaphore()

    def greet(axis, peer):
        pl.semaphore_signal(barrier, inc=1, device_id={axis: peer}, device_id_type=MESH)

    others = 0
    if slots:
        at = lax.axis_index("ctx")
        core = lax.rem(at, 2)
        row = lax.div(at, 2)
        core_peer = at + 1 - 2 * core
        row_peer = at + 2 - 4 * row
        seq = lax.axis_index("fsdp")
        others = 2 + slots - 1
        greet("ctx", core_peer)
        greet("ctx", row_peer)
        for d in range(1, slots):
            greet("fsdp", lax.rem(seq + d, slots))
    greet("tp", pair)

    @pl.when(inner)
    def _():
        greet("tp", across)
        pl.semaphore_wait(barrier, others + 2)

    @pl.when(outer)
    def _():
        pl.semaphore_wait(barrier, others + 1)

    def cols(c):
        return pl.ds(pl.multiple_of(c * width, width), width)

    def remote(source, target, send, recv, axis, peer):
        return pltpu.make_async_remote_copy(
            source, target, send, recv, device_id={axis: peer}, device_id_type=MESH
        )

    def copy_a(c):
        return remote(mine.at[c], got_a.at[c], a_send.at[c], a_recv.at[c], "tp", pair)

    def copy_b(c):
        return remote(mine.at[c], got_b.at[c], b_send.at[c], b_recv.at[c], "tp", across)

    def copy_c(c):
        place = out.at[:, cols(c)]
        return remote(place, place, c_send.at[c], c_recv.at[c], "tp", pair)

    def finish(c):
        copy_b(c).wait_recv()
        out[:, cols(c)] = (mine[c].astype(f32) + got_b[c].astype(f32)).astype(bf16)
        copy_c(c).start()

    if slots:
        from_core, with_core, from_row, held, held_a, held_b, full, g_send, g_recv = refs[10:]
        summed = held_a.shape[0]
        rest = pl.ds(summed, full.shape[0] - summed)

        def core_copy(j):
            source = terms.at[2 * j + 1 - core]
            return remote(source, from_core.at[j], g_send.at[j], g_recv.at[j], "ctx", core_peer)

        def row_copy():
            source = with_core.at[1 - row]
            return remote(source, from_row, g_send.at[2], g_recv.at[2], "ctx", row_peer)

        def line_a():
            source = held.at[pl.ds(0, summed)]
            return remote(source, held_a, g_send.at[3], g_recv.at[3], "tp", pair)

        def line_b():
            source = held.at[pl.ds(0, summed)]
            return remote(source, held_b, g_send.at[4], g_recv.at[4], "tp", across)

        def line_c():
            place = full.at[pl.ds(0, summed)]
            return remote(place, place, g_send.at[5], g_recv.at[5], "tp", pair)

        def seq_copy(d):
            peer = lax.rem(seq + d, slots)
            return remote(
                full, every.at[seq, at], g_send.at[8 + d], g_recv.at[8 + d], "fsdp", peer
            )

        def row_back():
            place = every.at[:, at]
            return remote(place, place, g_send.at[6], g_recv.at[6], "ctx", row_peer)

        def core_back(j):
            place = every.at[:, 2 * j + core]
            return remote(place, place, g_send.at[7 + j], g_recv.at[7 + j], "ctx", core_peer)

        core_copy(0).start()
        core_copy(1).start()

        def reduce_terms(c):
            @pl.when(c == 1)
            def _():
                for j in range(2):
                    core_copy(j).wait_recv()
                    total = terms[2 * j + core].astype(f32) + from_core[j].astype(f32)
                    with_core[j] = total.astype(bf16)
                row_copy().start()

            @pl.when(c == 3)
            def _():
                row_copy().wait_recv()
                held[...] = (with_core[row].astype(f32) + from_row[...].astype(f32)).astype(bf16)
                full[rest, :] = held[rest, :]

            @pl.when((c == 3) & outer)
            def _():
                line_a().start()

            @pl.when((c == 6) & inner)
            def _():
                line_a().wait_recv()
                total = held[:summed].astype(f32) + held_a[...].astype(f32)
                held[:summed] = total.astype(bf16)
                line_b().start()

            @pl.when((c == 8) & inner)
            def _():
                line_b().wait_recv()
                total = held[:summed].astype(f32) + held_b[...].astype(f32)
                full[:summed] = total.astype(bf16)
                line_c().start()

            @pl.when((c == 11) & outer)
            def _():
                line_c().wait_recv()

            @pl.when(c == 11)
            def _():
                every[seq, at] = full[...]
                for d in range(1, slots):
                    seq_copy(d).start()

            @pl.when(c == 13)
            def _():
                for d in range(1, slots):
                    seq_copy(d).wait_recv()
                row_back().start()

            @pl.when(c == 15)
            def _():
                row_back().wait_recv()
                core_back(0).start()
                core_back(1).start()

    def body(c, carry):
        for i, (left, right) in enumerate(zip(lefts, rights)):
            for m in range(0, left.shape[0], 256):
                term = dot_nt(left[m : m + 256, :], right[cols(c), :])
                part[m : m + 256, :] = term if i == 0 else part[m : m + 256, :] + term

        @pl.when(outer)
        def _():
            mine[c] = part[...].astype(bf16)
            copy_a(c).start()

        @pl.when(inner)
        def _():
            copy_a(c).wait_recv()
            mine[c] = (part[...] + got_a[c].astype(f32)).astype(bf16)
            copy_b(c).start()

        @pl.when(inner & (c >= 1))
        def _():
            finish(c - 1)

        if slots:
            reduce_terms(c)
        return carry

    lax.fori_loop(0, chunks, body, 0)

    @pl.when(inner)
    def _():
        finish(chunks - 1)

        def drain(c, carry):
            copy_b(c).wait_send()
            copy_c(c).wait_send()
            return carry

        lax.fori_loop(0, chunks, drain, 0)

    @pl.when(outer)
    def _():
        def drain(c, carry):
            copy_a(c).wait_send()
            copy_c(c).wait_recv()
            return carry

        lax.fori_loop(0, chunks, drain, 0)

    if slots:
        for j in range(2):
            core_copy(j).wait_send()
            core_back(j).wait()
        row_copy().wait_send()
        row_back().wait_send()
        for d in range(1, slots):
            seq_copy(d).wait_send()

        @pl.when(outer)
        def _():
            line_a().wait_send()

        @pl.when(inner)
        def _():
            line_b().wait_send()
            line_c().wait_send()


def matmul_sum(lefts, rights, collective_id, width=128, terms=None, slots=0, summed=0):
    rows = lefts[0].shape[0]
    total = rights[0].shape[0]
    chunks = total // width
    flops = sum(2 * rows * total * left.shape[1] for left in lefts)
    moved = sum(left.size + right.size for left, right in zip(lefts, rights)) + rows * total
    scratch = (
        [pltpu.VMEM((rows, width), f32)]
        + [pltpu.VMEM((chunks, rows, width), bf16)] * 3
        + [pltpu.SemaphoreType.DMA((chunks,))] * 6
    )
    shapes = [jax.ShapeDtypeStruct((rows, total), bf16)]
    operands = [*lefts, *rights]
    if slots:
        assert chunks >= 17
        block = terms.shape[1:]
        lead = (summed, block[1])
        operands.append(terms)
        shapes.append(jax.ShapeDtypeStruct((slots, *terms.shape), bf16))
        scratch += [
            pltpu.VMEM((2, *block), bf16),
            pltpu.VMEM((2, *block), bf16),
            pltpu.VMEM(block, bf16),
            pltpu.VMEM(block, bf16),
            pltpu.VMEM(lead, bf16),
            pltpu.VMEM(lead, bf16),
            pltpu.VMEM(block, bf16),
            pltpu.SemaphoreType.DMA((9 + slots,)),
            pltpu.SemaphoreType.DMA((9 + slots,)),
        ]
    vmem = pl.BlockSpec(memory_space=pltpu.VMEM)
    result = pl.pallas_call(
        functools.partial(sum_kernel, len(lefts), width, chunks, slots),
        out_shape=shapes,
        in_specs=[vmem] * len(operands),
        out_specs=[vmem] * len(shapes),
        scratch_shapes=scratch,
        compiler_params=pltpu.CompilerParams(
            collective_id=collective_id, has_side_effects=True, vmem_limit_bytes=60 * 1024 * 1024
        ),
        cost_estimate=pl.CostEstimate(flops=flops, bytes_accessed=2 * moved, transcendentals=0),
        name=f"matmul_sum_{collective_id}",
    )(*operands)
    return result if slots else result[0]


def ffn_kernel(
    n2_all,
    cot_all,
    u_gu,
    gain,
    b_gate,
    a_down,
    b_down,
    a_gu,
    ffn_all,
    h1_all,
    att_all,
    w_out,
    b_out,
    a_out,
    y_all,
    act_all,
    e_all,
    dg_all,
    du_all,
    dh_all,
    e_att_all,
    d_ob_all,
    w_gate,
    w_up,
    w_down,
    n2_buf,
    cot_buf,
    act_buf,
    e_buf,
    dg_buf,
    du_buf,
    keep_up,
    keep_gate,
    h1_buf,
    att_buf,
    cot_back,
    dh_buf,
    e_att_buf,
    d_ob_buf,
    part,
    mine,
    got_a,
    got_b,
    total,
    load_sem,
    in_sem,
    back_sem,
    out_sem,
    a_send,
    a_recv,
    b_send,
    b_recv,
    c_send,
    c_recv,
):
    n, rows, width = n2_all.shape
    ring = mine.shape[0]
    rank = b_down.shape[0]
    tile = width // 3
    z = lax.axis_index("tp")
    inner = (z == 1) | (z == 2)
    outer = (z == 0) | (z == 3)
    pair = z + 1 - 2 * lax.rem(z, 2)
    across = 3 - z

    weights = [
        pltpu.make_async_copy(
            ffn_all.at[:, pl.ds(i * width, width)], target, load_sem.at[i]
        )
        for i, target in enumerate((w_gate, w_up, w_down))
    ]

    def n2_copy(c):
        return pltpu.make_async_copy(n2_all.at[c], n2_buf.at[lax.rem(c, 2)], in_sem.at[lax.rem(c, 2)])

    def cot_copy(c):
        slot = lax.rem(c, 2)
        return pltpu.make_async_copy(cot_all.at[c], cot_buf.at[slot], in_sem.at[2 + slot])

    def last_in(i, c):
        source, target = ((h1_all, h1_buf), (att_all, att_buf), (cot_all, cot_back))[i]
        return pltpu.make_async_copy(source.at[c], target, back_sem.at[i])

    for i in range(3):
        last_in(i, 0).start()
    n2_copy(0).start()
    for copy in weights:
        copy.start()
    n2_copy(1).start()
    cot_copy(0).start()
    cot_copy(1).start()

    barrier = pltpu.get_barrier_semaphore()
    pl.semaphore_signal(barrier, inc=1, device_id={"tp": pair}, device_id_type=MESH)

    @pl.when(inner)
    def _():
        pl.semaphore_signal(barrier, inc=1, device_id={"tp": across}, device_id_type=MESH)
        pl.semaphore_wait(barrier, 2)

    @pl.when(outer)
    def _():
        pl.semaphore_wait(barrier, 1)

    def remote(source, target, send, recv, peer):
        return pltpu.make_async_remote_copy(
            source, target, send, recv, device_id={"tp": peer}, device_id_type=MESH
        )

    def copy_a(k):
        slot = lax.rem(k, ring)
        return remote(mine.at[slot], got_a.at[slot], a_send.at[k], a_recv.at[k], pair)

    def copy_b(k):
        slot = lax.rem(k, ring)
        return remote(mine.at[slot], got_b.at[slot], b_send.at[k], b_recv.at[k], across)

    def copy_c(k):
        place = total.at[lax.rem(k, n)]
        return remote(place, place, c_send.at[k], c_recv.at[k], pair)

    def finish(k):
        slot = lax.rem(k, ring)
        copy_b(k).wait_recv()
        total[lax.rem(k, n)] = (mine[slot].astype(f32) + got_b[slot].astype(f32)).astype(bf16)
        copy_c(k).start()

    def exchange(k):
        slot = lax.rem(k, ring)

        @pl.when(outer & (k >= ring))
        def _():
            copy_c(k - ring).wait_recv()
            copy_a(k - ring).wait_send()

        @pl.when(outer)
        def _():
            mine[slot] = part[...].astype(bf16)
            copy_a(k).start()

        @pl.when(inner & (k >= ring))
        def _():
            copy_b(k - ring).wait_send()

        @pl.when(inner)
        def _():
            copy_a(k).wait_recv()
            mine[slot] = (part[...] + got_a[slot].astype(f32)).astype(bf16)
            copy_b(k).start()

        @pl.when(inner & (k >= n + 1))
        def _():
            copy_c(k - 1 - n).wait_send()

        @pl.when(inner & (k >= 1))
        def _():
            finish(k - 1)

    def put(i, buf, target, c):
        return pltpu.make_async_copy(buf, target.at[c], out_sem.at[i])

    def act_out(c):
        return put(0, act_buf, act_all, c)

    def forward(k, carry):
        n2_copy(k).wait()

        @pl.when(k == 0)
        def _():
            weights[0].wait()
            weights[1].wait()

        @pl.when(k >= 1)
        def _():
            act_out(k - 1).wait()

        slot = lax.rem(k, 2)
        u_here = u_gu[k]
        for i in range(3):
            cols = slice(i * tile, (i + 1) * tile)
            gate = dot_nn(n2_buf[slot], w_gate[:, cols]) + dot_nn(u_here[:, :rank], b_gate[0, :, cols])
            upper = dot_nn(n2_buf[slot], w_up[:, cols]) + dot_nn(u_here[:, rank:], b_gate[1, :, cols])
            square = gate * gate
            slant = math.sqrt(2.0 / math.pi)
            bend = jnp.tanh(slant * (gate + 0.044715 * (square * gate)))
            side = 0.5 * (1.0 + bend)
            curve = gate * side
            rise = side + 0.5 * gate * (1.0 - bend * bend) * (
                slant * (1.0 + 3.0 * 0.044715 * square)
            )
            act_buf[:, cols] = (curve * upper).astype(bf16)
            keep_up[k, :, cols] = curve.astype(bf16)
            keep_gate[k, :, cols] = (rise * upper).astype(bf16)

        @pl.when(k + 2 < n)
        def _():
            n2_copy(k + 2).start()

        act_out(k).start()

        @pl.when(k == 0)
        def _():
            weights[2].wait()

        u_down = dot_nt(act_buf[...], a_down[...]).astype(bf16)
        for i in range(3):
            cols = slice(i * tile, (i + 1) * tile)
            part[:, cols] = dot_nt(act_buf[...], w_down[cols, :]) + dot_nn(u_down, b_down[:, cols])
        exchange(k)
        return carry

    def back_out(i, c):
        if i == 0:
            return put(1, e_buf, e_all, c)
        if i == 1:
            return put(2, dg_buf, dg_all, c)
        if i == 2:
            return put(3, du_buf, du_all, c)
        return put(4, total.at[c], y_all, c)

    def backward(c, carry):
        cot_copy(c).wait()
        back_out(3, c).start()

        @pl.when(c >= 1)
        def _():
            for i in range(3):
                back_out(i, c - 1).wait()

        slot = lax.rem(c, 2)

        def norm(i, inside):
            lines = pl.ds(pl.multiple_of(i * 16, 16), 16)
            values = total[c, lines, :].astype(f32)
            scale = lax.rsqrt(jnp.mean(values * values, axis=-1, keepdims=True) + epsilon)
            unit = values * scale
            weighted = cot_buf[slot, lines, :].astype(f32) * gain[2:3]
            e_buf[lines, :] = (
                scale * (weighted - unit * jnp.mean(weighted * unit, axis=-1, keepdims=True))
            ).astype(bf16)
            return inside

        lax.fori_loop(0, rows // 16, norm, 0)

        @pl.when(c + 2 < n)
        def _():
            cot_copy(c + 2).start()

        back_out(0, c).start()
        du_down = dot_nt(e_buf[...], b_down[...]).astype(bf16)
        for i in range(3):
            cols = slice(i * tile, (i + 1) * tile)
            d_act = dot_nn(e_buf[...], w_down[:, cols]) + dot_nn(du_down, a_down[:, cols])
            dg_buf[:, cols] = (d_act * keep_gate[c, :, cols].astype(f32)).astype(bf16)
            du_buf[:, cols] = (d_act * keep_up[c, :, cols].astype(f32)).astype(bf16)
        back_out(1, c).start()
        back_out(2, c).start()
        du_gate = dot_nt(dg_buf[...], b_gate[0]).astype(bf16)
        du_up = dot_nt(du_buf[...], b_gate[1]).astype(bf16)
        for i in range(3):
            cols = slice(i * tile, (i + 1) * tile)
            part[:, cols] = (
                dot_nt(dg_buf[...], w_gate[cols, :])
                + dot_nt(du_buf[...], w_up[cols, :])
                + dot_nn(du_gate, a_gu[0, :, cols])
                + dot_nn(du_up, a_gu[1, :, cols])
            )
        back_out(3, c).wait()
        exchange(n + c)
        return carry

    def last_out(i, c):
        source, target = (
            (dh_buf, dh_all),
            (e_att_buf, e_att_all),
            (d_ob_buf, d_ob_all),
        )[i]
        return put(5 + i, source, target, c)

    def last(c):
        for i in range(3):
            last_in(i, c).wait()

        @pl.when(c >= 1)
        def _():
            for i in range(3):
                last_out(i, c - 1).wait()

        def lines_of(i, inside):
            lines = pl.ds(pl.multiple_of(i * 16, 16), 16)
            values = h1_buf[lines, :]
            scale = lax.rsqrt(jnp.mean(values * values, axis=-1, keepdims=True) + epsilon)
            unit = values * scale
            weighted = total[c, lines, :].astype(f32) * gain[1:2]
            d_h1 = cot_back[lines, :].astype(f32) + scale * (
                weighted - unit * jnp.mean(weighted * unit, axis=-1, keepdims=True)
            )
            dh_buf[lines, :] = d_h1
            values = att_buf[lines, :].astype(f32)
            scale = lax.rsqrt(jnp.mean(values * values, axis=-1, keepdims=True) + epsilon)
            unit = values * scale
            weighted = d_h1 * gain[0:1]
            e_att_buf[lines, :] = (
                scale * (weighted - unit * jnp.mean(weighted * unit, axis=-1, keepdims=True))
            ).astype(bf16)
            return inside

        lax.fori_loop(0, rows // 16, lines_of, 0)

        @pl.when(c + 1 < n)
        def _():
            for i in range(3):
                last_in(i, c + 1).start()

        du_out = dot_nt(e_att_buf[...], b_out[...]).astype(bf16)
        d_ob_buf[...] = (dot_nn(e_att_buf[...], w_out[...]) + dot_nn(du_out, a_out[...])).astype(
            bf16
        )
        for i in range(3):
            last_out(i, c).start()

    def backward_and_last(c, carry):
        backward(c, carry)

        @pl.when(c >= ring)
        def _():
            last(c - ring)

        return carry

    lax.fori_loop(0, n, forward, 0)
    lax.fori_loop(0, n, backward_and_last, 0)
    act_out(n - 1).wait()
    for i in range(3):
        back_out(i, n - 1).wait()

    def end(c, carry):
        @pl.when(outer)
        def _():
            copy_c(n + c).wait_recv()
            copy_a(n + c).wait_send()

        @pl.when(inner & (c == n - 2))
        def _():
            copy_c(n - 1).wait_send()
            finish(2 * n - 1)

        last(c)
        return carry

    lax.fori_loop(n - ring, n, end, 0)
    for i in range(3):
        last_out(i, n - 1).wait()

    @pl.when(inner)
    def _():
        def drain(k, carry):
            copy_b(k).wait_send()
            return carry

        lax.fori_loop(2 * n - ring, 2 * n, drain, 0)

        def drain_c(k, carry):
            copy_c(k).wait_send()
            return carry

        lax.fori_loop(n, 2 * n, drain_c, 0)


def feed_forward(
    n2,
    cot,
    u_gu,
    gain,
    b_gate,
    a_down,
    b_down,
    a_gu,
    ffn_full,
    h1,
    y_att,
    w_out,
    b_out,
    a_out,
    collective_id,
):
    rows, width = n2.shape
    hidden = ffn_full.shape[1] // 3
    assert hidden == width
    step = 128
    n = rows // step
    ring = 4
    full = jax.ShapeDtypeStruct((n, step, width), bf16)
    shapes = [full] * 5 + [
        jax.ShapeDtypeStruct((n, step, width), f32),
        full,
        jax.ShapeDtypeStruct((n, step, w_out.shape[1]), bf16),
    ]
    vmem = pl.BlockSpec(memory_space=pltpu.VMEM)
    anywhere = pl.BlockSpec(memory_space=pl.ANY)
    block = pltpu.VMEM((step, width), bf16)
    results = pl.pallas_call(
        ffn_kernel,
        out_shape=shapes,
        in_specs=[anywhere] * 2 + [vmem] * 6 + [anywhere] * 3 + [vmem] * 3,
        out_specs=[anywhere] * len(shapes),
        scratch_shapes=[pltpu.VMEM((width, width), bf16)] * 3
        + [pltpu.VMEM((2, step, width), bf16)] * 2
        + [block] * 4
        + [pltpu.VMEM((n, step, width), bf16)] * 2
        + [pltpu.VMEM((step, width), f32), block, block]
        + [pltpu.VMEM((step, width), f32), block, pltpu.VMEM((step, w_out.shape[1]), bf16)]
        + [pltpu.VMEM((step, width), f32)]
        + [pltpu.VMEM((ring, step, width), bf16)] * 3
        + [pltpu.VMEM((n, step, width), bf16)]
        + [
            pltpu.SemaphoreType.DMA((3,)),
            pltpu.SemaphoreType.DMA((4,)),
            pltpu.SemaphoreType.DMA((3,)),
            pltpu.SemaphoreType.DMA((8,)),
        ]
        + [pltpu.SemaphoreType.DMA((2 * n,))] * 6,
        compiler_params=pltpu.CompilerParams(
            collective_id=collective_id, has_side_effects=True, vmem_limit_bytes=67043328
        ),
        cost_estimate=pl.CostEstimate(
            flops=12 * rows * width * hidden, bytes_accessed=60 * 2**20, transcendentals=rows * hidden
        ),
        name=f"feed_forward_{collective_id}",
    )(
        n2.reshape(n, step, width),
        cot.reshape(n, step, width),
        u_gu.reshape(n, step, -1),
        gain,
        b_gate,
        a_down,
        b_down,
        a_gu,
        ffn_full,
        h1.reshape(n, step, width),
        y_att.reshape(n, step, width),
        w_out,
        b_out,
        a_out,
    )
    return [value.reshape(rows, -1) for value in results]


def attend_kernel(tile, bases, q, limit, keys, values, out, sums):
    rows = q.shape[0]
    block = keys.shape[0] // bases.shape[0]
    last = limit[...]
    acc = jnp.zeros((rows, HEAD_SIZE), f32)
    norm = jnp.zeros((rows, 1), f32)
    for i in range(keys.shape[0] // tile):
        span = slice(i * tile, (i + 1) * tile)
        base = bases[i * tile // block] + (i * tile) % block
        raw = dot_nt(q[...], keys[span, :])
        weight = jnp.exp(soft_cap * jnp.tanh(raw * (1.0 / soft_cap)))
        place = lax.broadcasted_iota(jnp.int32, (rows, tile), 1) + base
        weight = jnp.where(place <= last, weight, 0.0)
        norm = norm + jnp.sum(weight, axis=-1, keepdims=True)
        acc = acc + dot_nn(weight.astype(bf16), values[span, :])
    out[...] = (acc / norm).astype(bf16)
    sums[...] = norm


def attend(q, limit, keys, values, bases):
    rows, cols = q.shape
    step = 256
    return pl.pallas_call(
        functools.partial(attend_kernel, 768),
        out_shape=[
            jax.ShapeDtypeStruct((rows, cols), bf16),
            jax.ShapeDtypeStruct((cols // HEAD_SIZE, rows, 1), f32),
        ],
        grid=(rows // step, cols // HEAD_SIZE),
        in_specs=[
            pl.BlockSpec(memory_space=pltpu.SMEM),
            pl.BlockSpec((step, HEAD_SIZE), lambda i, g: (i, g)),
            pl.BlockSpec((step, 1), lambda i, g: (i, 0)),
            pl.BlockSpec(keys.shape, lambda i, g: (0, 0)),
            pl.BlockSpec(keys.shape, lambda i, g: (0, 0)),
        ],
        out_specs=[
            pl.BlockSpec((step, HEAD_SIZE), lambda i, g: (i, g)),
            pl.BlockSpec((None, step, 1), lambda i, g: (g, i, 0)),
        ],
        compiler_params=pltpu.CompilerParams(vmem_limit_bytes=50 * 2**20),
        cost_estimate=pl.CostEstimate(
            flops=4 * rows * cols * keys.shape[0],
            bytes_accessed=8 * 2**20,
            transcendentals=2 * rows * cols * keys.shape[0] // HEAD_SIZE,
        ),
        name="attend",
    )(bases, q, limit, keys, values)


def attend_back_kernel(
    tile, bases, q, d_out, limit, inverse, delta, keys, values, dq, near, far, dk_sum, dv_sum
):
    rows = q.shape[0]
    total = keys.shape[0]
    block = total // bases.shape[0]
    here = pl.program_id(0) * pl.num_programs(1) + pl.program_id(1)
    steps = pl.num_programs(0) * pl.num_programs(1)

    @pl.when(here == 0)
    def _():
        dk_sum[...] = jnp.zeros_like(dk_sum)
        dv_sum[...] = jnp.zeros_like(dv_sum)

    last = limit[...]
    scale = inverse[...]
    shift = delta[...]
    dq_sum = jnp.zeros((rows, HEAD_SIZE), f32)
    for i in range(total // tile):
        span = slice(i * tile, (i + 1) * tile)
        base = bases[i * tile // block] + (i * tile) % block
        raw = dot_nt(keys[span, :], q[...])
        bend = jnp.tanh(raw * (1.0 / soft_cap))
        place = lax.broadcasted_iota(jnp.int32, (tile, rows), 0) + base
        weight = jnp.where(place <= last, jnp.exp(soft_cap * bend) * scale, 0.0)
        d_weight = dot_nt(values[span, :], d_out[...])
        d_raw = (weight * (d_weight - shift) * (1.0 - bend * bend)).astype(bf16)
        dv_sum[span, :] += dot_nn(weight.astype(bf16), d_out[...])
        dk_sum[span, :] += dot_nn(d_raw, q[...])
        dq_sum = dq_sum + dot_tn(d_raw, keys[span, :])
    dq[...] = dq_sum

    @pl.when(here == steps - 1)
    def _():
        half = total // 2
        near[0] = dk_sum[:half]
        near[1] = dv_sum[:half]
        far[0] = dk_sum[half:].astype(bf16)
        far[1] = dv_sum[half:].astype(bf16)


def attend_back(q, d_out, limit, inverse, delta, keys, values, bases):
    rows, cols = q.shape
    step = 256
    total = keys.shape[0]
    mat = pl.BlockSpec((step, HEAD_SIZE), lambda i, g: (i, g))
    line = pl.BlockSpec((None, 1, step), lambda i, g: (g, 0, i))
    whole = pl.BlockSpec(keys.shape, lambda i, g: (0, 0))
    half = (2, total // 2, HEAD_SIZE)
    return pl.pallas_call(
        functools.partial(attend_back_kernel, 768),
        out_shape=[
            jax.ShapeDtypeStruct((rows, cols), f32),
            jax.ShapeDtypeStruct(half, f32),
            jax.ShapeDtypeStruct(half, bf16),
        ],
        grid=(rows // step, cols // HEAD_SIZE),
        in_specs=[
            pl.BlockSpec(memory_space=pltpu.SMEM),
            mat,
            mat,
            pl.BlockSpec((1, step), lambda i, g: (0, i)),
            line,
            line,
            whole,
            whole,
        ],
        out_specs=[
            mat,
            pl.BlockSpec(half, lambda i, g: (0, 0, 0)),
            pl.BlockSpec(half, lambda i, g: (0, 0, 0)),
        ],
        scratch_shapes=[pltpu.VMEM((total, HEAD_SIZE), f32)] * 2,
        compiler_params=pltpu.CompilerParams(vmem_limit_bytes=60 * 2**20),
        cost_estimate=pl.CostEstimate(
            flops=10 * rows * cols * total,
            bytes_accessed=16 * 2**20,
            transcendentals=2 * rows * cols * total // HEAD_SIZE,
        ),
        name="attend_back",
    )(bases, q, d_out, limit, inverse, delta, keys, values)


def q_pairs(q_cols, k_cols):
    return k_cols == HEAD_SIZE and q_cols == QUERY_HEADS // KEY_HEADS * HEAD_SIZE


def swap(values, step):
    return lax.ppermute(values, "ctx", [(i, i ^ step) for i in range(lax.axis_size("ctx"))])


def per_device(
    tokens,
    cotangent,
    prefix_length,
    sequence_adapter_index,
    gains,
    query_weight,
    key_weight,
    value_weight,
    output_weight,
    gate_weight,
    up_weight,
    down_weight,
    adapter_first_input,
    adapter_second_query,
    adapter_second_keyvalue,
    adapter_second_gate,
    adapter_first_output,
    adapter_first_down,
    adapter_second_output,
):
    seqs, rows, width = tokens.shape
    assert seqs == 1 and lax.axis_size("ctx") == 4 and lax.axis_size("tp") == 4
    assert q_pairs(query_weight.shape[1], key_weight.shape[1])
    scale = HEAD_SIZE ** (-0.5)
    q_cols = query_weight.shape[1]
    k_cols = key_weight.shape[1]
    adapter_count, rank = adapter_second_query.shape[:2]
    both = ("fsdp", "ctx")
    adapter = sequence_adapter_index[0]

    def chosen(table, dim):
        return lax.dynamic_index_in_dim(table, adapter, dim, keepdims=False)

    def gathered(shard):
        return lax.all_gather(shard, both, axis=0, tiled=True)

    kv_full = gathered(jnp.concatenate([key_weight, value_weight], axis=1))
    ffn_shard = jnp.concatenate([gate_weight, up_weight, down_weight.T], axis=1)
    query_shard = jnp.concatenate([query_weight, output_weight.T], axis=1)
    residual = tokens[0].astype(f32)
    n1 = rms_norm(residual, gains[0]).astype(bf16)
    a_in = chosen(adapter_first_input, 1)
    a_qkv = jnp.concatenate([a_in[0], a_in[1], a_in[2]], axis=1)
    u_qkv = dot_nn(n1, a_qkv).astype(bf16)
    query_shard, n1, u_qkv = lax.optimization_barrier((query_shard, n1, u_qkv))
    query_full = gather_shards(query_shard, lax.axis_size("fsdp"), 3)
    kv_full, query_full = lax.optimization_barrier((kv_full, query_full))
    qkv_cols = q_cols + 2 * k_cols
    out_full = query_full[:, q_cols:]
    query_full = query_full[:, :q_cols]

    b_query = chosen(adapter_second_query, 0)
    b_kv = chosen(adapter_second_keyvalue, 1)
    b_gate = chosen(adapter_second_gate, 1)
    a_out = chosen(adapter_first_output, 0)
    a_down = chosen(adapter_first_down, 0)
    b_out = chosen(adapter_second_output, 1)
    a_gu = jnp.concatenate([a_in[3], a_in[4]], axis=1)

    ctx = lax.axis_index("ctx")
    query_pos = ctx * rows + jnp.arange(rows, dtype=jnp.int32)
    half = HEAD_SIZE // 2
    freqs = jnp.exp(jnp.arange(half, dtype=f32) * (-2.0 * math.log(10000.0) / HEAD_SIZE))
    angle = query_pos.astype(f32)[:, None] * freqs[None, :]
    cosine = jnp.cos(angle)
    sine = jnp.sin(angle)

    lin_kv = dot_nn(n1, kv_full)
    key = lin_kv[:, :k_cols] + dot_nn(u_qkv[:, rank : 2 * rank], b_kv[0])
    value = lin_kv[:, k_cols:] + dot_nn(u_qkv[:, 2 * rank :], b_kv[1])
    ka = rotate(key, cosine, sine).astype(bf16)
    va = value.astype(bf16)
    own = jnp.stack([ka, va])
    query_full, _ = lax.optimization_barrier((query_full, own))
    query = dot_nn(n1, query_full) + dot_nn(u_qkv[:, :rank], b_query)
    qa = (rotate(query, cosine, sine) * scale).astype(bf16)

    from_row = swap(own, 2)
    from_row, ffn_shard = lax.optimization_barrier((from_row, ffn_shard))
    ffn_full = gathered(ffn_shard)
    near = jnp.concatenate([own, from_row], axis=1)
    far = swap(near, 1)
    keys, values = jnp.concatenate([near, far], axis=1)
    bases = jnp.stack([ctx, ctx ^ 2, ctx ^ 1, ctx ^ 3]) * rows
    limit = jnp.maximum(query_pos, prefix_length[0] - 1)
    ob, sums = attend(qa, limit[:, None], keys, values, bases)

    u_out = dot_nn(ob, a_out).astype(bf16)
    y_att = matmul_sum([ob, u_out], [out_full, b_out[0].T], 1)
    h1 = residual + rms_norm(y_att.astype(f32), gains[1])
    n2 = rms_norm(h1, gains[2]).astype(bf16)
    u_gu = dot_nn(n2, a_gu).astype(bf16)
    y_ffn, act, e_ffn, d_gate, d_up, dh1, e_att, d_ob = feed_forward(
        n2,
        cotangent[0],
        u_gu,
        gains[1:],
        b_gate,
        a_down.T,
        b_out[1],
        jnp.stack([a_in[3].T, a_in[4].T]),
        ffn_full,
        h1,
        y_att,
        out_full,
        b_out[0],
        a_out.T,
        2,
    )
    overlap = d_ob.astype(f32) * ob.astype(f32)
    delta = jnp.stack(
        [
            jnp.sum(overlap[:, at : at + HEAD_SIZE], axis=-1)[None]
            for at in range(0, q_cols, HEAD_SIZE)
        ]
    )
    dqa, d_near, d_far = attend_back(
        qa,
        d_ob,
        limit[None],
        (1.0 / sums)[..., 0][:, None],
        delta,
        keys,
        values,
        bases,
    )
    d_query = (rotate(dqa, cosine, -sine) * scale).astype(bf16)
    d_near = d_near + swap(d_far, 1).astype(f32)
    d_row = d_near[:, rows:].astype(bf16)
    d_row, y_ffn, act, e_ffn, d_gate, d_up, e_att, d_query = lax.optimization_barrier(
        (d_row, y_ffn, act, e_ffn, d_gate, d_up, e_att, d_query)
    )
    d_own = d_near[:, :rows] + swap(d_row, 2).astype(f32)
    final = (h1 + rms_norm(y_ffn.astype(f32), gains[3])).astype(bf16)
    u_down = dot_nn(act, a_down).astype(bf16)
    du_down = dot_nt(e_ffn, b_out[1]).astype(bf16)
    du_out = dot_nt(e_att, b_out[0]).astype(bf16)
    du_gate = dot_nt(d_gate, b_gate[0]).astype(bf16)
    du_up = dot_nt(d_up, b_gate[1]).astype(bf16)
    du_gu = jnp.concatenate([du_gate, du_up], axis=1)

    d_key = rotate(d_own[0], cosine, -sine).astype(bf16)
    d_value = d_own[1].astype(bf16)
    d_kv = jnp.concatenate([d_key, d_value], axis=1)
    du_query = dot_nt(d_query, b_query).astype(bf16)
    du_key = dot_nt(d_key, b_kv[0]).astype(bf16)
    du_value = dot_nt(d_value, b_kv[1]).astype(bf16)
    du_qkv = jnp.concatenate([du_query, du_key, du_value], axis=1)

    wide = jnp.concatenate(
        [
            dot_tn(du_qkv, n1),
            dot_tn(du_gu, n2),
            dot_tn(u_out, e_att),
            dot_tn(u_down, e_ffn),
        ]
    )
    hidden = d_gate.shape[1]
    g_b_gate = dot_tn(u_gu[:, :rank], d_gate)
    g_b_up = dot_tn(u_gu[:, rank:], d_up)
    g_a_down = dot_tn(du_down, act)
    g_b_query = dot_tn(u_qkv[:, :rank], d_query)
    g_b_key = dot_tn(u_qkv[:, rank : 2 * rank], d_key)
    g_b_value = dot_tn(u_qkv[:, 2 * rank :], d_value)
    g_a_out = dot_tn(du_out, ob)
    small = jnp.concatenate([g_b_query, g_b_key, g_b_value, g_a_out], axis=1)
    small = jnp.pad(small, ((0, 0), (0, hidden - small.shape[1])))
    split = jnp.concatenate([g_b_gate, g_b_up, g_a_down, small])

    slots = lax.axis_size("fsdp")
    first = ((ctx == 0) & (lax.axis_index("tp") == 0)).astype(f32)
    note = jnp.full((1, width), adapter.astype(f32) * first)
    wide = jnp.pad(jnp.concatenate([wide, note]), ((0, 8 * rank - wide.shape[0] - 1), (0, 0)))
    terms = jnp.concatenate(
        [wide.reshape(4, 2 * rank, width), split.reshape(4, rank, width)], axis=1
    ).astype(bf16)
    dn1, every = matmul_sum(
        [d_query, d_kv, du_qkv], [query_full, kv_full, a_qkv], 4, terms=terms, slots=slots, summed=2 * rank
    )
    dn1 = dn1.astype(f32)
    input_grad = dh1 + norm_back(residual, gains[0], dn1)

    wide_all = every[:, :, : 2 * rank].astype(f32).reshape(slots, 8 * rank, width)
    split_all = every[:, :, 2 * rank :].astype(f32).reshape(slots, 4 * rank, width)
    used = wide_all[:, 7 * rank, 0].astype(jnp.int32)
    select = (used[:, None] == jnp.arange(adapter_count, dtype=jnp.int32)[None, :]).astype(f32)

    def to_adapters(terms):
        return jnp.sum(select[:, :, None, None] * terms[:, None], axis=0)

    share = width // (slots * lax.axis_size("ctx"))
    start = (lax.axis_index("fsdp") * lax.axis_size("ctx") + ctx) * share
    wide_own = to_adapters(lax.dynamic_slice_in_dim(wide_all, start, share, axis=2))
    wide_own = wide_own[:, : 7 * rank].reshape(adapter_count, 7, rank, share)
    split_own = to_adapters(split_all).reshape(adapter_count, 4, rank, hidden)
    grad_a_in = wide_own[:, :5].transpose(1, 0, 3, 2)
    grad_b_out = wide_own[:, 5:].transpose(1, 0, 2, 3)
    small_own = split_own[:, 3]
    grad_b_query = small_own[:, :, :q_cols]
    grad_b_kv = jnp.stack(
        [small_own[:, :, q_cols : q_cols + k_cols], small_own[:, :, q_cols + k_cols : qkv_cols]]
    )
    grad_a_out = small_own[:, :, qkv_cols : qkv_cols + q_cols].transpose(0, 2, 1)
    grad_b_gate_up = split_own[:, :2].transpose(1, 0, 2, 3)
    grad_a_down = split_own[:, 2].transpose(0, 2, 1)
    return (
        final[None],
        input_grad[None],
        grad_a_in,
        grad_b_query,
        grad_b_kv,
        grad_b_gate_up,
        grad_a_out,
        grad_a_down,
        grad_b_out,
    )


def solution(mesh):
    both = ("fsdp", "ctx")
    in_specs = (
        P("fsdp", "ctx", None),
        P("fsdp", "ctx", None),
        P("fsdp"),
        P("fsdp"),
        P(),
        P(both, "tp"),
        P(both, "tp"),
        P(both, "tp"),
        P("tp", both),
        P(both, "tp"),
        P(both, "tp"),
        P("tp", both),
        P(),
        P(None, None, "tp"),
        P(None, None, None, "tp"),
        P(None, None, None, "tp"),
        P(None, "tp", None),
        P(None, "tp", None),
        P(),
    )
    out_specs = (
        P("fsdp", "ctx", None),
        P("fsdp", "ctx", None),
        P(None, None, both, None),
        P(None, None, "tp"),
        P(None, None, None, "tp"),
        P(None, None, None, "tp"),
        P(None, "tp", None),
        P(None, "tp", None),
        P(None, None, None, both),
    )
    return jax.shard_map(
        per_device, mesh=mesh, in_specs=in_specs, out_specs=out_specs, check_vma=False
    )
```

```python
import functools
import math

import jax
import jax.numpy as jnp
from jax import lax
from jax.experimental import pallas as pl
from jax.experimental.pallas import tpu as pltpu
from jax.sharding import PartitionSpec as P

QUERY_HEADS = 8
KEY_HEADS = 4
HEAD_SIZE = 256

epsilon = 1e-06
soft_cap = 50.0
MESH = pl.DeviceIdType.MESH
f32 = jnp.float32
bf16 = jnp.bfloat16


def rms_norm(values, gain):
    return values * lax.rsqrt(jnp.mean(values * values, axis=-1, keepdims=True) + epsilon) * gain


def norm_back(values, gain, incoming):
    scale = lax.rsqrt(jnp.mean(values * values, axis=-1, keepdims=True) + epsilon)
    unit = values * scale
    weighted = incoming * gain
    return scale * (weighted - unit * jnp.mean(weighted * unit, axis=-1, keepdims=True))


def rotate(values, cosine, sine):
    half = HEAD_SIZE // 2
    parts = []
    for at in range(0, values.shape[1], HEAD_SIZE):
        first = values[:, at : at + half]
        second = values[:, at + half : at + HEAD_SIZE]
        parts += [first * cosine - second * sine, second * cosine + first * sine]
    return jnp.concatenate(parts, axis=1)


def dot_nn(left, right):
    return lax.dot_general(left, right, (((1,), (0,)), ((), ())), preferred_element_type=f32)


def dot_nt(left, right):
    return lax.dot_general(left, right, (((1,), (1,)), ((), ())), preferred_element_type=f32)


def dot_tn(left, right):
    return lax.dot_general(left, right, (((0,), (0,)), ((), ())), preferred_element_type=f32)


def gather_kernel(seqs, shard, out, w_send, w_recv, own_sem):
    at = lax.axis_index("ctx")
    core = lax.rem(at, 2)
    row = lax.div(at, 2)
    core_peer = at + 1 - 2 * core
    row_peer = at + 2 - 4 * row
    seq = lax.axis_index("fsdp")
    half = shard.shape[1] // 2
    left = pl.ds(0, half)
    right = pl.ds(half, half)
    own = pltpu.make_async_copy(shard, out.at[seq, row, core], own_sem)
    own.start()

    barrier = pltpu.get_barrier_semaphore()

    def greet(axis, peer):
        pl.semaphore_signal(barrier, inc=1, device_id={axis: peer}, device_id_type=MESH)

    greet("ctx", core_peer)
    greet("ctx", row_peer)
    for d in range(1, seqs):
        greet("fsdp", lax.rem(seq + d, seqs))
    pl.semaphore_wait(barrier, seqs + 1)

    def remote(i, source, target, axis, peer):
        return pltpu.make_async_remote_copy(
            source,
            target,
            w_send.at[i],
            w_recv.at[i],
            device_id={axis: peer},
            device_id_type=MESH,
        )

    row_first = remote(
        0, shard.at[:, right], out.at[seq, row, core, :, right], "ctx", row_peer
    )
    row_first.start()
    seq_first = []
    for d in range(1, seqs):
        peer = lax.rem(seq + d, seqs)
        copy = remote(d, shard.at[:, left], out.at[seq, row, core, :, left], "fsdp", peer)
        copy.start()
        seq_first.append(copy)
    own.wait()
    for copy in seq_first:
        copy.wait()
    place = out.at[:, row, core, :, left]
    row_second = remote(seqs, place, place, "ctx", row_peer)
    row_second.start()
    row_first.wait()
    place = out.at[seq, :, core, :, right]
    seq_second = []
    for d in range(1, seqs):
        copy = remote(seqs + d, place, place, "fsdp", lax.rem(seq + d, seqs))
        copy.start()
        seq_second.append(copy)
    row_second.wait()
    for copy in seq_second:
        copy.wait()
    place = out.at[:, :, core]
    core_last = remote(2 * seqs, place, place, "ctx", core_peer)
    core_last.start()
    core_last.wait()


def gather_shards(shard, seqs, collective_id):
    rows, cols = shard.shape
    full = pl.pallas_call(
        functools.partial(gather_kernel, seqs),
        out_shape=jax.ShapeDtypeStruct((seqs, 2, 2, rows, cols), bf16),
        in_specs=[pl.BlockSpec(memory_space=pltpu.VMEM)],
        out_specs=pl.BlockSpec(memory_space=pl.ANY),
        scratch_shapes=[
            pltpu.SemaphoreType.DMA((2 * seqs + 1,)),
            pltpu.SemaphoreType.DMA((2 * seqs + 1,)),
            pltpu.SemaphoreType.DMA,
        ],
        compiler_params=pltpu.CompilerParams(
            collective_id=collective_id, has_side_effects=True, vmem_limit_bytes=16 * 2**20
        ),
        cost_estimate=pl.CostEstimate(
            flops=0, bytes_accessed=8 * seqs * rows * cols, transcendentals=0
        ),
        name=f"gather_{collective_id}",
    )(shard)
    return full.reshape(-1, cols)


def sum_kernel(count, width, chunks, slots, *refs):
    lefts = refs[:count]
    rights = refs[count : 2 * count]
    refs = refs[2 * count :]
    terms = None
    if slots:
        terms, out, every = refs[:3]
        refs = refs[3:]
    else:
        out = refs[0]
        refs = refs[1:]
    part, mine, got_a, got_b, a_send, a_recv, b_send, b_recv, c_send, c_recv = refs[:10]
    z = lax.axis_index("tp")
    inner = (z == 1) | (z == 2)
    outer = (z == 0) | (z == 3)
    pair = z + 1 - 2 * lax.rem(z, 2)
    across = 3 - z
    barrier = pltpu.get_barrier_semaphore()

    def greet(axis, peer):
        pl.semaphore_signal(barrier, inc=1, device_id={axis: peer}, device_id_type=MESH)

    others = 0
    if slots:
        at = lax.axis_index("ctx")
        core = lax.rem(at, 2)
        row = lax.div(at, 2)
        core_peer = at + 1 - 2 * core
        row_peer = at + 2 - 4 * row
        seq = lax.axis_index("fsdp")
        others = 2 + slots - 1
        greet("ctx", core_peer)
        greet("ctx", row_peer)
        for d in range(1, slots):
            greet("fsdp", lax.rem(seq + d, slots))
    greet("tp", pair)

    @pl.when(inner)
    def _():
        greet("tp", across)
        pl.semaphore_wait(barrier, others + 2)

    @pl.when(outer)
    def _():
        pl.semaphore_wait(barrier, others + 1)

    def cols(c):
        return pl.ds(pl.multiple_of(c * width, width), width)

    def remote(source, target, send, recv, axis, peer):
        return pltpu.make_async_remote_copy(
            source, target, send, recv, device_id={axis: peer}, device_id_type=MESH
        )

    def copy_a(c):
        return remote(mine.at[c], got_a.at[c], a_send.at[c], a_recv.at[c], "tp", pair)

    def copy_b(c):
        return remote(mine.at[c], got_b.at[c], b_send.at[c], b_recv.at[c], "tp", across)

    def copy_c(c):
        place = out.at[:, cols(c)]
        return remote(place, place, c_send.at[c], c_recv.at[c], "tp", pair)

    def finish(c):
        copy_b(c).wait_recv()
        out[:, cols(c)] = (mine[c].astype(f32) + got_b[c].astype(f32)).astype(bf16)
        copy_c(c).start()

    if slots:
        from_core, with_core, from_row, held, held_a, held_b, full, g_send, g_recv = refs[10:]
        summed = held_a.shape[0]
        rest = pl.ds(summed, full.shape[0] - summed)

        def core_copy(j):
            source = terms.at[2 * j + 1 - core]
            return remote(source, from_core.at[j], g_send.at[j], g_recv.at[j], "ctx", core_peer)

        def row_copy():
            source = with_core.at[1 - row]
            return remote(source, from_row, g_send.at[2], g_recv.at[2], "ctx", row_peer)

        def line_a():
            source = held.at[pl.ds(0, summed)]
            return remote(source, held_a, g_send.at[3], g_recv.at[3], "tp", pair)

        def line_b():
            source = held.at[pl.ds(0, summed)]
            return remote(source, held_b, g_send.at[4], g_recv.at[4], "tp", across)

        def line_c():
            place = full.at[pl.ds(0, summed)]
            return remote(place, place, g_send.at[5], g_recv.at[5], "tp", pair)

        def seq_copy(d):
            peer = lax.rem(seq + d, slots)
            return remote(
                full, every.at[seq, at], g_send.at[8 + d], g_recv.at[8 + d], "fsdp", peer
            )

        def row_back():
            place = every.at[:, at]
            return remote(place, place, g_send.at[6], g_recv.at[6], "ctx", row_peer)

        def core_back(j):
            place = every.at[:, 2 * j + core]
            return remote(place, place, g_send.at[7 + j], g_recv.at[7 + j], "ctx", core_peer)

        core_copy(0).start()
        core_copy(1).start()

        def reduce_terms(c):
            @pl.when(c == 1)
            def _():
                for j in range(2):
                    core_copy(j).wait_recv()
                    total = terms[2 * j + core].astype(f32) + from_core[j].astype(f32)
                    with_core[j] = total.astype(bf16)
                row_copy().start()

            @pl.when(c == 3)
            def _():
                row_copy().wait_recv()
                held[...] = (with_core[row].astype(f32) + from_row[...].astype(f32)).astype(bf16)
                full[rest, :] = held[rest, :]

            @pl.when((c == 3) & outer)
            def _():
                line_a().start()

            @pl.when((c == 6) & inner)
            def _():
                line_a().wait_recv()
                total = held[:summed].astype(f32) + held_a[...].astype(f32)
                held[:summed] = total.astype(bf16)
                line_b().start()

            @pl.when((c == 8) & inner)
            def _():
                line_b().wait_recv()
                total = held[:summed].astype(f32) + held_b[...].astype(f32)
                full[:summed] = total.astype(bf16)
                line_c().start()

            @pl.when((c == 11) & outer)
            def _():
                line_c().wait_recv()

            @pl.when(c == 11)
            def _():
                every[seq, at] = full[...]
                for d in range(1, slots):
                    seq_copy(d).start()

            @pl.when(c == 13)
            def _():
                for d in range(1, slots):
                    seq_copy(d).wait_recv()
                row_back().start()

            @pl.when(c == 15)
            def _():
                row_back().wait_recv()
                core_back(0).start()
                core_back(1).start()

    def body(c, carry):
        for i, (left, right) in enumerate(zip(lefts, rights)):
            for m in range(0, left.shape[0], 256):
                term = dot_nt(left[m : m + 256, :], right[cols(c), :])
                part[m : m + 256, :] = term if i == 0 else part[m : m + 256, :] + term

        @pl.when(outer)
        def _():
            mine[c] = part[...].astype(bf16)
            copy_a(c).start()

        @pl.when(inner)
        def _():
            copy_a(c).wait_recv()
            mine[c] = (part[...] + got_a[c].astype(f32)).astype(bf16)
            copy_b(c).start()

        @pl.when(inner & (c >= 1))
        def _():
            finish(c - 1)

        if slots:
            reduce_terms(c)
        return carry

    lax.fori_loop(0, chunks, body, 0)

    @pl.when(inner)
    def _():
        finish(chunks - 1)

        def drain(c, carry):
            copy_b(c).wait_send()
            copy_c(c).wait_send()
            return carry

        lax.fori_loop(0, chunks, drain, 0)

    @pl.when(outer)
    def _():
        def drain(c, carry):
            copy_a(c).wait_send()
            copy_c(c).wait_recv()
            return carry

        lax.fori_loop(0, chunks, drain, 0)

    if slots:
        for j in range(2):
            core_copy(j).wait_send()
            core_back(j).wait()
        row_copy().wait_send()
        row_back().wait_send()
        for d in range(1, slots):
            seq_copy(d).wait_send()

        @pl.when(outer)
        def _():
            line_a().wait_send()

        @pl.when(inner)
        def _():
            line_b().wait_send()
            line_c().wait_send()


def matmul_sum(lefts, rights, collective_id, width=128, terms=None, slots=0, summed=0):
    rows = lefts[0].shape[0]
    total = rights[0].shape[0]
    chunks = total // width
    flops = sum(2 * rows * total * left.shape[1] for left in lefts)
    moved = sum(left.size + right.size for left, right in zip(lefts, rights)) + rows * total
    scratch = (
        [pltpu.VMEM((rows, width), f32)]
        + [pltpu.VMEM((chunks, rows, width), bf16)] * 3
        + [pltpu.SemaphoreType.DMA((chunks,))] * 6
    )
    shapes = [jax.ShapeDtypeStruct((rows, total), bf16)]
    operands = [*lefts, *rights]
    if slots:
        assert chunks >= 17
        block = terms.shape[1:]
        lead = (summed, block[1])
        operands.append(terms)
        shapes.append(jax.ShapeDtypeStruct((slots, *terms.shape), bf16))
        scratch += [
            pltpu.VMEM((2, *block), bf16),
            pltpu.VMEM((2, *block), bf16),
            pltpu.VMEM(block, bf16),
            pltpu.VMEM(block, bf16),
            pltpu.VMEM(lead, bf16),
            pltpu.VMEM(lead, bf16),
            pltpu.VMEM(block, bf16),
            pltpu.SemaphoreType.DMA((9 + slots,)),
            pltpu.SemaphoreType.DMA((9 + slots,)),
        ]
    vmem = pl.BlockSpec(memory_space=pltpu.VMEM)
    result = pl.pallas_call(
        functools.partial(sum_kernel, len(lefts), width, chunks, slots),
        out_shape=shapes,
        in_specs=[vmem] * len(operands),
        out_specs=[vmem] * len(shapes),
        scratch_shapes=scratch,
        compiler_params=pltpu.CompilerParams(
            collective_id=collective_id, has_side_effects=True, vmem_limit_bytes=60 * 1024 * 1024
        ),
        cost_estimate=pl.CostEstimate(flops=flops, bytes_accessed=2 * moved, transcendentals=0),
        name=f"matmul_sum_{collective_id}",
    )(*operands)
    return result if slots else result[0]


def ffn_kernel(
    n2_all,
    cot_all,
    u_gu,
    gain,
    b_gate,
    a_down,
    b_down,
    a_gu,
    ffn_all,
    h1_all,
    att_all,
    w_out,
    b_out,
    a_out,
    y_all,
    act_all,
    e_all,
    dg_all,
    du_all,
    dh_all,
    e_att_all,
    d_ob_all,
    w_gate,
    w_up,
    w_down,
    n2_buf,
    cot_buf,
    act_buf,
    e_buf,
    dg_buf,
    du_buf,
    keep_up,
    keep_gate,
    h1_buf,
    att_buf,
    cot_back,
    dh_buf,
    e_att_buf,
    d_ob_buf,
    part,
    mine,
    got_a,
    got_b,
    total,
    load_sem,
    in_sem,
    back_sem,
    out_sem,
    a_send,
    a_recv,
    b_send,
    b_recv,
    c_send,
    c_recv,
):
    n, rows, width = n2_all.shape
    ring = mine.shape[0]
    rank = b_down.shape[0]
    tile = width // 3
    z = lax.axis_index("tp")
    inner = (z == 1) | (z == 2)
    outer = (z == 0) | (z == 3)
    pair = z + 1 - 2 * lax.rem(z, 2)
    across = 3 - z

    weights = [
        pltpu.make_async_copy(
            ffn_all.at[:, pl.ds(i * width, width)], target, load_sem.at[i]
        )
        for i, target in enumerate((w_gate, w_up, w_down))
    ]

    def n2_copy(c):
        return pltpu.make_async_copy(n2_all.at[c], n2_buf.at[lax.rem(c, 2)], in_sem.at[lax.rem(c, 2)])

    def cot_copy(c):
        slot = lax.rem(c, 2)
        return pltpu.make_async_copy(cot_all.at[c], cot_buf.at[slot], in_sem.at[2 + slot])

    def last_in(i, c):
        source, target = ((h1_all, h1_buf), (att_all, att_buf), (cot_all, cot_back))[i]
        return pltpu.make_async_copy(source.at[c], target, back_sem.at[i])

    for i in range(3):
        last_in(i, 0).start()
    n2_copy(0).start()
    for copy in weights:
        copy.start()
    n2_copy(1).start()
    cot_copy(0).start()
    cot_copy(1).start()

    barrier = pltpu.get_barrier_semaphore()
    pl.semaphore_signal(barrier, inc=1, device_id={"tp": pair}, device_id_type=MESH)

    @pl.when(inner)
    def _():
        pl.semaphore_signal(barrier, inc=1, device_id={"tp": across}, device_id_type=MESH)
        pl.semaphore_wait(barrier, 2)

    @pl.when(outer)
    def _():
        pl.semaphore_wait(barrier, 1)

    def remote(source, target, send, recv, peer):
        return pltpu.make_async_remote_copy(
            source, target, send, recv, device_id={"tp": peer}, device_id_type=MESH
        )

    def copy_a(k):
        slot = lax.rem(k, ring)
        return remote(mine.at[slot], got_a.at[slot], a_send.at[k], a_recv.at[k], pair)

    def copy_b(k):
        slot = lax.rem(k, ring)
        return remote(mine.at[slot], got_b.at[slot], b_send.at[k], b_recv.at[k], across)

    def copy_c(k):
        place = total.at[lax.rem(k, n)]
        return remote(place, place, c_send.at[k], c_recv.at[k], pair)

    def finish(k):
        slot = lax.rem(k, ring)
        copy_b(k).wait_recv()
        total[lax.rem(k, n)] = (mine[slot].astype(f32) + got_b[slot].astype(f32)).astype(bf16)
        copy_c(k).start()

    def exchange(k):
        slot = lax.rem(k, ring)

        @pl.when(outer & (k >= ring))
        def _():
            copy_c(k - ring).wait_recv()
            copy_a(k - ring).wait_send()

        @pl.when(outer)
        def _():
            mine[slot] = part[...].astype(bf16)
            copy_a(k).start()

        @pl.when(inner & (k >= ring))
        def _():
            copy_b(k - ring).wait_send()

        @pl.when(inner)
        def _():
            copy_a(k).wait_recv()
            mine[slot] = (part[...] + got_a[slot].astype(f32)).astype(bf16)
            copy_b(k).start()

        @pl.when(inner & (k >= n + 1))
        def _():
            copy_c(k - 1 - n).wait_send()

        @pl.when(inner & (k >= 1))
        def _():
            finish(k - 1)

    def put(i, buf, target, c):
        return pltpu.make_async_copy(buf, target.at[c], out_sem.at[i])

    def act_out(c):
        return put(0, act_buf, act_all, c)

    def forward(k, carry):
        n2_copy(k).wait()

        @pl.when(k == 0)
        def _():
            weights[0].wait()
            weights[1].wait()

        @pl.when(k >= 1)
        def _():
            act_out(k - 1).wait()

        slot = lax.rem(k, 2)
        u_here = u_gu[k]
        for i in range(3):
            cols = slice(i * tile, (i + 1) * tile)
            gate = dot_nn(n2_buf[slot], w_gate[:, cols]) + dot_nn(u_here[:, :rank], b_gate[0, :, cols])
            upper = dot_nn(n2_buf[slot], w_up[:, cols]) + dot_nn(u_here[:, rank:], b_gate[1, :, cols])
            square = gate * gate
            slant = math.sqrt(2.0 / math.pi)
            bend = jnp.tanh(slant * (gate + 0.044715 * (square * gate)))
            side = 0.5 * (1.0 + bend)
            curve = gate * side
            rise = side + 0.5 * gate * (1.0 - bend * bend) * (
                slant * (1.0 + 3.0 * 0.044715 * square)
            )
            act_buf[:, cols] = (curve * upper).astype(bf16)
            keep_up[k, :, cols] = curve.astype(bf16)
            keep_gate[k, :, cols] = (rise * upper).astype(bf16)

        @pl.when(k + 2 < n)
        def _():
            n2_copy(k + 2).start()

        act_out(k).start()

        @pl.when(k == 0)
        def _():
            weights[2].wait()

        u_down = dot_nt(act_buf[...], a_down[...]).astype(bf16)
        for i in range(3):
            cols = slice(i * tile, (i + 1) * tile)
            part[:, cols] = dot_nt(act_buf[...], w_down[cols, :]) + dot_nn(u_down, b_down[:, cols])
        exchange(k)
        return carry

    def back_out(i, c):
        if i == 0:
            return put(1, e_buf, e_all, c)
        if i == 1:
            return put(2, dg_buf, dg_all, c)
        if i == 2:
            return put(3, du_buf, du_all, c)
        return put(4, total.at[c], y_all, c)

    def backward(c, carry):
        cot_copy(c).wait()
        back_out(3, c).start()

        @pl.when(c >= 1)
        def _():
            for i in range(3):
                back_out(i, c - 1).wait()

        slot = lax.rem(c, 2)

        def norm(i, inside):
            lines = pl.ds(pl.multiple_of(i * 16, 16), 16)
            values = total[c, lines, :].astype(f32)
            scale = lax.rsqrt(jnp.mean(values * values, axis=-1, keepdims=True) + epsilon)
            unit = values * scale
            weighted = cot_buf[slot, lines, :].astype(f32) * gain[2:3]
            e_buf[lines, :] = (
                scale * (weighted - unit * jnp.mean(weighted * unit, axis=-1, keepdims=True))
            ).astype(bf16)
            return inside

        lax.fori_loop(0, rows // 16, norm, 0)

        @pl.when(c + 2 < n)
        def _():
            cot_copy(c + 2).start()

        back_out(0, c).start()
        du_down = dot_nt(e_buf[...], b_down[...]).astype(bf16)
        for i in range(3):
            cols = slice(i * tile, (i + 1) * tile)
            d_act = dot_nn(e_buf[...], w_down[:, cols]) + dot_nn(du_down, a_down[:, cols])
            dg_buf[:, cols] = (d_act * keep_gate[c, :, cols].astype(f32)).astype(bf16)
            du_buf[:, cols] = (d_act * keep_up[c, :, cols].astype(f32)).astype(bf16)
        back_out(1, c).start()
        back_out(2, c).start()
        du_gate = dot_nt(dg_buf[...], b_gate[0]).astype(bf16)
        du_up = dot_nt(du_buf[...], b_gate[1]).astype(bf16)
        for i in range(3):
            cols = slice(i * tile, (i + 1) * tile)
            part[:, cols] = (
                dot_nt(dg_buf[...], w_gate[cols, :])
                + dot_nt(du_buf[...], w_up[cols, :])
                + dot_nn(du_gate, a_gu[0, :, cols])
                + dot_nn(du_up, a_gu[1, :, cols])
            )
        back_out(3, c).wait()
        exchange(n + c)
        return carry

    def last_out(i, c):
        source, target = (
            (dh_buf, dh_all),
            (e_att_buf, e_att_all),
            (d_ob_buf, d_ob_all),
        )[i]
        return put(5 + i, source, target, c)

    def last(c):
        for i in range(3):
            last_in(i, c).wait()

        @pl.when(c >= 1)
        def _():
            for i in range(3):
                last_out(i, c - 1).wait()

        def lines_of(i, inside):
            lines = pl.ds(pl.multiple_of(i * 16, 16), 16)
            values = h1_buf[lines, :]
            scale = lax.rsqrt(jnp.mean(values * values, axis=-1, keepdims=True) + epsilon)
            unit = values * scale
            weighted = total[c, lines, :].astype(f32) * gain[1:2]
            d_h1 = cot_back[lines, :].astype(f32) + scale * (
                weighted - unit * jnp.mean(weighted * unit, axis=-1, keepdims=True)
            )
            dh_buf[lines, :] = d_h1
            values = att_buf[lines, :].astype(f32)
            scale = lax.rsqrt(jnp.mean(values * values, axis=-1, keepdims=True) + epsilon)
            unit = values * scale
            weighted = d_h1 * gain[0:1]
            e_att_buf[lines, :] = (
                scale * (weighted - unit * jnp.mean(weighted * unit, axis=-1, keepdims=True))
            ).astype(bf16)
            return inside

        lax.fori_loop(0, rows // 16, lines_of, 0)

        @pl.when(c + 1 < n)
        def _():
            for i in range(3):
                last_in(i, c + 1).start()

        du_out = dot_nt(e_att_buf[...], b_out[...]).astype(bf16)
        d_ob_buf[...] = (dot_nn(e_att_buf[...], w_out[...]) + dot_nn(du_out, a_out[...])).astype(
            bf16
        )
        for i in range(3):
            last_out(i, c).start()

    def backward_and_last(c, carry):
        backward(c, carry)

        @pl.when(c >= ring)
        def _():
            last(c - ring)

        return carry

    lax.fori_loop(0, n, forward, 0)
    lax.fori_loop(0, n, backward_and_last, 0)
    act_out(n - 1).wait()
    for i in range(3):
        back_out(i, n - 1).wait()

    def end(c, carry):
        @pl.when(outer)
        def _():
            copy_c(n + c).wait_recv()
            copy_a(n + c).wait_send()

        @pl.when(inner & (c == n - 2))
        def _():
            copy_c(n - 1).wait_send()
            finish(2 * n - 1)

        last(c)
        return carry

    lax.fori_loop(n - ring, n, end, 0)
    for i in range(3):
        last_out(i, n - 1).wait()

    @pl.when(inner)
    def _():
        def drain(k, carry):
            copy_b(k).wait_send()
            return carry

        lax.fori_loop(2 * n - ring, 2 * n, drain, 0)

        def drain_c(k, carry):
            copy_c(k).wait_send()
            return carry

        lax.fori_loop(n, 2 * n, drain_c, 0)


def feed_forward(
    n2,
    cot,
    u_gu,
    gain,
    b_gate,
    a_down,
    b_down,
    a_gu,
    ffn_full,
    h1,
    y_att,
    w_out,
    b_out,
    a_out,
    collective_id,
):
    rows, width = n2.shape
    hidden = ffn_full.shape[1] // 3
    assert hidden == width
    step = 128
    n = rows // step
    ring = 4
    full = jax.ShapeDtypeStruct((n, step, width), bf16)
    shapes = [full] * 5 + [
        jax.ShapeDtypeStruct((n, step, width), f32),
        full,
        jax.ShapeDtypeStruct((n, step, w_out.shape[1]), bf16),
    ]
    vmem = pl.BlockSpec(memory_space=pltpu.VMEM)
    anywhere = pl.BlockSpec(memory_space=pl.ANY)
    block = pltpu.VMEM((step, width), bf16)
    results = pl.pallas_call(
        ffn_kernel,
        out_shape=shapes,
        in_specs=[anywhere] * 2 + [vmem] * 6 + [anywhere] * 3 + [vmem] * 3,
        out_specs=[anywhere] * len(shapes),
        scratch_shapes=[pltpu.VMEM((width, width), bf16)] * 3
        + [pltpu.VMEM((2, step, width), bf16)] * 2
        + [block] * 4
        + [pltpu.VMEM((n, step, width), bf16)] * 2
        + [pltpu.VMEM((step, width), f32), block, block]
        + [pltpu.VMEM((step, width), f32), block, pltpu.VMEM((step, w_out.shape[1]), bf16)]
        + [pltpu.VMEM((step, width), f32)]
        + [pltpu.VMEM((ring, step, width), bf16)] * 3
        + [pltpu.VMEM((n, step, width), bf16)]
        + [
            pltpu.SemaphoreType.DMA((3,)),
            pltpu.SemaphoreType.DMA((4,)),
            pltpu.SemaphoreType.DMA((3,)),
            pltpu.SemaphoreType.DMA((8,)),
        ]
        + [pltpu.SemaphoreType.DMA((2 * n,))] * 6,
        compiler_params=pltpu.CompilerParams(
            collective_id=collective_id, has_side_effects=True, vmem_limit_bytes=67043328
        ),
        cost_estimate=pl.CostEstimate(
            flops=12 * rows * width * hidden, bytes_accessed=60 * 2**20, transcendentals=rows * hidden
        ),
        name=f"feed_forward_{collective_id}",
    )(
        n2.reshape(n, step, width),
        cot.reshape(n, step, width),
        u_gu.reshape(n, step, -1),
        gain,
        b_gate,
        a_down,
        b_down,
        a_gu,
        ffn_full,
        h1.reshape(n, step, width),
        y_att.reshape(n, step, width),
        w_out,
        b_out,
        a_out,
    )
    return [value.reshape(rows, -1) for value in results]


def attend_kernel(tile, bases, q, limit, keys, values, out, sums):
    rows = q.shape[0]
    block = keys.shape[0] // bases.shape[0]
    last = limit[...]
    acc = jnp.zeros((rows, HEAD_SIZE), f32)
    norm = jnp.zeros((rows, 1), f32)
    for i in range(keys.shape[0] // tile):
        span = slice(i * tile, (i + 1) * tile)
        base = bases[i * tile // block] + (i * tile) % block
        raw = dot_nt(q[...], keys[span, :])
        weight = jnp.exp(soft_cap * jnp.tanh(raw * (1.0 / soft_cap)))
        place = lax.broadcasted_iota(jnp.int32, (rows, tile), 1) + base
        weight = jnp.where(place <= last, weight, 0.0)
        norm = norm + jnp.sum(weight, axis=-1, keepdims=True)
        acc = acc + dot_nn(weight.astype(bf16), values[span, :])
    out[...] = (acc / norm).astype(bf16)
    sums[...] = norm


def attend(q, limit, keys, values, bases):
    rows, cols = q.shape
    step = 256
    return pl.pallas_call(
        functools.partial(attend_kernel, 768),
        out_shape=[
            jax.ShapeDtypeStruct((rows, cols), bf16),
            jax.ShapeDtypeStruct((cols // HEAD_SIZE, rows, 1), f32),
        ],
        grid=(rows // step, cols // HEAD_SIZE),
        in_specs=[
            pl.BlockSpec(memory_space=pltpu.SMEM),
            pl.BlockSpec((step, HEAD_SIZE), lambda i, g: (i, g)),
            pl.BlockSpec((step, 1), lambda i, g: (i, 0)),
            pl.BlockSpec(keys.shape, lambda i, g: (0, 0)),
            pl.BlockSpec(keys.shape, lambda i, g: (0, 0)),
        ],
        out_specs=[
            pl.BlockSpec((step, HEAD_SIZE), lambda i, g: (i, g)),
            pl.BlockSpec((None, step, 1), lambda i, g: (g, i, 0)),
        ],
        compiler_params=pltpu.CompilerParams(vmem_limit_bytes=50 * 2**20),
        cost_estimate=pl.CostEstimate(
            flops=4 * rows * cols * keys.shape[0],
            bytes_accessed=8 * 2**20,
            transcendentals=2 * rows * cols * keys.shape[0] // HEAD_SIZE,
        ),
        name="attend",
    )(bases, q, limit, keys, values)


def attend_back_kernel(
    tile, bases, q, d_out, limit, inverse, delta, keys, values, dq, near, far, dk_sum, dv_sum
):
    rows = q.shape[0]
    total = keys.shape[0]
    block = total // bases.shape[0]
    here = pl.program_id(0) * pl.num_programs(1) + pl.program_id(1)
    steps = pl.num_programs(0) * pl.num_programs(1)

    @pl.when(here == 0)
    def _():
        dk_sum[...] = jnp.zeros_like(dk_sum)
        dv_sum[...] = jnp.zeros_like(dv_sum)

    last = limit[...]
    scale = inverse[...]
    shift = delta[...]
    dq_sum = jnp.zeros((rows, HEAD_SIZE), f32)
    for i in range(total // tile):
        span = slice(i * tile, (i + 1) * tile)
        base = bases[i * tile // block] + (i * tile) % block
        raw = dot_nt(keys[span, :], q[...])
        bend = jnp.tanh(raw * (1.0 / soft_cap))
        place = lax.broadcasted_iota(jnp.int32, (tile, rows), 0) + base
        weight = jnp.where(place <= last, jnp.exp(soft_cap * bend) * scale, 0.0)
        d_weight = dot_nt(values[span, :], d_out[...])
        d_raw = (weight * (d_weight - shift) * (1.0 - bend * bend)).astype(bf16)
        dv_sum[span, :] += dot_nn(weight.astype(bf16), d_out[...])
        dk_sum[span, :] += dot_nn(d_raw, q[...])
        dq_sum = dq_sum + dot_tn(d_raw, keys[span, :])
    dq[...] = dq_sum

    @pl.when(here == steps - 1)
    def _():
        half = total // 2
        near[0] = dk_sum[:half]
        near[1] = dv_sum[:half]
        far[0] = dk_sum[half:].astype(bf16)
        far[1] = dv_sum[half:].astype(bf16)


def attend_back(q, d_out, limit, inverse, delta, keys, values, bases):
    rows, cols = q.shape
    step = 256
    total = keys.shape[0]
    mat = pl.BlockSpec((step, HEAD_SIZE), lambda i, g: (i, g))
    line = pl.BlockSpec((None, 1, step), lambda i, g: (g, 0, i))
    whole = pl.BlockSpec(keys.shape, lambda i, g: (0, 0))
    half = (2, total // 2, HEAD_SIZE)
    return pl.pallas_call(
        functools.partial(attend_back_kernel, 768),
        out_shape=[
            jax.ShapeDtypeStruct((rows, cols), f32),
            jax.ShapeDtypeStruct(half, f32),
            jax.ShapeDtypeStruct(half, bf16),
        ],
        grid=(rows // step, cols // HEAD_SIZE),
        in_specs=[
            pl.BlockSpec(memory_space=pltpu.SMEM),
            mat,
            mat,
            pl.BlockSpec((1, step), lambda i, g: (0, i)),
            line,
            line,
            whole,
            whole,
        ],
        out_specs=[
            mat,
            pl.BlockSpec(half, lambda i, g: (0, 0, 0)),
            pl.BlockSpec(half, lambda i, g: (0, 0, 0)),
        ],
        scratch_shapes=[pltpu.VMEM((total, HEAD_SIZE), f32)] * 2,
        compiler_params=pltpu.CompilerParams(vmem_limit_bytes=60 * 2**20),
        cost_estimate=pl.CostEstimate(
            flops=10 * rows * cols * total,
            bytes_accessed=16 * 2**20,
            transcendentals=2 * rows * cols * total // HEAD_SIZE,
        ),
        name="attend_back",
    )(bases, q, d_out, limit, inverse, delta, keys, values)


def q_pairs(q_cols, k_cols):
    return k_cols == HEAD_SIZE and q_cols == QUERY_HEADS // KEY_HEADS * HEAD_SIZE


def swap(values, step):
    return lax.ppermute(values, "ctx", [(i, i ^ step) for i in range(lax.axis_size("ctx"))])


def per_device(
    tokens,
    cotangent,
    prefix_length,
    sequence_adapter_index,
    gains,
    query_weight,
    key_weight,
    value_weight,
    output_weight,
    gate_weight,
    up_weight,
    down_weight,
    adapter_first_input,
    adapter_second_query,
    adapter_second_keyvalue,
    adapter_second_gate,
    adapter_first_output,
    adapter_first_down,
    adapter_second_output,
):
    seqs, rows, width = tokens.shape
    assert seqs == 1 and lax.axis_size("ctx") == 4 and lax.axis_size("tp") == 4
    assert q_pairs(query_weight.shape[1], key_weight.shape[1])
    scale = HEAD_SIZE ** (-0.5)
    q_cols = query_weight.shape[1]
    k_cols = key_weight.shape[1]
    adapter_count, rank = adapter_second_query.shape[:2]
    both = ("fsdp", "ctx")
    adapter = sequence_adapter_index[0]

    def chosen(table, dim):
        return lax.dynamic_index_in_dim(table, adapter, dim, keepdims=False)

    def gathered(shard):
        return lax.all_gather(shard, both, axis=0, tiled=True)

    kv_full = gathered(jnp.concatenate([key_weight, value_weight], axis=1))
    ffn_shard = jnp.concatenate([gate_weight, up_weight, down_weight.T], axis=1)
    query_shard = jnp.concatenate([query_weight, output_weight.T], axis=1)
    residual = tokens[0].astype(f32)
    n1 = rms_norm(residual, gains[0]).astype(bf16)
    a_in = chosen(adapter_first_input, 1)
    a_qkv = jnp.concatenate([a_in[0], a_in[1], a_in[2]], axis=1)
    u_qkv = dot_nn(n1, a_qkv).astype(bf16)
    query_shard, n1, u_qkv = lax.optimization_barrier((query_shard, n1, u_qkv))
    query_full = gather_shards(query_shard, lax.axis_size("fsdp"), 3)
    kv_full, query_full, ffn_shard = lax.optimization_barrier((kv_full, query_full, ffn_shard))
    ffn_full = gathered(ffn_shard)
    qkv_cols = q_cols + 2 * k_cols
    out_full = query_full[:, q_cols:]
    query_full = query_full[:, :q_cols]

    b_query = chosen(adapter_second_query, 0)
    b_kv = chosen(adapter_second_keyvalue, 1)
    b_gate = chosen(adapter_second_gate, 1)
    a_out = chosen(adapter_first_output, 0)
    a_down = chosen(adapter_first_down, 0)
    b_out = chosen(adapter_second_output, 1)

    ctx = lax.axis_index("ctx")
    query_pos = ctx * rows + jnp.arange(rows, dtype=jnp.int32)
    half = HEAD_SIZE // 2
    freqs = jnp.exp(jnp.arange(half, dtype=f32) * (-2.0 * math.log(10000.0) / HEAD_SIZE))
    angle = query_pos.astype(f32)[:, None] * freqs[None, :]
    cosine = jnp.cos(angle)
    sine = jnp.sin(angle)

    lin_kv = dot_nn(n1, kv_full)
    key = lin_kv[:, :k_cols] + dot_nn(u_qkv[:, rank : 2 * rank], b_kv[0])
    value = lin_kv[:, k_cols:] + dot_nn(u_qkv[:, 2 * rank :], b_kv[1])
    ka = rotate(key, cosine, sine).astype(bf16)
    va = value.astype(bf16)
    own = jnp.stack([ka, va])
    query_full, _ = lax.optimization_barrier((query_full, own))
    query = dot_nn(n1, query_full) + dot_nn(u_qkv[:, :rank], b_query)
    qa = (rotate(query, cosine, sine) * scale).astype(bf16)

    from_row = swap(own, 2)
    from_row, qa, a_gu, b_gate, a_down_t, a_out_t = lax.optimization_barrier(
        (from_row, qa, jnp.stack([a_in[3].T, a_in[4].T]), b_gate, a_down.T, a_out.T)
    )
    near = jnp.concatenate([own, from_row], axis=1)
    far = swap(near, 1)
    keys, values = jnp.concatenate([near, far], axis=1)
    bases = jnp.stack([ctx, ctx ^ 2, ctx ^ 1, ctx ^ 3]) * rows
    limit = jnp.maximum(query_pos, prefix_length[0] - 1)
    ob, sums = attend(qa, limit[:, None], keys, values, bases)

    u_out = dot_nn(ob, a_out).astype(bf16)
    y_att = matmul_sum([ob, u_out], [out_full, b_out[0].T], 1)
    h1 = residual + rms_norm(y_att.astype(f32), gains[1])
    n2 = rms_norm(h1, gains[2]).astype(bf16)
    u_gu = dot_nt(n2, a_gu.reshape(2 * rank, width)).astype(bf16)
    y_ffn, act, e_ffn, d_gate, d_up, dh1, e_att, d_ob = feed_forward(
        n2,
        cotangent[0],
        u_gu,
        gains[1:],
        b_gate,
        a_down_t,
        b_out[1],
        a_gu,
        ffn_full,
        h1,
        y_att,
        out_full,
        b_out[0],
        a_out_t,
        2,
    )
    overlap = d_ob.astype(f32) * ob.astype(f32)
    delta = jnp.stack(
        [
            jnp.sum(overlap[:, at : at + HEAD_SIZE], axis=-1)[None]
            for at in range(0, q_cols, HEAD_SIZE)
        ]
    )
    dqa, d_near, d_far = attend_back(
        qa,
        d_ob,
        limit[None],
        (1.0 / sums)[..., 0][:, None],
        delta,
        keys,
        values,
        bases,
    )
    d_query = (rotate(dqa, cosine, -sine) * scale).astype(bf16)
    d_near = d_near + swap(d_far, 1).astype(f32)
    d_row = d_near[:, rows:].astype(bf16)
    d_row, y_ffn, act, e_ffn, d_gate, d_up, e_att, d_query = lax.optimization_barrier(
        (d_row, y_ffn, act, e_ffn, d_gate, d_up, e_att, d_query)
    )
    d_own = d_near[:, :rows] + swap(d_row, 2).astype(f32)
    final = (h1 + rms_norm(y_ffn.astype(f32), gains[3])).astype(bf16)
    u_down = dot_nn(act, a_down).astype(bf16)
    du_down = dot_nt(e_ffn, b_out[1]).astype(bf16)
    du_out = dot_nt(e_att, b_out[0]).astype(bf16)
    du_gate = dot_nt(d_gate, b_gate[0]).astype(bf16)
    du_up = dot_nt(d_up, b_gate[1]).astype(bf16)
    du_gu = jnp.concatenate([du_gate, du_up], axis=1)

    d_key = rotate(d_own[0], cosine, -sine).astype(bf16)
    d_value = d_own[1].astype(bf16)
    d_kv = jnp.concatenate([d_key, d_value], axis=1)
    du_query = dot_nt(d_query, b_query).astype(bf16)
    du_key = dot_nt(d_key, b_kv[0]).astype(bf16)
    du_value = dot_nt(d_value, b_kv[1]).astype(bf16)
    du_qkv = jnp.concatenate([du_query, du_key, du_value], axis=1)

    wide = jnp.concatenate(
        [
            dot_tn(du_qkv, n1),
            dot_tn(du_gu, n2),
            dot_tn(u_out, e_att),
            dot_tn(u_down, e_ffn),
        ]
    )
    hidden = d_gate.shape[1]
    g_b_gate = dot_tn(u_gu[:, :rank], d_gate)
    g_b_up = dot_tn(u_gu[:, rank:], d_up)
    g_a_down = dot_tn(du_down, act)
    g_b_query = dot_tn(u_qkv[:, :rank], d_query)
    g_b_key = dot_tn(u_qkv[:, rank : 2 * rank], d_key)
    g_b_value = dot_tn(u_qkv[:, 2 * rank :], d_value)
    g_a_out = dot_tn(du_out, ob)
    small = jnp.concatenate([g_b_query, g_b_key, g_b_value, g_a_out], axis=1)
    small = jnp.pad(small, ((0, 0), (0, hidden - small.shape[1])))
    split = jnp.concatenate([g_b_gate, g_b_up, g_a_down, small])

    slots = lax.axis_size("fsdp")
    first = ((ctx == 0) & (lax.axis_index("tp") == 0)).astype(f32)
    note = jnp.full((1, width), adapter.astype(f32) * first)
    wide = jnp.pad(jnp.concatenate([wide, note]), ((0, 8 * rank - wide.shape[0] - 1), (0, 0)))
    terms = jnp.concatenate(
        [wide.reshape(4, 2 * rank, width), split.reshape(4, rank, width)], axis=1
    ).astype(bf16)
    dn1, every = matmul_sum(
        [d_query, d_kv, du_qkv], [query_full, kv_full, a_qkv], 4, terms=terms, slots=slots, summed=2 * rank
    )
    dn1 = dn1.astype(f32)
    input_grad = dh1 + norm_back(residual, gains[0], dn1)

    wide_all = every[:, :, : 2 * rank].astype(f32).reshape(slots, 8 * rank, width)
    split_all = every[:, :, 2 * rank :].astype(f32).reshape(slots, 4 * rank, width)
    used = wide_all[:, 7 * rank, 0].astype(jnp.int32)
    select = (used[:, None] == jnp.arange(adapter_count, dtype=jnp.int32)[None, :]).astype(f32)

    def to_adapters(terms):
        return jnp.sum(select[:, :, None, None] * terms[:, None], axis=0)

    share = width // (slots * lax.axis_size("ctx"))
    start = (lax.axis_index("fsdp") * lax.axis_size("ctx") + ctx) * share
    wide_own = to_adapters(lax.dynamic_slice_in_dim(wide_all, start, share, axis=2))
    wide_own = wide_own[:, : 7 * rank].reshape(adapter_count, 7, rank, share)
    split_own = to_adapters(split_all).reshape(adapter_count, 4, rank, hidden)
    grad_a_in = wide_own[:, :5].transpose(1, 0, 3, 2)
    grad_b_out = wide_own[:, 5:].transpose(1, 0, 2, 3)
    small_own = split_own[:, 3]
    grad_b_query = small_own[:, :, :q_cols]
    grad_b_kv = jnp.stack(
        [small_own[:, :, q_cols : q_cols + k_cols], small_own[:, :, q_cols + k_cols : qkv_cols]]
    )
    grad_a_out = small_own[:, :, qkv_cols : qkv_cols + q_cols].transpose(0, 2, 1)
    grad_b_gate_up = split_own[:, :2].transpose(1, 0, 2, 3)
    grad_a_down = split_own[:, 2].transpose(0, 2, 1)
    return (
        final[None],
        input_grad[None],
        grad_a_in,
        grad_b_query,
        grad_b_kv,
        grad_b_gate_up,
        grad_a_out,
        grad_a_down,
        grad_b_out,
    )


def solution(mesh):
    both = ("fsdp", "ctx")
    in_specs = (
        P("fsdp", "ctx", None),
        P("fsdp", "ctx", None),
        P("fsdp"),
        P("fsdp"),
        P(),
        P(both, "tp"),
        P(both, "tp"),
        P(both, "tp"),
        P("tp", both),
        P(both, "tp"),
        P(both, "tp"),
        P("tp", both),
        P(),
        P(None, None, "tp"),
        P(None, None, None, "tp"),
        P(None, None, None, "tp"),
        P(None, "tp", None),
        P(None, "tp", None),
        P(),
    )
    out_specs = (
        P("fsdp", "ctx", None),
        P("fsdp", "ctx", None),
        P(None, None, both, None),
        P(None, None, "tp"),
        P(None, None, None, "tp"),
        P(None, None, None, "tp"),
        P(None, "tp", None),
        P(None, "tp", None),
        P(None, None, None, both),
    )
    return jax.shard_map(
        per_device, mesh=mesh, in_specs=in_specs, out_specs=out_specs, check_vma=False
    )
```
